32 devices in a mesh: data: 1 (over z), dap2: 4 (over y), dap: 8 (over x, core).
Axes of the slice: x: 4, y: 4, z: 1, core: 2. Of those that a mesh axis runs over, the one named last changes fastest.
The devices are a block of a 4x4x8 slice.
Arguments:
- pair_act: float32 [384, 384, 128], P(('data', 'dap'), 'dap2')
- pair_mask: int32 [384, 384], P(('data', 'dap'), 'dap2')
- ln_z: bfloat16 [4, 2, 2, 128], replicated
- w_ab: bfloat16 [4, 2, 128, 512], replicated
- w_g: bfloat16 [4, 2, 128, 128], replicated
- ln_x: bfloat16 [4, 2, 2, 128], replicated
- w_o: bfloat16 [4, 2, 128, 128], replicated
Outputs:
- output: float32 [384, 384, 128], P(('data', 'dap'), 'dap2')
All inputs are finite; a program needn't handle non-finite values.
Results may differ from the reference program's by a relative error of at most 0.00360306.
Values are sent between devices in bfloat16 or wider.
A program may use at most 768 MiB of HBM per device.

```python
import jax
import jax.numpy as jnp
from jax import lax

N_RES = 384
C_Z = 128
C_HID = 128
LAYERS = 4
ROW_BLOCK = 64
LN_EPS = 1e-5


def norm_params(base_key, width):
    key_gain, key_bias = jax.random.split(base_key)
    gain = 1.0 + 0.3 * jax.random.normal(key_gain, (LAYERS, 2, 1, width), jnp.float32)
    bias = 0.3 * jax.random.normal(key_bias, (LAYERS, 2, 1, width), jnp.float32)
    return jnp.concatenate([gain, bias], axis=2).astype(jnp.bfloat16)


def setup_inputs(seed: int = 0, part: int = 0) -> dict:
    part_key = jax.random.fold_in(jax.random.key(seed), part)
    key_act, key_len, key_hole = jax.random.split(part_key, 3)
    key_lnz, key_ab, key_gate, key_lnx, key_out = jax.random.split(jax.random.key(seed + 1), 5)
    pair_act = jax.random.normal(key_act, (N_RES, N_RES, C_Z), jnp.float32)
    valid_len = jax.random.randint(key_len, (), N_RES - N_RES // 8, N_RES - N_RES // 16 + 1)
    hole_draw = jax.random.randint(key_hole, (N_RES, N_RES), 0, 32)
    inside = jnp.arange(N_RES) < valid_len
    pair_mask = (inside[:, None] & inside[None, :] & (hole_draw != 0)).astype(jnp.int32)
    w_ab = (jax.random.normal(key_ab, (LAYERS, 2, C_Z, 4 * C_HID), jnp.float32) * C_Z ** -0.5).astype(jnp.bfloat16)
    w_g = (jax.random.normal(key_gate, (LAYERS, 2, C_Z, C_Z), jnp.float32) * C_Z ** -0.5).astype(jnp.bfloat16)
    w_o = (jax.random.normal(key_out, (LAYERS, 2, C_HID, C_Z), jnp.float32) * (C_HID * LAYERS) ** -0.5).astype(jnp.bfloat16)
    return {"pair_act": pair_act, "pair_mask": pair_mask, "ln_z": norm_params(key_lnz, C_Z), "w_ab": w_ab, "w_g": w_g, "ln_x": norm_params(key_lnx, C_HID), "w_o": w_o}


def layer_norm(values, params):
    mean = jnp.mean(values, axis=-1, keepdims=True)
    centered = values - mean
    variance = jnp.mean(centered * centered, axis=-1, keepdims=True)
    scaled = centered * lax.rsqrt(variance + LN_EPS)
    return (scaled * params[0].astype(jnp.float32) + params[1].astype(jnp.float32)).astype(jnp.bfloat16)


def project_rows(z_rows, mask_rows, ln_params, w_ab):
    z_norm = layer_norm(z_rows, ln_params)
    projected = jnp.dot(z_norm.reshape(-1, C_Z), w_ab, preferred_element_type=jnp.float32).reshape(ROW_BLOCK, N_RES, 4 * C_HID)
    keep_mask = mask_rows.astype(jnp.float32)[:, :, None]
    a_proj = (keep_mask * jax.nn.sigmoid(projected[:, :, C_HID:2 * C_HID]) * projected[:, :, :C_HID]).astype(jnp.bfloat16)
    b_proj = (keep_mask * jax.nn.sigmoid(projected[:, :, 3 * C_HID:]) * projected[:, :, 2 * C_HID:3 * C_HID]).astype(jnp.bfloat16)
    return a_proj, b_proj


def tri_update(pair_state, pair_mask, ln_z, w_ab, w_g, ln_x, w_o, outgoing):
    n_blocks = N_RES // ROW_BLOCK
    z_blocks = pair_state.reshape(n_blocks, ROW_BLOCK, N_RES, C_Z)
    mask_blocks = pair_mask.reshape(n_blocks, ROW_BLOCK, N_RES)

    def project_block(block_pair):
        return project_rows(block_pair[0], block_pair[1], ln_z, w_ab)

    a_all, b_all = lax.map(project_block, (z_blocks, mask_blocks))
    a_all = a_all.reshape(N_RES, N_RES, C_HID)
    b_all = b_all.reshape(N_RES, N_RES, C_HID)
    if not outgoing:
        a_all = jnp.swapaxes(a_all, 0, 1)
        b_all = jnp.swapaxes(b_all, 0, 1)
    b_wide = b_all.astype(jnp.float32)

    def finish_block(block_pair):
        z_rows, a_rows = block_pair
        x_sum = jnp.einsum("ikc,jkc->ijc", a_rows.astype(jnp.float32), b_wide)
        x_norm = layer_norm(x_sum, ln_x)
        update_val = jnp.dot(x_norm.reshape(-1, C_HID), w_o, preferred_element_type=jnp.float32).reshape(ROW_BLOCK, N_RES, C_Z)
        z_norm = layer_norm(z_rows, ln_z)
        gate_val = jax.nn.sigmoid(jnp.dot(z_norm.reshape(-1, C_Z), w_g, preferred_element_type=jnp.float32)).reshape(ROW_BLOCK, N_RES, C_Z)
        return z_rows + gate_val * update_val

    new_blocks = lax.map(finish_block, (z_blocks, a_all.reshape(n_blocks, ROW_BLOCK, N_RES, C_HID)))
    return new_blocks.reshape(N_RES, N_RES, C_Z)


def reference(pair_act, pair_mask, ln_z, w_ab, w_g, ln_x, w_o):
    def one_layer(pair_state, layer_params):
        ln_z_layer, w_ab_layer, w_g_layer, ln_x_layer, w_o_layer = layer_params
        pair_state = tri_update(pair_state, pair_mask, ln_z_layer[0], w_ab_layer[0], w_g_layer[0], ln_x_layer[0], w_o_layer[0], True)
        pair_state = tri_update(pair_state, pair_mask, ln_z_layer[1], w_ab_layer[1], w_g_layer[1], ln_x_layer[1], w_o_layer[1], False)
        return pair_state, None

    pair_out, _ = lax.scan(one_layer, pair_act, (ln_z, w_ab, w_g, ln_x, w_o))
    return pair_out
```

```python
import functools

import jax
import jax.numpy as jnp
from jax import lax
from jax.experimental import pallas as pl
from jax.experimental.pallas import tpu as pltpu
from jax.sharding import PartitionSpec as P

LN_EPS = 1e-5
LANES = 128
GROUPS = 4
TILES = 3
MESH = pl.DeviceIdType.MESH


def lane_iota(shape):
    return lax.broadcasted_iota(jnp.int32, shape, len(shape) - 1)


def pack_tiles(blocks, cols):
    part = LANES - cols
    lane = lane_iota(blocks[0].shape)
    return [jnp.where(lane < cols, blocks[t], pltpu.roll(blocks[3], cols - part * t, 1)) for t in range(TILES)]


def last_group(tiles, cols):
    part = LANES - cols
    lane = lane_iota(tiles[0].shape)
    moved = [pltpu.roll(tiles[t], part * (t + 1), 1) for t in range(TILES)]
    return jnp.where(lane < part, moved[0], jnp.where(lane < 2 * part, moved[1], moved[2]))


def norm_sublanes(values, gain, bias):
    mean = jnp.mean(values, axis=0, keepdims=True)
    centered = values - mean
    variance = jnp.mean(centered * centered, axis=0, keepdims=True)
    return (centered * lax.rsqrt(variance + LN_EPS) * gain + bias).astype(jnp.bfloat16)


def kernel(n_dap, n_dap2, n_updates, z_ref, m_ref, w_ref, ln_ref, out_ref, zt, zn, stage, send, recv, xs, xr, lnb,
           send_sem, recv_sem, xsend_sem, xrecv_sem):
    rows, cols, width = z_ref.shape
    n_all = n_dap * n_dap2
    pitch = stage.shape[2] // n_all
    per = width // GROUPS
    full = rows * n_dap
    my_p, my_q = lax.axis_index("dap"), lax.axis_index("dap2")
    me = my_p * n_dap2 + my_q

    barrier = pltpu.get_barrier_semaphore()

    @pl.loop(1, n_all)
    def _(off):
        peer = lax.rem(me + off, n_all)
        pl.semaphore_signal(barrier, inc=1, device_id={"dap": peer // n_dap2, "dap2": lax.rem(peer, n_dap2)}, device_id_type=MESH)

    pl.semaphore_wait(barrier, n_all - 1)

    def load_params(update):
        for k in range(4):
            lnb[k] = jnp.broadcast_to(ln_ref[update, :, k:k + 1], (width, LANES))

    def project_row(i, update):
        n_row = norm_sublanes(zt[i], lnb[0], lnb[1])
        zn[i] = n_row
        keep = m_ref[pl.ds(i, 1), :]
        a_blocks, b_blocks = [], []
        for g in range(GROUPS):
            q = jnp.dot(w_ref[update, g * 4 * per:(g + 1) * 4 * per, :], n_row, preferred_element_type=jnp.float32)
            a_blocks.append(jax.nn.sigmoid(q[per:2 * per]) * q[:per] * keep)
            b_blocks.append(jax.nn.sigmoid(q[3 * per:]) * q[2 * per:3 * per] * keep)
        for side, blocks in enumerate((a_blocks, b_blocks)):
            for t, tile in enumerate(pack_tiles(blocks, cols)):
                stage[side, t, pl.ds(i, n_all, stride=pitch), :] = tile

    def finish_row(i, update):
        tiles = [xr[t, pl.ds(i, n_all, stride=pitch), :] for t in range(TILES)]
        x_row = jnp.concatenate([*tiles, last_group(tiles, cols)], axis=0)
        x_norm = norm_sublanes(x_row, lnb[2], lnb[3])
        gate = jnp.dot(w_ref[update, 4 * width:5 * width, :], zn[i], preferred_element_type=jnp.float32)
        value = jnp.dot(w_ref[update, 5 * width:6 * width, :], x_norm, preferred_element_type=jnp.float32)
        zt[i] = zt[i] + jax.nn.sigmoid(gate) * value

    def pack_sends():
        @pl.loop(0, n_all)
        def _(g):
            for side in range(2):
                for t in range(TILES):
                    send[g, side, t] = stage[side, t, pl.ds(pl.multiple_of(g * pitch, 8), rows), :].astype(jnp.bfloat16)

    def ab_slot(parity):
        return recv.at[parity, :, :, pl.ds(pl.multiple_of(my_p * rows, 16), rows), pl.ds(pl.multiple_of(my_q * LANES, LANES), LANES)]

    def x_slots(p, q):
        return xs.at[q, :, pl.ds(pl.multiple_of(p * rows, 8), rows), :], xr.at[:, pl.ds(pl.multiple_of(me * pitch, 8), rows), :]

    def ab_copy(peer, parity):
        return pltpu.make_async_remote_copy(
            src_ref=send.at[peer],
            dst_ref=ab_slot(parity),
            send_sem=send_sem, recv_sem=recv_sem.at[parity],
            device_id={"dap": peer // n_dap2, "dap2": lax.rem(peer, n_dap2)}, device_id_type=MESH)

    def x_copy(peer):
        p, q = peer // n_dap2, lax.rem(peer, n_dap2)
        src, dst = x_slots(p, q)
        return pltpu.make_async_remote_copy(
            src_ref=src,
            dst_ref=dst,
            send_sem=xsend_sem, recv_sem=xrecv_sem,
            device_id={"dap": p, "dap2": q}, device_id_type=MESH)

    def wait_bytes(ref, sem):
        pltpu.make_async_copy(ref, ref, sem).wait()

    def exchange(parity):
        kept = pltpu.make_async_copy(send.at[me], ab_slot(parity), recv_sem.at[parity])
        kept.start()

        @pl.loop(1, n_all)
        def _(off):
            ab_copy(lax.rem(me + off, n_all), parity).start()

        wait_bytes(recv.at[parity], recv_sem.at[parity])

    def store_x(q, row, blocks):
        for t, tile in enumerate(pack_tiles(blocks, cols)):
            xs[q, t, pl.ds(row, cols), :] = tile

    def contract_outgoing(parity):
        @pl.loop(0, full // cols)
        def _(chunk):
            row = pl.multiple_of(chunk * cols, 16)
            lane = lax.rem(lane_iota((cols, n_dap2 * LANES)), LANES)
            a_tiles = [recv[parity, 0, t, pl.ds(row, cols), :] for t in range(TILES)]
            zero = jnp.zeros_like(a_tiles[0])
            low = [jnp.where(lane < cols, a, zero) for a in a_tiles]
            high = [jnp.where(lane < cols, zero, a) for a in a_tiles]

            @pl.loop(0, n_dap2)
            def _(q):
                b_tiles = [recv[parity, 1, t, pl.ds(pl.multiple_of(q * cols, 16), cols), :] for t in range(TILES)]

                def dot(a, b):
                    x = lax.dot_general(a, b, (((1,), (1,)), ((), ())), preferred_element_type=jnp.float32)
                    return jnp.concatenate([x, jnp.zeros((cols, LANES - cols), jnp.float32)], axis=1)

                blocks = [dot(low[t], b_tiles[t]) for t in range(TILES)]
                blocks.append(dot(high[0], b_tiles[0]) + dot(high[1], b_tiles[1]) + dot(high[2], b_tiles[2]))
                store_x(q, row, blocks)

    def contract_incoming(parity):
        def tiles_of(side, q):
            lanes = pl.ds(pl.multiple_of(q * LANES, LANES), LANES)
            tiles = [recv[parity, side, t, :, lanes] for t in range(TILES)]
            fourth = last_group([tile.astype(jnp.float32) for tile in tiles], cols).astype(jnp.bfloat16)
            return [*tiles, fourth]

        @pl.loop(0, n_dap2)
        def _(qi):
            a_all = [a.T[:cols] for a in tiles_of(0, qi)]

            @pl.loop(0, n_dap2)
            def _(qj):
                blocks = [jnp.dot(a, b, preferred_element_type=jnp.float32) for a, b in zip(a_all, tiles_of(1, qj))]
                store_x(qj, pl.multiple_of(qi * cols, 8), blocks)

    def send_x():
        kept = pltpu.make_async_copy(*x_slots(my_p, my_q), xrecv_sem)
        kept.start()

        @pl.loop(1, n_all)
        def _(off):
            x_copy(lax.rem(me + off, n_all)).start()

    def one_update(update, parity, contract, last):
        pack_sends()
        exchange(parity)
        contract(parity)
        wait_bytes(send.at[pl.ds(0, n_all - 1)], send_sem)
        send_x()
        wait_bytes(xs, xrecv_sem)
        wait_bytes(xr.at[:, pl.ds(0, (n_all - 1) * rows), :], xsend_sem)

        @pl.loop(0, rows)
        def _(i):
            finish_row(i, update)

        load_params(jnp.minimum(update + 1, n_updates - 1))

        @pl.loop(0, rows)
        def _(i):
            project_row(i, jnp.minimum(update + 1, n_updates - 1))

    @pl.loop(0, rows)
    def _(i):
        zt[i] = jnp.zeros((width, LANES), jnp.float32)
        zt[i, :, :cols] = z_ref[i].T

    load_params(0)

    @pl.loop(0, rows)
    def _(i):
        project_row(i, 0)

    @pl.loop(0, n_updates // 2)
    def _(layer):
        one_update(2 * layer, 0, contract_outgoing, False)
        one_update(2 * layer + 1, 1, contract_incoming, False)

    @pl.loop(0, rows)
    def _(i):
        out_ref[i] = zt[i].T[:cols]


def solution(mesh):
    n_dap, n_dap2 = mesh.shape["dap"], mesh.shape["dap2"]
    n_all = n_dap * n_dap2
    pair_spec = P(("data", "dap"), "dap2", None)
    mask_spec = P(("data", "dap"), "dap2")

    def local_stack(pair_act, pair_mask, ln_z, w_ab, w_g, ln_x, w_o):
        rows, cols, width = pair_act.shape
        n_updates = w_o.shape[0] * w_o.shape[1]
        per = width // GROUPS
        full = rows * n_dap
        pitch = rows + 8
        mask = jnp.pad(pair_mask.astype(jnp.float32), ((0, 0), (0, LANES - cols)))
        w_ab = w_ab.reshape(n_updates, width, 4, GROUPS, per).transpose(0, 3, 2, 4, 1).reshape(n_updates, 4 * width, width)
        w_g = w_g.reshape(n_updates, width, width).transpose(0, 2, 1)
        w_o = w_o.reshape(n_updates, width, width).transpose(0, 2, 1)
        weights = jnp.concatenate([w_ab, w_g, w_o], axis=1)
        norms = jnp.concatenate([ln_z, ln_x], axis=2).reshape(n_updates, 4, width).transpose(0, 2, 1).astype(jnp.float32)
        vmem = pl.BlockSpec(memory_space=pltpu.VMEM)
        return pl.pallas_call(
            functools.partial(kernel, n_dap, n_dap2, n_updates),
            out_shape=jax.ShapeDtypeStruct((rows, cols, width), jnp.float32),
            in_specs=[vmem] * 4,
            out_specs=vmem,
            scratch_shapes=[
                pltpu.VMEM((rows, width, LANES), jnp.float32),
                pltpu.VMEM((rows, width, LANES), jnp.bfloat16),
                pltpu.VMEM((2, TILES, n_all * pitch, LANES), jnp.float32),
                pltpu.VMEM((n_all, 2, TILES, rows, LANES), jnp.bfloat16),
                pltpu.VMEM((2, 2, TILES, full, n_dap2 * LANES), jnp.bfloat16),
                pltpu.VMEM((n_dap2, TILES, full, LANES), jnp.float32),
                pltpu.VMEM((TILES, n_all * pitch, LANES), jnp.float32),
                pltpu.VMEM((4, width, LANES), jnp.float32),
                pltpu.SemaphoreType.DMA,
                pltpu.SemaphoreType.DMA((2,)),
                pltpu.SemaphoreType.DMA,
                pltpu.SemaphoreType.DMA,
            ],
            compiler_params=pltpu.CompilerParams(collective_id=0, has_side_effects=True, vmem_limit_bytes=60 * 1024 * 1024),
            name="triangle_stack",
        )(pair_act, mask, weights, norms)

    return jax.shard_map(local_stack, mesh=mesh, in_specs=(pair_spec, mask_spec, P(), P(), P(), P(), P()), out_specs=pair_spec, check_vma=False)
```

```python
import functools

import jax
import jax.numpy as jnp
from jax import lax
from jax.experimental import pallas as pl
from jax.experimental.pallas import tpu as pltpu
from jax.sharding import PartitionSpec as P

LN_EPS = 1e-5
LANES = 128
GROUPS = 4
TILES = 3
CHUNK = 16
UNROLL = 2
MESH = pl.DeviceIdType.MESH


def lane_iota(shape):
    return lax.broadcasted_iota(jnp.int32, shape, len(shape) - 1)


def pack_tiles(blocks, cols):
    part = LANES - cols
    lane = lane_iota(blocks[0].shape)
    return [jnp.where(lane < cols, blocks[t], pltpu.roll(blocks[3], cols - part * t, 1)) for t in range(TILES)]


def last_group(tiles, cols):
    part = LANES - cols
    lane = lane_iota(tiles[0].shape)
    moved = [pltpu.roll(tiles[t], part * (t + 1), 1) for t in range(TILES)]
    return jnp.where(lane < part, moved[0], jnp.where(lane < 2 * part, moved[1], moved[2]))


def norm_sublanes(values, gain, bias):
    mean = jnp.mean(values, axis=0, keepdims=True)
    centered = values - mean
    variance = jnp.mean(centered * centered, axis=0, keepdims=True)
    return (centered * lax.rsqrt(variance + LN_EPS) * gain + bias).astype(jnp.bfloat16)


def kernel(n_dap, n_dap2, n_updates, z_ref, m_ref, w_ref, ln_ref, out_ref, zt, zn, stage, send, recv, at, bl, xs, xr, lnb,
           send_sem, recv_sem, xsend_sem, xrecv_sem):
    rows, cols, width = z_ref.shape
    n_all = n_dap * n_dap2
    pitch, stage_pitch = xr.shape[1] // n_all, stage.shape[2] // n_all
    per = width // GROUPS
    full = rows * n_dap
    n_chunks = rows // CHUNK
    my_p, my_q = lax.axis_index("dap"), lax.axis_index("dap2")
    me = my_p * n_dap2 + my_q

    barrier = pltpu.get_barrier_semaphore()

    @pl.loop(1, n_all)
    def _(off):
        peer = lax.rem(me + off, n_all)
        pl.semaphore_signal(barrier, inc=1, device_id={"dap": peer // n_dap2, "dap2": lax.rem(peer, n_dap2)}, device_id_type=MESH)

    def load_params(first, update):
        for k in (first, first + 1):
            lnb[k] = jnp.broadcast_to(ln_ref[update, :, k:k + 1], (width, LANES))

    def project_rows(indices, local, states, update):
        normed = [norm_sublanes(state, lnb[0], lnb[1]) for state in states]
        for i, n_row in zip(indices, normed):
            zn[i] = n_row
        keeps = [m_ref[pl.ds(i, 1), :] for i in indices]
        blocks = [([], []) for _ in indices]
        for g in range(GROUPS):
            weight = w_ref[update, g * 4 * per:(g + 1) * 4 * per, :]
            for keep, n_row, (a_blocks, b_blocks) in zip(keeps, normed, blocks):
                q = jnp.dot(weight, n_row, preferred_element_type=jnp.float32)
                a_blocks.append(jax.nn.sigmoid(q[per:2 * per]) * q[:per] * keep)
                b_blocks.append(jax.nn.sigmoid(q[3 * per:]) * q[2 * per:3 * per] * keep)
        for k, sides in zip(local, blocks):
            for side in range(2):
                for t, tile in enumerate(pack_tiles(sides[side], cols)):
                    stage[side, t, pl.ds(k, n_all, stride=stage_pitch), :] = tile

    def finish_rows(indices, update):
        tiles = [[xr[t, pl.ds(i, n_all, stride=pitch), :] for t in range(TILES)] for i in indices]
        x_rows = [jnp.concatenate([*tile, last_group(tile, cols)], axis=0) for tile in tiles]
        gates = [jnp.dot(w_ref[update, 4 * width:5 * width, :], zn[i], preferred_element_type=jnp.float32) for i in indices]
        normed = [norm_sublanes(x_row, lnb[2], lnb[3]) for x_row in x_rows]
        values = [jnp.dot(w_ref[update, 5 * width:6 * width, :], x_norm, preferred_element_type=jnp.float32) for x_norm in normed]
        return [zt[i] + jax.nn.sigmoid(gate) * value for i, gate, value in zip(indices, gates, values)]

    def for_rows(r, body):
        @pl.loop(0, CHUNK // UNROLL)
        def _(k):
            local = [k * UNROLL + s for s in range(UNROLL)]
            body([r * CHUNK + i for i in local], local)

    def coords(peer):
        return {"dap": peer // n_dap2, "dap2": lax.rem(peer, n_dap2)}

    def chunk_rows(p, r):
        return pl.ds(pl.multiple_of(p * rows + r * CHUNK, CHUNK), CHUNK)

    def wait_bytes(ref, sem):
        pltpu.make_async_copy(ref, ref, sem).wait()

    def send_chunk(r, parity):
        @pl.loop(0, n_all)
        def _(g):
            for side in range(2):
                for t in range(TILES):
                    send[r, g, side, t] = stage[side, t, pl.ds(pl.multiple_of(g * stage_pitch, 8), CHUNK), :].astype(jnp.bfloat16)

        slot = recv.at[parity, :, :, chunk_rows(my_p, r), pl.ds(pl.multiple_of(my_q * LANES, LANES), LANES)]
        pltpu.make_async_copy(send.at[r, me], slot, recv_sem.at[parity, r]).start()

        @pl.loop(1, n_all)
        def _(off):
            peer = lax.rem(me + off, n_all)
            pltpu.make_async_remote_copy(src_ref=send.at[r, peer], dst_ref=slot, send_sem=send_sem.at[r], recv_sem=recv_sem.at[parity, r],
                                         device_id=coords(peer), device_id_type=MESH).start()

    def send_x(r):
        def slots(p, q):
            return (xs.at[q, :, pl.ds(pl.multiple_of((r * n_dap + p) * CHUNK, CHUNK), CHUNK), :],
                    xr.at[:, pl.ds(pl.multiple_of(me * pitch + r * CHUNK, 8), CHUNK), :])

        pltpu.make_async_copy(*slots(my_p, my_q), xrecv_sem.at[r]).start()

        @pl.loop(1, n_all)
        def _(off):
            peer = lax.rem(me + off, n_all)
            src, dst = slots(peer // n_dap2, lax.rem(peer, n_dap2))
            pltpu.make_async_remote_copy(src_ref=src, dst_ref=dst, send_sem=xsend_sem.at[r], recv_sem=xrecv_sem.at[r],
                                         device_id=coords(peer), device_id_type=MESH).start()

    def contract_chunk(r, q, blocks):
        for t, tile in enumerate(pack_tiles(blocks, cols)):
            xs[q, t, pl.ds(pl.multiple_of(r * n_dap * CHUNK, CHUNK), n_dap * CHUNK), :] = tile

    def gather_rows(ref, r):
        return jnp.concatenate([ref[chunk_rows(p, r), :] for p in range(n_dap)], axis=0)

    def contract_outgoing(parity):
        @pl.loop(0, n_chunks)
        def _(r):
            lane = lax.rem(lane_iota((n_dap * CHUNK, n_dap2 * LANES)), LANES)
            a_tiles = [gather_rows(recv.at[parity, 0, t], r) for t in range(TILES)]
            zero = jnp.zeros_like(a_tiles[0])
            low = [jnp.where(lane < cols, a, zero) for a in a_tiles]
            high = [jnp.where(lane < cols, zero, a) for a in a_tiles]

            @pl.loop(0, n_dap2)
            def _(q):
                b_tiles = [recv[parity, 1, t, pl.ds(pl.multiple_of(q * cols, 16), cols), :] for t in range(TILES)]

                def dot(a, b):
                    x = lax.dot_general(a, b, (((1,), (1,)), ((), ())), preferred_element_type=jnp.float32)
                    return jnp.concatenate([x, jnp.zeros((x.shape[0], LANES - cols), jnp.float32)], axis=1)

                blocks = [dot(low[t], b_tiles[t]) for t in range(TILES)]
                blocks.append(dot(high[0], b_tiles[0]) + dot(high[1], b_tiles[1]) + dot(high[2], b_tiles[2]))
                contract_chunk(r, q, blocks)

            send_x(r)

    def contract_incoming(parity):
        @pl.loop(0, n_dap2)
        def _(q):
            lanes = pl.ds(pl.multiple_of(q * LANES, LANES), LANES)
            for side in range(2):
                tiles = [recv[parity, side, t, :, lanes] for t in range(TILES)]
                last = last_group([tile.astype(jnp.float32) for tile in tiles], cols).astype(jnp.bfloat16)
                if side:
                    bl[:, lanes] = last
                else:
                    for g, tile in enumerate([*tiles, last]):
                        at[g, pl.ds(pl.multiple_of(q * cols, 16), cols), :] = tile.T[:cols]

        @pl.loop(0, n_chunks)
        def _(r):
            a_all = [gather_rows(at.at[g], r) for g in range(GROUPS)]

            @pl.loop(0, n_dap2)
            def _(q):
                lanes = pl.ds(pl.multiple_of(q * LANES, LANES), LANES)
                b_all = [*[recv[parity, 1, t, :, lanes] for t in range(TILES)], bl[:, lanes]]
                contract_chunk(r, q, [jnp.dot(a, b, preferred_element_type=jnp.float32) for a, b in zip(a_all, b_all)])

            send_x(r)

    def exchange(update, parity, contract, more):
        for r in range(n_chunks):
            wait_bytes(recv.at[parity, :, :, pl.ds(0, n_dap * CHUNK), :], recv_sem.at[parity, r])
        contract(parity)
        for r in range(n_chunks):
            wait_bytes(send.at[r, pl.ds(0, n_all - 1)], send_sem.at[r])
        load_params(2, update)

        def arrived(r):
            wait_bytes(xs.at[:, :, pl.ds(0, n_dap * CHUNK), :], xrecv_sem.at[r])

        def go_on():
            load_params(0, update + 1)

            @pl.loop(0, n_chunks)
            def _(r):
                arrived(r)

                def body(indices, local):
                    states = finish_rows(indices, update)
                    for i, state in zip(indices, states):
                        zt[i] = state
                    project_rows(indices, local, states, update + 1)

                for_rows(r, body)
                send_chunk(r, 1 - parity)

        def end():
            @pl.loop(0, n_chunks)
            def _(r):
                arrived(r)

                def body(indices, local):
                    for i, state in zip(indices, finish_rows(indices, update)):
                        out_ref[i] = state.T[:cols]

                for_rows(r, body)

        if more is None:
            go_on()
        else:
            pl.when(more)(go_on)
            pl.when(jnp.logical_not(more))(end)
        for r in range(n_chunks):
            wait_bytes(xr.at[:, pl.ds(0, (n_all - 1) * CHUNK), :], xsend_sem.at[r])

    load_params(0, 0)
    pl.semaphore_wait(barrier, n_all - 1)

    @pl.loop(0, n_chunks)
    def _(r):
        def body(indices, local):
            states = [jnp.concatenate([z_ref[i].T, jnp.zeros((width, LANES - cols), jnp.float32)], axis=1) for i in indices]
            for i, state in zip(indices, states):
                zt[i] = state
            project_rows(indices, local, states, 0)

        for_rows(r, body)
        send_chunk(r, 0)

    @pl.loop(0, n_updates // 2)
    def _(layer):
        exchange(2 * layer, 0, contract_outgoing, None)
        exchange(2 * layer + 1, 1, contract_incoming, layer < n_updates // 2 - 1)


def solution(mesh):
    n_dap, n_dap2 = mesh.shape["dap"], mesh.shape["dap2"]
    n_all = n_dap * n_dap2
    pair_spec = P(("data", "dap"), "dap2", None)
    mask_spec = P(("data", "dap"), "dap2")

    def local_stack(pair_act, pair_mask, ln_z, w_ab, w_g, ln_x, w_o):
        rows, cols, width = pair_act.shape
        n_updates = w_o.shape[0] * w_o.shape[1]
        per = width // GROUPS
        full = rows * n_dap
        pitch, stage_pitch = rows + 8, CHUNK + 8
        n_chunks = rows // CHUNK
        mask = jnp.pad(pair_mask.astype(jnp.float32), ((0, 0), (0, LANES - cols)))
        w_ab = w_ab.reshape(n_updates, width, 4, GROUPS, per).transpose(0, 3, 2, 4, 1).reshape(n_updates, 4 * width, width)
        w_g = w_g.reshape(n_updates, width, width).transpose(0, 2, 1)
        w_o = w_o.reshape(n_updates, width, width).transpose(0, 2, 1)
        weights = jnp.concatenate([w_ab, w_g, w_o], axis=1)
        norms = jnp.concatenate([ln_z, ln_x], axis=2).reshape(n_updates, 4, width).transpose(0, 2, 1).astype(jnp.float32)
        vmem = pl.BlockSpec(memory_space=pltpu.VMEM)
        return pl.pallas_call(
            functools.partial(kernel, n_dap, n_dap2, n_updates),
            out_shape=jax.ShapeDtypeStruct((rows, cols, width), jnp.float32),
            in_specs=[vmem] * 4,
            out_specs=vmem,
            scratch_shapes=[
                pltpu.VMEM((rows, width, LANES), jnp.float32),
                pltpu.VMEM((rows, width, LANES), jnp.bfloat16),
                pltpu.VMEM((2, TILES, n_all * stage_pitch, LANES), jnp.float32),
                pltpu.VMEM((n_chunks, n_all, 2, TILES, CHUNK, LANES), jnp.bfloat16),
                pltpu.VMEM((2, 2, TILES, full, n_dap2 * LANES), jnp.bfloat16),
                pltpu.VMEM((GROUPS, full, full), jnp.bfloat16),
                pltpu.VMEM((full, n_dap2 * LANES), jnp.bfloat16),
                pltpu.VMEM((n_dap2, TILES, full, LANES), jnp.float32),
                pltpu.VMEM((TILES, n_all * pitch, LANES), jnp.float32),
                pltpu.VMEM((4, width, LANES), jnp.float32),
                pltpu.SemaphoreType.DMA((n_chunks,)),
                pltpu.SemaphoreType.DMA((2, n_chunks)),
                pltpu.SemaphoreType.DMA((n_chunks,)),
                pltpu.SemaphoreType.DMA((n_chunks,)),
            ],
            compiler_params=pltpu.CompilerParams(collective_id=0, has_side_effects=True, vmem_limit_bytes=60 * 1024 * 1024),
            name="triangle_stack",
        )(pair_act, mask, weights, norms)

    return jax.shard_map(local_stack, mesh=mesh, in_specs=(pair_spec, mask_spec, P(), P(), P(), P(), P()), out_specs=pair_spec, check_vma=False)
```

```python
import functools

import jax
import jax.numpy as jnp
from jax import lax
from jax.experimental import pallas as pl
from jax.experimental.pallas import tpu as pltpu
from jax.sharding import PartitionSpec as P

LN_EPS = 1e-5
LANES = 128
GROUPS = 4
TILES = 3
CHUNK = 16
UNROLL = 2
MESH = pl.DeviceIdType.MESH


def lane_iota(shape):
    return lax.broadcasted_iota(jnp.int32, shape, len(shape) - 1)


def pack_tiles(blocks, cols):
    part = LANES - cols
    lane = lane_iota(blocks[0].shape)
    return [jnp.where(lane < cols, blocks[t], pltpu.roll(blocks[3], cols - part * t, 1)) for t in range(TILES)]


def last_group(tiles, cols):
    part = LANES - cols
    lane = lane_iota(tiles[0].shape)
    moved = [pltpu.roll(tiles[t], part * (t + 1), 1) for t in range(TILES)]
    return jnp.where(lane < part, moved[0], jnp.where(lane < 2 * part, moved[1], moved[2]))


def pack_columns(blocks, cols):
    part = LANES - cols
    lane = lane_iota(blocks[0].shape)
    tiles = []
    for t in range(TILES):
        moved = [block if g == t else pltpu.roll(block, part * (g - t) % LANES, 1) for g, block in enumerate(blocks)]
        tile = moved[GROUPS - 1]
        for g in reversed(range(GROUPS - 1)):
            tile = jnp.where(lane < part * (g + 1), moved[g], tile)
        tiles.append(tile)
    return tiles


def norm_sublanes(values, gain, bias):
    mean = jnp.mean(values, axis=0, keepdims=True)
    centered = values - mean
    variance = jnp.mean(centered * centered, axis=0, keepdims=True)
    return (centered * lax.rsqrt(variance + LN_EPS) * gain + bias).astype(jnp.bfloat16)


def kernel(n_dap, n_dap2, n_updates, z_ref, m_ref, w_ref, ln_ref, out_ref, zt, zn, stage, send, recv, bl, xs, xr, lnb,
           send_sem, recv_sem, xsend_sem, xrecv_sem):
    rows, cols, width = z_ref.shape
    n_all = n_dap * n_dap2
    pitch, stage_pitch = xr.shape[1] // n_all, stage.shape[1] // n_all
    per = width // GROUPS
    full = rows * n_dap
    n_chunks = rows // CHUNK
    halves = cols // rows
    my_p, my_q = lax.axis_index("dap"), lax.axis_index("dap2")
    me = my_p * n_dap2 + my_q

    barrier = pltpu.get_barrier_semaphore()

    @pl.loop(1, n_all)
    def _(off):
        peer = lax.rem(me + off, n_all)
        pl.semaphore_signal(barrier, inc=1, device_id={"dap": peer // n_dap2, "dap2": lax.rem(peer, n_dap2)}, device_id_type=MESH)

    def load_params(first, update):
        for k in (first, first + 1):
            lnb[k] = jnp.broadcast_to(ln_ref[update, :, k:k + 1], (width, LANES))

    def project_rows(indices, local, states, update, incoming):
        normed = [norm_sublanes(state, lnb[0], lnb[1]) for state in states]
        for i, n_row in zip(indices, normed):
            zn[i] = n_row
        keeps = [m_ref[pl.ds(i, 1), :] for i in indices]
        blocks = [([], []) for _ in indices]
        for g in range(GROUPS):
            weight = w_ref[update, g * 4 * per:(g + 1) * 4 * per, :]
            for keep, n_row, (a_blocks, b_blocks) in zip(keeps, normed, blocks):
                q = jnp.dot(weight, n_row, preferred_element_type=jnp.float32)
                a_blocks.append(jax.nn.sigmoid(q[per:2 * per]) * q[:per] * keep)
                b_blocks.append(jax.nn.sigmoid(q[3 * per:]) * q[2 * per:3 * per] * keep)
        for k, sides in zip(local, blocks):
            a_pack = pack_columns if incoming else pack_tiles
            for t, tile in enumerate([*pack_tiles(sides[1], cols), *a_pack(sides[0], cols)]):
                stage[t, pl.ds(k, n_all, stride=stage_pitch), :] = tile

    def finish_rows(indices, update):
        tiles = [[xr[t, pl.ds(i, n_all, stride=pitch), :] for t in range(TILES)] for i in indices]
        x_rows = [jnp.concatenate([*tile, last_group(tile, cols)], axis=0) for tile in tiles]
        gates = [jnp.dot(w_ref[update, 4 * width:5 * width, :], zn[i], preferred_element_type=jnp.float32) for i in indices]
        normed = [norm_sublanes(x_row, lnb[2], lnb[3]) for x_row in x_rows]
        values = [jnp.dot(w_ref[update, 5 * width:6 * width, :], x_norm, preferred_element_type=jnp.float32) for x_norm in normed]
        return [zt[i] + jax.nn.sigmoid(gate) * value for i, gate, value in zip(indices, gates, values)]

    def for_rows(r, body):
        @pl.loop(0, CHUNK // UNROLL)
        def _(k):
            local = [k * UNROLL + s for s in range(UNROLL)]
            body([r * CHUNK + i for i in local], local)

    def coords(peer):
        return {"dap": peer // n_dap2, "dap2": lax.rem(peer, n_dap2)}

    def chunk_rows(p, r):
        return pl.ds(pl.multiple_of(p * rows + r * CHUNK, CHUNK), CHUNK)

    def wait_bytes(ref, sem):
        pltpu.make_async_copy(ref, ref, sem).wait()

    def first_tiles(parity):
        return TILES + parity

    def send_part(parity, part, tiles, first_row, n_rows):
        row = pl.multiple_of(my_p * rows + first_row, CHUNK)
        slot = recv.at[parity, tiles, pl.ds(row, n_rows), pl.ds(pl.multiple_of(my_q * LANES, LANES), LANES)]
        here = pl.ds(pl.multiple_of(first_row, CHUNK), n_rows)
        pltpu.make_async_copy(send.at[me, tiles, here], slot, recv_sem.at[parity, part]).start()

        @pl.loop(1, n_all)
        def _(off):
            peer = lax.rem(me + off, n_all)
            pltpu.make_async_remote_copy(src_ref=send.at[peer, tiles, here], dst_ref=slot, send_sem=send_sem.at[part],
                                         recv_sem=recv_sem.at[parity, part], device_id=coords(peer), device_id_type=MESH).start()

    def pack_chunk(r):
        @pl.loop(0, n_all)
        def _(g):
            for t in range(2 * TILES):
                send[g, t, pl.ds(pl.multiple_of(r * CHUNK, CHUNK), CHUNK)] = stage[t, pl.ds(pl.multiple_of(g * stage_pitch, 8), CHUNK), :].astype(jnp.bfloat16)

    def send_chunk(r, parity):
        pack_chunk(r)
        if r == 0:
            send_part(parity, 0, pl.ds(0, 2 * TILES), 0, CHUNK)
        else:
            send_part(parity, r, pl.ds(0, first_tiles(parity)), r * CHUNK, CHUNK)
        if r == n_chunks - 1:
            send_part(parity, n_chunks, pl.ds(first_tiles(parity), 2 * TILES - first_tiles(parity)), CHUNK, rows - CHUNK)

    def part_shape(parity, part):
        if part == 0:
            return 2 * TILES, CHUNK
        if part < n_chunks:
            return first_tiles(parity), CHUNK
        return 2 * TILES - first_tiles(parity), rows - CHUNK

    def wait_received(parity, part):
        tiles, n_rows = part_shape(parity, part)
        wait_bytes(recv.at[parity, pl.ds(0, tiles), pl.ds(0, n_dap * n_rows), :], recv_sem.at[parity, part])

    def wait_sent(parity, part):
        tiles, n_rows = part_shape(parity, part)
        wait_bytes(send.at[pl.ds(0, n_all - 1), pl.ds(0, tiles), pl.ds(0, n_rows)], send_sem.at[part])

    def send_x(r):
        def slots(p, q):
            return (xs.at[q, :, pl.ds(pl.multiple_of((r * n_dap + p) * CHUNK, CHUNK), CHUNK), :],
                    xr.at[:, pl.ds(pl.multiple_of(me * pitch + r * CHUNK, 8), CHUNK), :])

        pltpu.make_async_copy(*slots(my_p, my_q), xrecv_sem.at[r]).start()

        @pl.loop(1, n_all)
        def _(off):
            peer = lax.rem(me + off, n_all)
            src, dst = slots(peer // n_dap2, lax.rem(peer, n_dap2))
            pltpu.make_async_remote_copy(src_ref=src, dst_ref=dst, send_sem=xsend_sem.at[r], recv_sem=xrecv_sem.at[r],
                                         device_id=coords(peer), device_id_type=MESH).start()

    def contract_chunk(r, q, blocks):
        for t, tile in enumerate(pack_tiles(blocks, cols)):
            xs[q, t, pl.ds(pl.multiple_of(r * n_dap * CHUNK, CHUNK), n_dap * CHUNK), :] = tile

    def gather_rows(ref, r):
        return jnp.concatenate([ref[chunk_rows(p, r), :] for p in range(n_dap)], axis=0)

    def contract_outgoing(parity):
        def chunk(r):
            lane = lax.rem(lane_iota((n_dap * CHUNK, n_dap2 * LANES)), LANES)
            a_tiles = [gather_rows(recv.at[parity, TILES + t], r) for t in range(TILES)]
            zero = jnp.zeros_like(a_tiles[0])
            low = [jnp.where(lane < cols, a, zero) for a in a_tiles]
            high = [jnp.where(lane < cols, zero, a) for a in a_tiles]

            @pl.loop(0, n_dap2)
            def _(q):
                b_tiles = [jnp.concatenate([recv[parity, t, chunk_rows(q * halves + h, s), :] for s in range(n_chunks) for h in range(halves)], axis=0)
                           for t in range(TILES)]

                def dot(a, b):
                    x = lax.dot_general(a, b, (((1,), (1,)), ((), ())), preferred_element_type=jnp.float32)
                    return jnp.concatenate([x, jnp.zeros((x.shape[0], LANES - cols), jnp.float32)], axis=1)

                blocks = [dot(low[t], b_tiles[t]) for t in range(TILES)]
                blocks.append(dot(high[0], b_tiles[0]) + dot(high[1], b_tiles[1]) + dot(high[2], b_tiles[2]))
                contract_chunk(r, q, blocks)

            send_x(r)

        for r in range(n_chunks):
            wait_received(parity, r)
        chunk(0)
        wait_received(parity, n_chunks)
        pl.loop(1, n_chunks)(chunk)

    def contract_incoming(parity):
        def chunk(r):
            part = LANES - cols
            turned = [recv[parity, TILES + r, :, q * LANES:(q + 1) * LANES].T for q in range(n_dap2)]
            a_all = [jnp.concatenate([a[g * part:(g + 1) * part] for a in turned], axis=0) for g in range(GROUPS)]

            @pl.loop(0, n_dap2)
            def _(q):
                lanes = pl.ds(pl.multiple_of(q * LANES, LANES), LANES)
                b_all = [*[recv[parity, t, :, lanes] for t in range(TILES)], bl[:, lanes]]
                contract_chunk(r, q, [jnp.dot(a, b, preferred_element_type=jnp.float32) for a, b in zip(a_all, b_all)])

            send_x(r)

        for r in range(n_chunks):
            wait_received(parity, r)

            @pl.loop(0, n_dap)
            def _(p):
                here = chunk_rows(p, r)
                for q in range(n_dap2):
                    lanes = slice(q * LANES, (q + 1) * LANES)
                    tiles = [recv[parity, t, here, lanes].astype(jnp.float32) for t in range(TILES)]
                    bl[here, lanes] = last_group(tiles, cols).astype(jnp.bfloat16)

        chunk(0)
        wait_received(parity, n_chunks)
        pl.loop(1, n_chunks)(chunk)

    def exchange(update, parity, contract, more):
        contract(parity)
        for part in range(n_chunks + 1):
            wait_sent(parity, part)
        load_params(2, update)

        def arrived(r):
            wait_bytes(xs.at[:, :, pl.ds(0, n_dap * CHUNK), :], xrecv_sem.at[r])

        def go_on():
            load_params(0, update + 1)

            def body(indices, local):
                states = finish_rows(indices, update)
                for i, state in zip(indices, states):
                    zt[i] = state
                project_rows(indices, local, states, update + 1, incoming=parity == 0)

            for r in range(n_chunks):
                arrived(r)
                for_rows(r, body)
                send_chunk(r, 1 - parity)

        def end():
            @pl.loop(0, n_chunks)
            def _(r):
                arrived(r)

                def body(indices, local):
                    for i, state in zip(indices, finish_rows(indices, update)):
                        turned = state.T
                        for s in range(n_chunks):
                            for h in range(halves):
                                lane = (s * halves + h) * CHUNK
                                out_ref[i, h * rows + s * CHUNK:h * rows + (s + 1) * CHUNK, :] = turned[lane:lane + CHUNK]

                for_rows(r, body)

        if more is None:
            go_on()
        else:
            pl.when(more)(go_on)
            pl.when(jnp.logical_not(more))(end)
        for r in range(n_chunks):
            wait_bytes(xr.at[:, pl.ds(0, (n_all - 1) * CHUNK), :], xsend_sem.at[r])

    load_params(0, 0)
    pl.semaphore_wait(barrier, n_all - 1)

    def first(indices, local):
        def turn(i):
            order = [z_ref[i, h * rows + s * CHUNK:h * rows + (s + 1) * CHUNK, :] for s in range(n_chunks) for h in range(halves)]
            return jnp.concatenate([jnp.concatenate(order, axis=0).T, jnp.zeros((width, LANES - cols), jnp.float32)], axis=1)

        states = [turn(i) for i in indices]
        for i, state in zip(indices, states):
            zt[i] = state
        project_rows(indices, local, states, 0, incoming=False)

    for r in range(n_chunks):
        for_rows(r, first)
        send_chunk(r, 0)

    @pl.loop(0, n_updates // 2)
    def _(layer):
        exchange(2 * layer, 0, contract_outgoing, None)
        exchange(2 * layer + 1, 1, contract_incoming, layer < n_updates // 2 - 1)


def solution(mesh):
    n_dap, n_dap2 = mesh.shape["dap"], mesh.shape["dap2"]
    n_all = n_dap * n_dap2
    pair_spec = P(("data", "dap"), "dap2", None)
    mask_spec = P(("data", "dap"), "dap2")

    def local_stack(pair_act, pair_mask, ln_z, w_ab, w_g, ln_x, w_o):
        rows, cols, width = pair_act.shape
        n_updates = w_o.shape[0] * w_o.shape[1]
        per = width // GROUPS
        full = rows * n_dap
        pitch, stage_pitch = rows + 8, CHUNK + 8
        n_chunks = rows // CHUNK
        mask = pair_mask.astype(jnp.float32).reshape(rows, cols // rows, rows // CHUNK, CHUNK).transpose(0, 2, 1, 3).reshape(rows, cols)
        mask = jnp.pad(mask, ((0, 0), (0, LANES - cols)))
        w_ab = w_ab.reshape(n_updates, width, 4, GROUPS, per).transpose(0, 3, 2, 4, 1).reshape(n_updates, 4 * width, width)
        w_g = w_g.reshape(n_updates, width, width).transpose(0, 2, 1)
        w_o = w_o.reshape(n_updates, width, width).transpose(0, 2, 1)
        weights = jnp.concatenate([w_ab, w_g, w_o], axis=1)
        norms = jnp.concatenate([ln_z, ln_x], axis=2).reshape(n_updates, 4, width).transpose(0, 2, 1).astype(jnp.float32)
        vmem = pl.BlockSpec(memory_space=pltpu.VMEM)
        return pl.pallas_call(
            functools.partial(kernel, n_dap, n_dap2, n_updates),
            out_shape=jax.ShapeDtypeStruct((rows, cols, width), jnp.float32),
            in_specs=[vmem] * 4,
            out_specs=vmem,
            scratch_shapes=[
                pltpu.VMEM((rows, width, LANES), jnp.float32),
                pltpu.VMEM((rows, width, LANES), jnp.bfloat16),
                pltpu.VMEM((2 * TILES, n_all * stage_pitch, LANES), jnp.float32),
                pltpu.VMEM((n_all, 2 * TILES, rows, LANES), jnp.bfloat16),
                pltpu.VMEM((2, 2 * TILES, full, n_dap2 * LANES), jnp.bfloat16),
                pltpu.VMEM((full, n_dap2 * LANES), jnp.bfloat16),
                pltpu.VMEM((n_dap2, TILES, full, LANES), jnp.float32),
                pltpu.VMEM((TILES, n_all * pitch, LANES), jnp.float32),
                pltpu.VMEM((4, width, LANES), jnp.float32),
                pltpu.SemaphoreType.DMA((n_chunks + 1,)),
                pltpu.SemaphoreType.DMA((2, n_chunks + 1)),
                pltpu.SemaphoreType.DMA((n_chunks,)),
                pltpu.SemaphoreType.DMA((n_chunks,)),
            ],
            compiler_params=pltpu.CompilerParams(collective_id=0, has_side_effects=True, vmem_limit_bytes=60 * 1024 * 1024),
            name="triangle_stack",
        )(pair_act, mask, weights, norms)

    return jax.shard_map(local_stack, mesh=mesh, in_specs=(pair_spec, mask_spec, P(), P(), P(), P(), P()), out_specs=pair_spec, check_vma=False)
```

```python
import functools

import jax
import jax.numpy as jnp
from jax import lax
from jax.experimental import pallas as pl
from jax.experimental.pallas import tpu as pltpu
from jax.sharding import PartitionSpec as P

LN_EPS = 1e-5
LANES = 128
GROUPS = 4
TILES = 3
CHUNK = 16
UNROLL = 8
MESH = pl.DeviceIdType.MESH


def lane_iota(shape):
    return lax.broadcasted_iota(jnp.int32, shape, len(shape) - 1)


def pack_tiles(blocks, cols):
    part = LANES - cols
    lane = lane_iota(blocks[0].shape)
    return [jnp.where(lane < cols, blocks[t], pltpu.roll(blocks[3], cols - part * t, 1)) for t in range(TILES)]


def last_group(tiles, cols):
    part = LANES - cols
    lane = lane_iota(tiles[0].shape)
    moved = [pltpu.roll(tiles[t], part * (t + 1), 1) for t in range(TILES)]
    return jnp.where(lane < part, moved[0], jnp.where(lane < 2 * part, moved[1], moved[2]))


def pack_columns(blocks, cols):
    part = LANES - cols
    lane = lane_iota(blocks[0].shape)
    tiles = []
    for t in range(TILES):
        moved = [block if g == t else pltpu.roll(block, part * (g - t) % LANES, 1) for g, block in enumerate(blocks)]
        tile = moved[GROUPS - 1]
        for g in reversed(range(GROUPS - 1)):
            tile = jnp.where(lane < part * (g + 1), moved[g], tile)
        tiles.append(tile)
    return tiles


def norm_sublanes(values, gain, bias):
    mean = jnp.mean(values, axis=0, keepdims=True)
    centered = values - mean
    variance = jnp.mean(centered * centered, axis=0, keepdims=True)
    return (centered * lax.rsqrt(variance + LN_EPS) * gain + bias).astype(jnp.bfloat16)


def kernel(n_dap, n_dap2, n_updates, z_ref, m_ref, w_ref, ln_ref, out_ref, zt, zn, stage, send, recv, bl, xs, xr, lnb,
           send_sem, recv_sem, xsend_sem, xrecv_sem):
    rows, cols, width = z_ref.shape
    n_all = n_dap * n_dap2
    pitch, stage_pitch = xr.shape[1] // n_all, stage.shape[1] // n_all
    per = width // GROUPS
    full = rows * n_dap
    n_chunks = rows // CHUNK
    halves = cols // rows
    my_p, my_q = lax.axis_index("dap"), lax.axis_index("dap2")
    me = my_p * n_dap2 + my_q

    barrier = pltpu.get_barrier_semaphore()

    @pl.loop(1, n_all)
    def _(off):
        peer = lax.rem(me + off, n_all)
        pl.semaphore_signal(barrier, inc=1, device_id={"dap": peer // n_dap2, "dap2": lax.rem(peer, n_dap2)}, device_id_type=MESH)

    def load_params(first, update):
        for k in (first, first + 1):
            lnb[k] = jnp.broadcast_to(ln_ref[update, :, k:k + 1], (width, LANES))

    def project_rows(indices, local, states, update, incoming):
        normed = [norm_sublanes(state, lnb[0], lnb[1]) for state in states]
        for i, n_row in zip(indices, normed):
            zn[i] = n_row
        keeps = [m_ref[pl.ds(i, 1), :] for i in indices]
        blocks = [([], []) for _ in indices]
        for g in range(GROUPS):
            weight = w_ref[update, g * 4 * per:(g + 1) * 4 * per, :]
            for keep, n_row, (a_blocks, b_blocks) in zip(keeps, normed, blocks):
                q = jnp.dot(weight, n_row, preferred_element_type=jnp.float32)
                a_blocks.append(jax.nn.sigmoid(q[per:2 * per]) * q[:per] * keep)
                b_blocks.append(jax.nn.sigmoid(q[3 * per:]) * q[2 * per:3 * per] * keep)
        for k, sides in zip(local, blocks):
            a_pack = pack_columns if incoming else pack_tiles
            for t, tile in enumerate([*pack_tiles(sides[1], cols), *a_pack(sides[0], cols)]):
                stage[t, pl.ds(k, n_all, stride=stage_pitch), :] = tile

    def finish_rows(indices, update):
        tiles = [[xr[t, pl.ds(i, n_all, stride=pitch), :] for t in range(TILES)] for i in indices]
        x_rows = [jnp.concatenate([*tile, last_group(tile, cols)], axis=0) for tile in tiles]
        gates = [jnp.dot(w_ref[update, 4 * width:5 * width, :], zn[i], preferred_element_type=jnp.float32) for i in indices]
        normed = [norm_sublanes(x_row, lnb[2], lnb[3]) for x_row in x_rows]
        values = [jnp.dot(w_ref[update, 5 * width:6 * width, :], x_norm, preferred_element_type=jnp.float32) for x_norm in normed]
        return [zt[i] + jax.nn.sigmoid(gate) * value for i, gate, value in zip(indices, gates, values)]

    def for_rows(r, body):
        @pl.loop(0, CHUNK // UNROLL)
        def _(k):
            local = [k * UNROLL + s for s in range(UNROLL)]
            body([r * CHUNK + i for i in local], local)

    def to_others(send_to):
        def row_of(step, columns):
            p = lax.rem(my_p + step, n_dap)
            for column in columns:
                send_to(p, lax.rem(my_q + column, n_dap2))

        far = sorted(range(n_dap2), key=lambda column: -min(column, n_dap2 - column))
        row_of(n_dap // 2, far)

        @pl.loop(1, n_dap // 2)
        def _(k):
            for column in far:
                row_of(n_dap // 2 - k, (column,))
                row_of(n_dap // 2 + k, (column,))

        row_of(0, far[:-1])

    def chunk_rows(p, r):
        return pl.ds(pl.multiple_of(p * rows + r * CHUNK, CHUNK), CHUNK)

    def wait_bytes(ref, sem):
        pltpu.make_async_copy(ref, ref, sem).wait()

    def first_tiles(parity):
        return TILES + parity

    def send_part(parity, part, tiles, first_row, n_rows):
        row = pl.multiple_of(my_p * rows + first_row, CHUNK)
        slot = recv.at[parity, tiles, pl.ds(row, n_rows), pl.ds(pl.multiple_of(my_q * LANES, LANES), LANES)]
        here = pl.ds(pl.multiple_of(first_row, CHUNK), n_rows)
        pltpu.make_async_copy(send.at[me, tiles, here], slot, recv_sem.at[parity, part]).start()

        def send_to(p, q):
            pltpu.make_async_remote_copy(src_ref=send.at[p * n_dap2 + q, tiles, here], dst_ref=slot, send_sem=send_sem.at[part],
                                         recv_sem=recv_sem.at[parity, part], device_id={"dap": p, "dap2": q}, device_id_type=MESH).start()

        to_others(send_to)

    def pack_chunk(r):
        @pl.loop(0, n_all)
        def _(g):
            for t in range(2 * TILES):
                send[g, t, pl.ds(pl.multiple_of(r * CHUNK, CHUNK), CHUNK)] = stage[t, pl.ds(pl.multiple_of(g * stage_pitch, 8), CHUNK), :].astype(jnp.bfloat16)

    def send_chunk(r, parity):
        pack_chunk(r)
        if r == 0:
            send_part(parity, 0, pl.ds(0, 2 * TILES), 0, CHUNK)
        else:
            send_part(parity, r, pl.ds(0, first_tiles(parity)), r * CHUNK, CHUNK)
        if r == n_chunks - 1:
            send_part(parity, n_chunks, pl.ds(first_tiles(parity), 2 * TILES - first_tiles(parity)), CHUNK, rows - CHUNK)

    def part_shape(parity, part):
        if part == 0:
            return 2 * TILES, CHUNK
        if part < n_chunks:
            return first_tiles(parity), CHUNK
        return 2 * TILES - first_tiles(parity), rows - CHUNK

    def wait_received(parity, part):
        tiles, n_rows = part_shape(parity, part)
        wait_bytes(recv.at[parity, pl.ds(0, tiles), pl.ds(0, n_dap * n_rows), :], recv_sem.at[parity, part])

    def wait_sent(parity, part):
        tiles, n_rows = part_shape(parity, part)
        wait_bytes(send.at[pl.ds(0, n_all - 1), pl.ds(0, tiles), pl.ds(0, n_rows)], send_sem.at[part])

    def send_x(r):
        def slots(p, q):
            return (xs.at[q, :, pl.ds(pl.multiple_of((r * n_dap + p) * CHUNK, CHUNK), CHUNK), :],
                    xr.at[:, pl.ds(pl.multiple_of(me * pitch + r * CHUNK, 8), CHUNK), :])

        pltpu.make_async_copy(*slots(my_p, my_q), xrecv_sem.at[r]).start()

        def send_to(p, q):
            src, dst = slots(p, q)
            pltpu.make_async_remote_copy(src_ref=src, dst_ref=dst, send_sem=xsend_sem.at[r], recv_sem=xrecv_sem.at[r],
                                         device_id={"dap": p, "dap2": q}, device_id_type=MESH).start()

        to_others(send_to)

    def contract_chunk(r, pair, blocks):
        for k in range(2):
            halved = [block[:, k * LANES:(k + 1) * LANES] for block in blocks]
            for t, tile in enumerate(pack_tiles(halved, cols)):
                xs[2 * pair + k, t, pl.ds(pl.multiple_of(r * n_dap * CHUNK, CHUNK), n_dap * CHUNK), :] = tile

    def gather_rows(ref, r):
        return jnp.concatenate([ref[chunk_rows(p, r), :] for p in range(n_dap)], axis=0)

    def contract_outgoing(parity):
        def chunk(r):
            lane = lax.rem(lane_iota((n_dap * CHUNK, n_dap2 * LANES)), LANES)
            a_tiles = [gather_rows(recv.at[parity, TILES + t], r) for t in range(TILES)]
            zero = jnp.zeros_like(a_tiles[0])
            low = [jnp.where(lane < cols, a, zero) for a in a_tiles]
            high = [jnp.where(lane < cols, zero, a) for a in a_tiles]

            @pl.loop(0, n_dap2 // 2)
            def _(pair):
                def b_rows(t):
                    pieces = []
                    for k in range(2):
                        pieces += [recv[parity, t, chunk_rows((2 * pair + k) * halves + h, s), :] for s in range(n_chunks) for h in range(halves)]
                        pieces.append(jnp.zeros((LANES - cols, n_dap2 * LANES), jnp.bfloat16))
                    return jnp.concatenate(pieces, axis=0)

                def dot(a, b):
                    return lax.dot_general(a, b, (((1,), (1,)), ((), ())), preferred_element_type=jnp.float32)

                b_tiles = [b_rows(t) for t in range(TILES)]
                blocks = [dot(low[t], b_tiles[t]) for t in range(TILES)]
                blocks.append(dot(high[0], b_tiles[0]) + dot(high[1], b_tiles[1]) + dot(high[2], b_tiles[2]))
                contract_chunk(r, pair, blocks)

            send_x(r)

        for r in range(n_chunks):
            wait_received(parity, r)
        chunk(0)
        wait_received(parity, n_chunks)
        pl.loop(1, n_chunks)(chunk)

    def contract_incoming(parity):
        def chunk(r):
            part = LANES - cols
            turned = [recv[parity, TILES + r, :, q * LANES:(q + 1) * LANES].T for q in range(n_dap2)]
            a_all = [jnp.concatenate([a[g * part:(g + 1) * part] for a in turned], axis=0) for g in range(GROUPS)]

            @pl.loop(0, n_dap2 // 2)
            def _(pair):
                lanes = pl.ds(pl.multiple_of(pair * 2 * LANES, LANES), 2 * LANES)
                b_all = [*[recv[parity, t, :, lanes] for t in range(TILES)], bl[:, lanes]]
                contract_chunk(r, pair, [jnp.dot(a, b, preferred_element_type=jnp.float32) for a, b in zip(a_all, b_all)])

            send_x(r)

        for r in range(n_chunks):
            wait_received(parity, r)

            @pl.loop(0, n_dap)
            def _(p):
                here = chunk_rows(p, r)
                for q in range(n_dap2):
                    lanes = slice(q * LANES, (q + 1) * LANES)
                    tiles = [recv[parity, t, here, lanes].astype(jnp.float32) for t in range(TILES)]
                    bl[here, lanes] = last_group(tiles, cols).astype(jnp.bfloat16)

        chunk(0)
        wait_received(parity, n_chunks)
        pl.loop(1, n_chunks)(chunk)

    def exchange(update, parity, contract, more):
        contract(parity)
        for part in range(n_chunks + 1):
            wait_sent(parity, part)
        load_params(2, update)

        def arrived(r):
            wait_bytes(xs.at[:, :, pl.ds(0, n_dap * CHUNK), :], xrecv_sem.at[r])

        def go_on():
            load_params(0, update + 1)

            def body(indices, local):
                states = finish_rows(indices, update)
                for i, state in zip(indices, states):
                    zt[i] = state
                project_rows(indices, local, states, update + 1, incoming=parity == 0)

            for r in range(n_chunks):
                arrived(r)
                for_rows(r, body)
                send_chunk(r, 1 - parity)

        def end():
            @pl.loop(0, n_chunks)
            def _(r):
                arrived(r)

                def body(indices, local):
                    for i, state in zip(indices, finish_rows(indices, update)):
                        turned = state.T
                        for s in range(n_chunks):
                            for h in range(halves):
                                lane = (s * halves + h) * CHUNK
                                out_ref[i, h * rows + s * CHUNK:h * rows + (s + 1) * CHUNK, :] = turned[lane:lane + CHUNK]

                for_rows(r, body)

        if more is None:
            go_on()
        else:
            pl.when(more)(go_on)
            pl.when(jnp.logical_not(more))(end)
        for r in range(n_chunks):
            wait_bytes(xr.at[:, pl.ds(0, (n_all - 1) * CHUNK), :], xsend_sem.at[r])

    load_params(0, 0)
    pl.semaphore_wait(barrier, n_all - 1)

    def first(indices, local):
        def turn(i):
            order = [z_ref[i, h * rows + s * CHUNK:h * rows + (s + 1) * CHUNK, :] for s in range(n_chunks) for h in range(halves)]
            return jnp.concatenate([jnp.concatenate(order, axis=0).T, jnp.zeros((width, LANES - cols), jnp.float32)], axis=1)

        states = [turn(i) for i in indices]
        for i, state in zip(indices, states):
            zt[i] = state
        project_rows(indices, local, states, 0, incoming=False)

    for r in range(n_chunks):
        for_rows(r, first)
        send_chunk(r, 0)

    @pl.loop(0, n_updates // 2)
    def _(layer):
        exchange(2 * layer, 0, contract_outgoing, None)
        exchange(2 * layer + 1, 1, contract_incoming, layer < n_updates // 2 - 1)


def solution(mesh):
    n_dap, n_dap2 = mesh.shape["dap"], mesh.shape["dap2"]
    n_all = n_dap * n_dap2
    pair_spec = P(("data", "dap"), "dap2", None)
    mask_spec = P(("data", "dap"), "dap2")

    def local_stack(pair_act, pair_mask, ln_z, w_ab, w_g, ln_x, w_o):
        rows, cols, width = pair_act.shape
        n_updates = w_o.shape[0] * w_o.shape[1]
        per = width // GROUPS
        full = rows * n_dap
        pitch, stage_pitch = rows + 8, CHUNK + 8
        n_chunks = rows // CHUNK
        mask = pair_mask.astype(jnp.float32).reshape(rows, cols // rows, rows // CHUNK, CHUNK).transpose(0, 2, 1, 3).reshape(rows, cols)
        mask = jnp.pad(mask, ((0, 0), (0, LANES - cols)))
        w_ab = w_ab.reshape(n_updates, width, 4, GROUPS, per).transpose(0, 3, 2, 4, 1).reshape(n_updates, 4 * width, width)
        w_g = w_g.reshape(n_updates, width, width).transpose(0, 2, 1)
        w_o = w_o.reshape(n_updates, width, width).transpose(0, 2, 1)
        weights = jnp.concatenate([w_ab, w_g, w_o], axis=1)
        norms = jnp.concatenate([ln_z, ln_x], axis=2).reshape(n_updates, 4, width).transpose(0, 2, 1).astype(jnp.float32)
        vmem = pl.BlockSpec(memory_space=pltpu.VMEM)
        return pl.pallas_call(
            functools.partial(kernel, n_dap, n_dap2, n_updates),
            out_shape=jax.ShapeDtypeStruct((rows, cols, width), jnp.float32),
            in_specs=[vmem] * 4,
            out_specs=vmem,
            scratch_shapes=[
                pltpu.VMEM((rows, width, LANES), jnp.float32),
                pltpu.VMEM((rows, width, LANES), jnp.bfloat16),
                pltpu.VMEM((2 * TILES, n_all * stage_pitch, LANES), jnp.float32),
                pltpu.VMEM((n_all, 2 * TILES, rows, LANES), jnp.bfloat16),
                pltpu.VMEM((2, 2 * TILES, full, n_dap2 * LANES), jnp.bfloat16),
                pltpu.VMEM((full, n_dap2 * LANES), jnp.bfloat16),
                pltpu.VMEM((n_dap2, TILES, full, LANES), jnp.float32),
                pltpu.VMEM((TILES, n_all * pitch, LANES), jnp.float32),
                pltpu.VMEM((4, width, LANES), jnp.float32),
                pltpu.SemaphoreType.DMA((n_chunks + 1,)),
                pltpu.SemaphoreType.DMA((2, n_chunks + 1)),
                pltpu.SemaphoreType.DMA((n_chunks,)),
                pltpu.SemaphoreType.DMA((n_chunks,)),
            ],
            compiler_params=pltpu.CompilerParams(collective_id=0, has_side_effects=True, vmem_limit_bytes=60 * 1024 * 1024),
            name="triangle_stack",
        )(pair_act, mask, weights, norms)

    return jax.shard_map(local_stack, mesh=mesh, in_specs=(pair_spec, mask_spec, P(), P(), P(), P(), P()), out_specs=pair_spec, check_vma=False)
```

```python
import functools

import jax
import jax.numpy as jnp
from jax import lax
from jax.experimental import pallas as pl
from jax.experimental.pallas import tpu as pltpu
from jax.sharding import PartitionSpec as P

LN_EPS = 1e-5
LANES = 128
GROUPS = 4
TILES = 3
CHUNK = 16
UNROLL = 8
BATCH = 3
MESH = pl.DeviceIdType.MESH


def lane_iota(shape):
    return lax.broadcasted_iota(jnp.int32, shape, len(shape) - 1)


def pack_tiles(blocks, cols):
    part = LANES - cols
    lane = lane_iota(blocks[0].shape)
    return [jnp.where(lane < cols, blocks[t], pltpu.roll(blocks[3], cols - part * t, 1)) for t in range(TILES)]


def last_group(tiles, cols):
    part = LANES - cols
    lane = lane_iota(tiles[0].shape)
    moved = [pltpu.roll(tiles[t], part * (t + 1), 1) for t in range(TILES)]
    return jnp.where(lane < part, moved[0], jnp.where(lane < 2 * part, moved[1], moved[2]))


def pack_columns(blocks, cols):
    part = LANES - cols
    lane = lane_iota(blocks[0].shape)
    tiles = []
    for t in range(TILES):
        moved = [block if g == t else pltpu.roll(block, part * (g - t) % LANES, 1) for g, block in enumerate(blocks)]
        tile = moved[GROUPS - 1]
        for g in reversed(range(GROUPS - 1)):
            tile = jnp.where(lane < part * (g + 1), moved[g], tile)
        tiles.append(tile)
    return tiles


def norm_sublanes(values, gain, bias):
    mean = jnp.mean(values, axis=0, keepdims=True)
    centered = values - mean
    variance = jnp.mean(centered * centered, axis=0, keepdims=True)
    return (centered * lax.rsqrt(variance + LN_EPS) * gain + bias).astype(jnp.bfloat16)


def kernel(n_dap, n_dap2, n_updates, z_ref, m_ref, w_ref, ln_ref, out_ref, zt, zn, stage, send, recv, bl, xs, xr, lnb,
           send_sem, recv_sem, xsend_sem, xrecv_sem):
    rows, cols, width = z_ref.shape
    n_all = n_dap * n_dap2
    pitch, stage_pitch = xr.shape[1] // n_all, stage.shape[1] // n_all
    per = width // GROUPS
    full = rows * n_dap
    n_chunks = rows // CHUNK
    halves = cols // rows
    my_p, my_q = lax.axis_index("dap"), lax.axis_index("dap2")
    me = my_p * n_dap2 + my_q

    barrier = pltpu.get_barrier_semaphore()

    @pl.loop(1, n_all)
    def _(off):
        peer = lax.rem(me + off, n_all)
        pl.semaphore_signal(barrier, inc=1, device_id={"dap": peer // n_dap2, "dap2": lax.rem(peer, n_dap2)}, device_id_type=MESH)

    def load_params(first, update):
        for k in (first, first + 1):
            lnb[k] = jnp.broadcast_to(ln_ref[update, :, k:k + 1], (width, LANES))

    def project_rows(indices, local, states, update, incoming):
        normed = [norm_sublanes(state, lnb[0], lnb[1]) for state in states]
        for i, n_row in zip(indices, normed):
            zn[i] = n_row
        keeps = [m_ref[pl.ds(i, 1), :] for i in indices]
        blocks = [([], []) for _ in indices]
        for g in range(GROUPS):
            weight = w_ref[update, g * 4 * per:(g + 1) * 4 * per, :]
            for keep, n_row, (a_blocks, b_blocks) in zip(keeps, normed, blocks):
                q = jnp.dot(weight, n_row, preferred_element_type=jnp.float32)
                a_blocks.append(jax.nn.sigmoid(q[per:2 * per]) * q[:per] * keep)
                b_blocks.append(jax.nn.sigmoid(q[3 * per:]) * q[2 * per:3 * per] * keep)
        for k, sides in zip(local, blocks):
            a_pack = pack_columns if incoming else pack_tiles
            for t, tile in enumerate([*pack_tiles(sides[1], cols), *a_pack(sides[0], cols)]):
                stage[t, pl.ds(k, n_all, stride=stage_pitch), :] = tile

    def finish_rows(indices, update):
        tiles = [[xr[t, pl.ds(i, n_all, stride=pitch), :] for t in range(TILES)] for i in indices]
        x_rows = [jnp.concatenate([*tile, last_group(tile, cols)], axis=0) for tile in tiles]
        gates = [jnp.dot(w_ref[update, 4 * width:5 * width, :], zn[i], preferred_element_type=jnp.float32) for i in indices]
        normed = [norm_sublanes(x_row, lnb[2], lnb[3]) for x_row in x_rows]
        values = [jnp.dot(w_ref[update, 5 * width:6 * width, :], x_norm, preferred_element_type=jnp.float32) for x_norm in normed]
        return [zt[i] + jax.nn.sigmoid(gate) * value for i, gate, value in zip(indices, gates, values)]

    def for_rows(r, body):
        @pl.loop(0, CHUNK // UNROLL)
        def _(k):
            local = [k * UNROLL + s for s in range(UNROLL)]
            body([r * CHUNK + i for i in local], local)

    def to_others(send_to):
        def step(off):
            peer = lax.rem(me + off, n_all)
            send_to(lax.div(peer, n_dap2), lax.rem(peer, n_dap2))

        @pl.loop(0, (n_all - 1) // BATCH)
        def _(k):
            for s in range(BATCH):
                step(1 + k * BATCH + s)

        for off in range((n_all - 1) // BATCH * BATCH + 1, n_all):
            step(off)

    def chunk_rows(p, r):
        return pl.ds(pl.multiple_of(p * rows + r * CHUNK, CHUNK), CHUNK)

    def wait_bytes(ref, sem):
        pltpu.make_async_copy(ref, ref, sem).wait()

    def first_tiles(parity):
        return TILES + parity

    def send_part(parity, part, tiles, first_row, n_rows):
        row = pl.multiple_of(my_p * rows + first_row, CHUNK)
        slot = recv.at[parity, tiles, pl.ds(row, n_rows), pl.ds(pl.multiple_of(my_q * LANES, LANES), LANES)]
        here = pl.ds(pl.multiple_of(first_row, CHUNK), n_rows)
        pltpu.make_async_copy(send.at[me, tiles, here], slot, recv_sem.at[parity, part]).start()

        def send_to(p, q):
            pltpu.make_async_remote_copy(src_ref=send.at[p * n_dap2 + q, tiles, here], dst_ref=slot, send_sem=send_sem.at[part],
                                         recv_sem=recv_sem.at[parity, part], device_id={"dap": p, "dap2": q}, device_id_type=MESH).start()

        to_others(send_to)

    def pack_chunk(r):
        @pl.loop(0, n_all)
        def _(g):
            for t in range(2 * TILES):
                send[g, t, pl.ds(pl.multiple_of(r * CHUNK, CHUNK), CHUNK)] = stage[t, pl.ds(pl.multiple_of(g * stage_pitch, 8), CHUNK), :].astype(jnp.bfloat16)

    def send_chunk(r, parity):
        early, late = first_tiles(parity), 2 * TILES - first_tiles(parity)
        pack_chunk(r)
        send_part(parity, r, pl.ds(0, early), r * CHUNK, CHUNK)

        @pl.when(r == 0)
        def _():
            send_part(parity, n_chunks, pl.ds(early, late), 0, CHUNK)

        @pl.when(r == n_chunks - 1)
        def _():
            send_part(parity, n_chunks + 1, pl.ds(early, late), CHUNK, rows - CHUNK)

    def part_shape(parity, part):
        if part < n_chunks:
            return first_tiles(parity), CHUNK
        return 2 * TILES - first_tiles(parity), CHUNK if part == n_chunks else rows - CHUNK

    def wait_received(parity, part):
        tiles, n_rows = part_shape(parity, part)
        wait_bytes(recv.at[parity, pl.ds(0, tiles), pl.ds(0, n_dap * n_rows), :], recv_sem.at[parity, part])

    def wait_sent(parity, part):
        tiles, n_rows = part_shape(parity, part)
        wait_bytes(send.at[pl.ds(0, n_all - 1), pl.ds(0, tiles), pl.ds(0, n_rows)], send_sem.at[part])

    def send_x(r):
        def slots(p, q):
            return (xs.at[q, :, pl.ds(pl.multiple_of((r * n_dap + p) * CHUNK, CHUNK), CHUNK), :],
                    xr.at[:, pl.ds(pl.multiple_of(me * pitch + r * CHUNK, 8), CHUNK), :])

        pltpu.make_async_copy(*slots(my_p, my_q), xrecv_sem.at[r]).start()

        def send_to(p, q):
            src, dst = slots(p, q)
            pltpu.make_async_remote_copy(src_ref=src, dst_ref=dst, send_sem=xsend_sem.at[r], recv_sem=xrecv_sem.at[r],
                                         device_id={"dap": p, "dap2": q}, device_id_type=MESH).start()

        to_others(send_to)

    def contract_chunk(r, pair, blocks):
        for k in range(2):
            halved = [block[:, k * LANES:(k + 1) * LANES] for block in blocks]
            for t, tile in enumerate(pack_tiles(halved, cols)):
                xs[2 * pair + k, t, pl.ds(pl.multiple_of(r * n_dap * CHUNK, CHUNK), n_dap * CHUNK), :] = tile

    def gather_rows(ref, r):
        return jnp.concatenate([ref[chunk_rows(p, r), :] for p in range(n_dap)], axis=0)

    def contract_outgoing(parity):
        def chunk(r):
            @pl.when(r == 1)
            def _():
                wait_received(parity, n_chunks + 1)

            lane = lax.rem(lane_iota((n_dap * CHUNK, n_dap2 * LANES)), LANES)
            a_tiles = [gather_rows(recv.at[parity, TILES + t], r) for t in range(TILES)]
            zero = jnp.zeros_like(a_tiles[0])
            low = [jnp.where(lane < cols, a, zero) for a in a_tiles]
            high = [jnp.where(lane < cols, zero, a) for a in a_tiles]

            @pl.loop(0, n_dap2 // 2)
            def _(pair):
                def b_rows(t):
                    pieces = []
                    for k in range(2):
                        pieces += [recv[parity, t, chunk_rows((2 * pair + k) * halves + h, s), :] for s in range(n_chunks) for h in range(halves)]
                        pieces.append(jnp.zeros((LANES - cols, n_dap2 * LANES), jnp.bfloat16))
                    return jnp.concatenate(pieces, axis=0)

                def dot(a, b):
                    return lax.dot_general(a, b, (((1,), (1,)), ((), ())), preferred_element_type=jnp.float32)

                b_tiles = [b_rows(t) for t in range(TILES)]
                blocks = [dot(low[t], b_tiles[t]) for t in range(TILES)]
                blocks.append(dot(high[0], b_tiles[0]) + dot(high[1], b_tiles[1]) + dot(high[2], b_tiles[2]))
                contract_chunk(r, pair, blocks)

            send_x(r)

        for part in range(n_chunks + 1):
            wait_received(parity, part)
        pl.loop(0, n_chunks)(chunk)

    def contract_incoming(parity):
        def chunk(r):
            @pl.when(r == 1)
            def _():
                wait_received(parity, n_chunks + 1)

            part = LANES - cols
            turned = [recv[parity, TILES + r, :, q * LANES:(q + 1) * LANES].T for q in range(n_dap2)]
            a_all = [jnp.concatenate([a[g * part:(g + 1) * part] for a in turned], axis=0) for g in range(GROUPS)]

            @pl.loop(0, n_dap2 // 2)
            def _(pair):
                lanes = pl.ds(pl.multiple_of(pair * 2 * LANES, LANES), 2 * LANES)
                b_all = [*[recv[parity, t, :, lanes] for t in range(TILES)], bl[:, lanes]]
                contract_chunk(r, pair, [jnp.dot(a, b, preferred_element_type=jnp.float32) for a, b in zip(a_all, b_all)])

            send_x(r)

        @pl.loop(0, n_chunks)
        def _(r):
            wait_bytes(recv.at[parity, pl.ds(0, first_tiles(parity)), pl.ds(0, n_dap * CHUNK), :], recv_sem.at[parity, r])

            @pl.loop(0, n_dap)
            def _(p):
                here = chunk_rows(p, r)
                for q in range(n_dap2):
                    lanes = slice(q * LANES, (q + 1) * LANES)
                    tiles = [recv[parity, t, here, lanes].astype(jnp.float32) for t in range(TILES)]
                    bl[here, lanes] = last_group(tiles, cols).astype(jnp.bfloat16)

        wait_received(parity, n_chunks)
        pl.loop(0, n_chunks)(chunk)

    def exchange(update, parity, contract, more):
        contract(parity)
        for part in range(n_chunks + 2):
            wait_sent(parity, part)
        load_params(2, update)

        def arrived(r):
            wait_bytes(xs.at[:, :, pl.ds(0, n_dap * CHUNK), :], xrecv_sem.at[r])

        def go_on():
            load_params(0, update + 1)

            def body(indices, local):
                states = finish_rows(indices, update)
                for i, state in zip(indices, states):
                    zt[i] = state
                project_rows(indices, local, states, update + 1, incoming=parity == 0)

            @pl.loop(0, n_chunks)
            def _(r):
                arrived(r)
                for_rows(r, body)
                send_chunk(r, 1 - parity)

        def end():
            @pl.loop(0, n_chunks)
            def _(r):
                arrived(r)

                def body(indices, local):
                    for i, state in zip(indices, finish_rows(indices, update)):
                        turned = state.T
                        for s in range(n_chunks):
                            for h in range(halves):
                                lane = (s * halves + h) * CHUNK
                                out_ref[i, h * rows + s * CHUNK:h * rows + (s + 1) * CHUNK, :] = turned[lane:lane + CHUNK]

                for_rows(r, body)

        if more is None:
            go_on()
        else:
            pl.when(more)(go_on)
            pl.when(jnp.logical_not(more))(end)
        for r in range(n_chunks):
            wait_bytes(xr.at[:, pl.ds(0, (n_all - 1) * CHUNK), :], xsend_sem.at[r])

    load_params(0, 0)
    pl.semaphore_wait(barrier, n_all - 1)

    def first(indices, local):
        def turn(i):
            order = [z_ref[i, h * rows + s * CHUNK:h * rows + (s + 1) * CHUNK, :] for s in range(n_chunks) for h in range(halves)]
            return jnp.concatenate([jnp.concatenate(order, axis=0).T, jnp.zeros((width, LANES - cols), jnp.float32)], axis=1)

        states = [turn(i) for i in indices]
        for i, state in zip(indices, states):
            zt[i] = state
        project_rows(indices, local, states, 0, incoming=False)

    @pl.loop(0, n_chunks)
    def _(r):
        for_rows(r, first)
        send_chunk(r, 0)

    @pl.loop(0, n_updates // 2)
    def _(layer):
        exchange(2 * layer, 0, contract_outgoing, None)
        exchange(2 * layer + 1, 1, contract_incoming, layer < n_updates // 2 - 1)


def solution(mesh):
    n_dap, n_dap2 = mesh.shape["dap"], mesh.shape["dap2"]
    n_all = n_dap * n_dap2
    pair_spec = P(("data", "dap"), "dap2", None)
    mask_spec = P(("data", "dap"), "dap2")

    def local_stack(pair_act, pair_mask, ln_z, w_ab, w_g, ln_x, w_o):
        rows, cols, width = pair_act.shape
        n_updates = w_o.shape[0] * w_o.shape[1]
        per = width // GROUPS
        full = rows * n_dap
        pitch, stage_pitch = rows + 8, CHUNK + 8
        n_chunks = rows // CHUNK
        mask = pair_mask.astype(jnp.float32).reshape(rows, cols // rows, rows // CHUNK, CHUNK).transpose(0, 2, 1, 3).reshape(rows, cols)
        mask = jnp.pad(mask, ((0, 0), (0, LANES - cols)))
        w_ab = w_ab.reshape(n_updates, width, 4, GROUPS, per).transpose(0, 3, 2, 4, 1).reshape(n_updates, 4 * width, width)
        w_g = w_g.reshape(n_updates, width, width).transpose(0, 2, 1)
        w_o = w_o.reshape(n_updates, width, width).transpose(0, 2, 1)
        weights = jnp.concatenate([w_ab, w_g, w_o], axis=1)
        norms = jnp.concatenate([ln_z, ln_x], axis=2).reshape(n_updates, 4, width).transpose(0, 2, 1).astype(jnp.float32)
        vmem = pl.BlockSpec(memory_space=pltpu.VMEM)
        return pl.pallas_call(
            functools.partial(kernel, n_dap, n_dap2, n_updates),
            out_shape=jax.ShapeDtypeStruct((rows, cols, width), jnp.float32),
            in_specs=[vmem] * 4,
            out_specs=vmem,
            scratch_shapes=[
                pltpu.VMEM((rows, width, LANES), jnp.float32),
                pltpu.VMEM((rows, width, LANES), jnp.bfloat16),
                pltpu.VMEM((2 * TILES, n_all * stage_pitch, LANES), jnp.float32),
                pltpu.VMEM((n_all, 2 * TILES, rows, LANES), jnp.bfloat16),
                pltpu.VMEM((2, 2 * TILES, full, n_dap2 * LANES), jnp.bfloat16),
                pltpu.VMEM((full, n_dap2 * LANES), jnp.bfloat16),
                pltpu.VMEM((n_dap2, TILES, full, LANES), jnp.float32),
                pltpu.VMEM((TILES, n_all * pitch, LANES), jnp.float32),
                pltpu.VMEM((4, width, LANES), jnp.float32),
                pltpu.SemaphoreType.DMA((n_chunks + 2,)),
                pltpu.SemaphoreType.DMA((2, n_chunks + 2)),
                pltpu.SemaphoreType.DMA((n_chunks,)),
                pltpu.SemaphoreType.DMA((n_chunks,)),
            ],
            compiler_params=pltpu.CompilerParams(collective_id=0, has_side_effects=True, vmem_limit_bytes=60 * 1024 * 1024),
            name="triangle_stack",
        )(pair_act, mask, weights, norms)

    return jax.shard_map(local_stack, mesh=mesh, in_specs=(pair_spec, mask_spec, P(), P(), P(), P(), P()), out_specs=pair_spec, check_vma=False)
```

```python
import functools

import jax
import jax.numpy as jnp
from jax import lax
from jax.experimental import pallas as pl
from jax.experimental.pallas import tpu as pltpu
from jax.sharding import PartitionSpec as P

LN_EPS = 1e-5
LANES = 128
GROUPS = 4
TILES = 3
CHUNK = 16
UNROLL = 8
BATCH = 3
MESH = pl.DeviceIdType.MESH


def lane_iota(shape):
    return lax.broadcasted_iota(jnp.int32, shape, len(shape) - 1)


def pack_tiles(blocks, cols):
    part = LANES - cols
    lane = lane_iota(blocks[0].shape)
    return [jnp.where(lane < cols, blocks[t], pltpu.roll(blocks[3], cols - part * t, 1)) for t in range(TILES)]


def last_group(tiles, cols):
    part = LANES - cols
    lane = lane_iota(tiles[0].shape)
    moved = [pltpu.roll(tiles[t], part * (t + 1), 1) for t in range(TILES)]
    return jnp.where(lane < part, moved[0], jnp.where(lane < 2 * part, moved[1], moved[2]))


def pack_columns(blocks, cols):
    part = LANES - cols
    lane = lane_iota(blocks[0].shape)
    tiles = []
    for t in range(TILES):
        moved = [block if g == t else pltpu.roll(block, part * (g - t) % LANES, 1) for g, block in enumerate(blocks)]
        tile = moved[GROUPS - 1]
        for g in reversed(range(GROUPS - 1)):
            tile = jnp.where(lane < part * (g + 1), moved[g], tile)
        tiles.append(tile)
    return tiles


def norm_sublanes(values, gain, bias):
    mean = jnp.mean(values, axis=0, keepdims=True)
    centered = values - mean
    variance = jnp.mean(centered * centered, axis=0, keepdims=True)
    return (centered * lax.rsqrt(variance + LN_EPS) * gain + bias).astype(jnp.bfloat16)


def kernel(n_dap, n_dap2, n_updates, z_ref, mask_ref, ln_z_ref, w_ab_ref, w_g_ref, ln_x_ref, w_o_ref, out_ref, m_ref, w_ref, zt, zn, stage, send, recv, bl, xs, xr, lnb,
           send_sem, recv_sem, xsend_sem, xrecv_sem):
    rows, cols, width = z_ref.shape
    n_all = n_dap * n_dap2
    pitch, stage_pitch = xr.shape[1] // n_all, stage.shape[1] // n_all
    per = width // GROUPS
    full = rows * n_dap
    n_chunks = rows // CHUNK
    halves = cols // rows
    my_p, my_q = lax.axis_index("dap"), lax.axis_index("dap2")
    me = my_p * n_dap2 + my_q

    barrier = pltpu.get_barrier_semaphore()

    @pl.loop(1, n_all)
    def _(off):
        peer = lax.rem(me + off, n_all)
        pl.semaphore_signal(barrier, inc=1, device_id={"dap": peer // n_dap2, "dap2": lax.rem(peer, n_dap2)}, device_id_type=MESH)

    def turn_columns(values):
        order = [values[h * rows + s * CHUNK:h * rows + (s + 1) * CHUNK] for s in range(n_chunks) for h in range(halves)]
        return jnp.concatenate(order, axis=0)

    def load_norm(first, norm_ref, update):
        params = norm_ref[update].astype(jnp.float32)
        for k in range(2):
            lnb[first + k] = jnp.broadcast_to(params[k:k + 1], (LANES, width)).T

    def load_projection(update):
        load_norm(0, ln_z_ref, update)
        for kind in range(4):
            turned = w_ab_ref[update, :, kind * width:(kind + 1) * width].T
            for g in range(GROUPS):
                w_ref[g * 4 * per + kind * per:g * 4 * per + (kind + 1) * per, :] = turned[g * per:(g + 1) * per]

    def load_finish(update):
        load_norm(2, ln_x_ref, update)
        w_ref[4 * width:5 * width, :] = w_g_ref[update].T
        w_ref[5 * width:6 * width, :] = w_o_ref[update].T

    def project_rows(indices, local, states, incoming):
        normed = [norm_sublanes(state, lnb[0], lnb[1]) for state in states]
        for i, n_row in zip(indices, normed):
            zn[i] = n_row
        keeps = [m_ref[pl.ds(i, 1), :] for i in indices]
        blocks = [([], []) for _ in indices]
        for g in range(GROUPS):
            weight = w_ref[g * 4 * per:(g + 1) * 4 * per, :]
            for keep, n_row, (a_blocks, b_blocks) in zip(keeps, normed, blocks):
                q = jnp.dot(weight, n_row, preferred_element_type=jnp.float32)
                a_blocks.append(jax.nn.sigmoid(q[per:2 * per]) * q[:per] * keep)
                b_blocks.append(jax.nn.sigmoid(q[3 * per:]) * q[2 * per:3 * per] * keep)
        for k, sides in zip(local, blocks):
            a_pack = pack_columns if incoming else pack_tiles
            for t, tile in enumerate([*pack_tiles(sides[1], cols), *a_pack(sides[0], cols)]):
                stage[t, pl.ds(k, n_all, stride=stage_pitch), :] = tile

    def finish_rows(indices):
        tiles = [[xr[t, pl.ds(i, n_all, stride=pitch), :] for t in range(TILES)] for i in indices]
        x_rows = [jnp.concatenate([*tile, last_group(tile, cols)], axis=0) for tile in tiles]
        gates = [jnp.dot(w_ref[4 * width:5 * width, :], zn[i], preferred_element_type=jnp.float32) for i in indices]
        normed = [norm_sublanes(x_row, lnb[2], lnb[3]) for x_row in x_rows]
        values = [jnp.dot(w_ref[5 * width:6 * width, :], x_norm, preferred_element_type=jnp.float32) for x_norm in normed]
        return [zt[i] + jax.nn.sigmoid(gate) * value for i, gate, value in zip(indices, gates, values)]

    def for_rows(r, body):
        @pl.loop(0, CHUNK // UNROLL)
        def _(k):
            local = [k * UNROLL + s for s in range(UNROLL)]
            body([r * CHUNK + i for i in local], local)

    def to_others(send_to):
        def step(off):
            peer = lax.rem(me + off, n_all)
            send_to(lax.div(peer, n_dap2), lax.rem(peer, n_dap2))

        @pl.loop(0, (n_all - 1) // BATCH)
        def _(k):
            for s in range(BATCH):
                step(1 + k * BATCH + s)

        for off in range((n_all - 1) // BATCH * BATCH + 1, n_all):
            step(off)

    def chunk_rows(p, r):
        return pl.ds(pl.multiple_of(p * rows + r * CHUNK, CHUNK), CHUNK)

    def wait_bytes(ref, sem):
        pltpu.make_async_copy(ref, ref, sem).wait()

    def first_tiles(parity):
        return TILES + parity

    def send_part(parity, part, tiles, first_row, n_rows):
        row = pl.multiple_of(my_p * rows + first_row, CHUNK)
        slot = recv.at[parity, tiles, pl.ds(row, n_rows), pl.ds(pl.multiple_of(my_q * LANES, LANES), LANES)]
        here = pl.ds(pl.multiple_of(first_row, CHUNK), n_rows)
        pltpu.make_async_copy(send.at[me, tiles, here], slot, recv_sem.at[parity, part]).start()

        def send_to(p, q):
            pltpu.make_async_remote_copy(src_ref=send.at[p * n_dap2 + q, tiles, here], dst_ref=slot, send_sem=send_sem.at[part],
                                         recv_sem=recv_sem.at[parity, part], device_id={"dap": p, "dap2": q}, device_id_type=MESH).start()

        to_others(send_to)

    def pack_chunk(r):
        @pl.loop(0, n_all)
        def _(g):
            for t in range(2 * TILES):
                send[g, t, pl.ds(pl.multiple_of(r * CHUNK, CHUNK), CHUNK)] = stage[t, pl.ds(pl.multiple_of(g * stage_pitch, 8), CHUNK), :].astype(jnp.bfloat16)

    def send_chunk(r, parity):
        early, late = first_tiles(parity), 2 * TILES - first_tiles(parity)
        pack_chunk(r)
        send_part(parity, r, pl.ds(0, early), r * CHUNK, CHUNK)

        @pl.when(r == 0)
        def _():
            send_part(parity, n_chunks, pl.ds(early, late), 0, CHUNK)

        @pl.when(r == n_chunks - 1)
        def _():
            send_part(parity, n_chunks + 1, pl.ds(early, late), CHUNK, rows - CHUNK)

    def part_shape(parity, part):
        if part < n_chunks:
            return first_tiles(parity), CHUNK
        return 2 * TILES - first_tiles(parity), CHUNK if part == n_chunks else rows - CHUNK

    def wait_received(parity, part):
        tiles, n_rows = part_shape(parity, part)
        wait_bytes(recv.at[parity, pl.ds(0, tiles), pl.ds(0, n_dap * n_rows), :], recv_sem.at[parity, part])

    def wait_sent(parity, part):
        tiles, n_rows = part_shape(parity, part)
        wait_bytes(send.at[pl.ds(0, n_all - 1), pl.ds(0, tiles), pl.ds(0, n_rows)], send_sem.at[part])

    def send_x(r):
        def slots(p, q):
            return (xs.at[q, :, pl.ds(pl.multiple_of((r * n_dap + p) * CHUNK, CHUNK), CHUNK), :],
                    xr.at[:, pl.ds(pl.multiple_of(me * pitch + r * CHUNK, 8), CHUNK), :])

        pltpu.make_async_copy(*slots(my_p, my_q), xrecv_sem.at[r]).start()

        def send_to(p, q):
            src, dst = slots(p, q)
            pltpu.make_async_remote_copy(src_ref=src, dst_ref=dst, send_sem=xsend_sem.at[r], recv_sem=xrecv_sem.at[r],
                                         device_id={"dap": p, "dap2": q}, device_id_type=MESH).start()

        to_others(send_to)

    def contract_chunk(r, pair, blocks):
        for k in range(2):
            halved = [block[:, k * LANES:(k + 1) * LANES] for block in blocks]
            for t, tile in enumerate(pack_tiles(halved, cols)):
                xs[2 * pair + k, t, pl.ds(pl.multiple_of(r * n_dap * CHUNK, CHUNK), n_dap * CHUNK), :] = tile

    def gather_rows(ref, r):
        return jnp.concatenate([ref[chunk_rows(p, r), :] for p in range(n_dap)], axis=0)

    def contract_outgoing(parity):
        def chunk(r):
            @pl.when(r == 1)
            def _():
                wait_received(parity, n_chunks + 1)

            lane = lax.rem(lane_iota((n_dap * CHUNK, n_dap2 * LANES)), LANES)
            a_tiles = [gather_rows(recv.at[parity, TILES + t], r) for t in range(TILES)]
            zero = jnp.zeros_like(a_tiles[0])
            low = [jnp.where(lane < cols, a, zero) for a in a_tiles]
            high = [jnp.where(lane < cols, zero, a) for a in a_tiles]

            @pl.loop(0, n_dap2 // 2)
            def _(pair):
                def b_rows(t):
                    pieces = []
                    for k in range(2):
                        pieces += [recv[parity, t, chunk_rows((2 * pair + k) * halves + h, s), :] for s in range(n_chunks) for h in range(halves)]
                        pieces.append(jnp.zeros((LANES - cols, n_dap2 * LANES), jnp.bfloat16))
                    return jnp.concatenate(pieces, axis=0)

                def dot(a, b):
                    return lax.dot_general(a, b, (((1,), (1,)), ((), ())), preferred_element_type=jnp.float32)

                b_tiles = [b_rows(t) for t in range(TILES)]
                blocks = [dot(low[t], b_tiles[t]) for t in range(TILES)]
                blocks.append(dot(high[0], b_tiles[0]) + dot(high[1], b_tiles[1]) + dot(high[2], b_tiles[2]))
                contract_chunk(r, pair, blocks)

            send_x(r)

        for part in range(n_chunks + 1):
            wait_received(parity, part)
        pl.loop(0, n_chunks)(chunk)

    def contract_incoming(parity):
        def chunk(r):
            @pl.when(r == 1)
            def _():
                wait_received(parity, n_chunks + 1)

            part = LANES - cols
            turned = [recv[parity, TILES + r, :, q * LANES:(q + 1) * LANES].T for q in range(n_dap2)]
            a_all = [jnp.concatenate([a[g * part:(g + 1) * part] for a in turned], axis=0) for g in range(GROUPS)]

            @pl.loop(0, n_dap2 // 2)
            def _(pair):
                lanes = pl.ds(pl.multiple_of(pair * 2 * LANES, LANES), 2 * LANES)
                b_all = [*[recv[parity, t, :, lanes] for t in range(TILES)], bl[:, lanes]]
                contract_chunk(r, pair, [jnp.dot(a, b, preferred_element_type=jnp.float32) for a, b in zip(a_all, b_all)])

            send_x(r)

        @pl.loop(0, n_chunks)
        def _(r):
            wait_bytes(recv.at[parity, pl.ds(0, first_tiles(parity)), pl.ds(0, n_dap * CHUNK), :], recv_sem.at[parity, r])

            @pl.loop(0, n_dap)
            def _(p):
                here = chunk_rows(p, r)
                for q in range(n_dap2):
                    lanes = slice(q * LANES, (q + 1) * LANES)
                    tiles = [recv[parity, t, here, lanes].astype(jnp.float32) for t in range(TILES)]
                    bl[here, lanes] = last_group(tiles, cols).astype(jnp.bfloat16)

        wait_received(parity, n_chunks)
        pl.loop(0, n_chunks)(chunk)

    def exchange(update, parity, contract, more):
        contract(parity)
        for part in range(n_chunks + 2):
            wait_sent(parity, part)
        load_finish(update)

        def arrived(r):
            wait_bytes(xs.at[:, :, pl.ds(0, n_dap * CHUNK), :], xrecv_sem.at[r])

        def go_on():
            load_projection(update + 1)

            def body(indices, local):
                states = finish_rows(indices)
                for i, state in zip(indices, states):
                    zt[i] = state
                project_rows(indices, local, states, incoming=parity == 0)

            @pl.loop(0, n_chunks)
            def _(r):
                arrived(r)
                for_rows(r, body)
                send_chunk(r, 1 - parity)

        def end():
            @pl.loop(0, n_chunks)
            def _(r):
                arrived(r)

                def body(indices, local):
                    for i, state in zip(indices, finish_rows(indices)):
                        turned = state.T
                        for s in range(n_chunks):
                            for h in range(halves):
                                lane = (s * halves + h) * CHUNK
                                out_ref[i, h * rows + s * CHUNK:h * rows + (s + 1) * CHUNK, :] = turned[lane:lane + CHUNK]

                for_rows(r, body)

        if more is None:
            go_on()
        else:
            pl.when(more)(go_on)
            pl.when(jnp.logical_not(more))(end)
        for r in range(n_chunks):
            wait_bytes(xr.at[:, pl.ds(0, (n_all - 1) * CHUNK), :], xsend_sem.at[r])

    load_projection(0)
    m_ref[...] = jnp.zeros((rows, LANES), jnp.float32)
    m_ref[:, :cols] = turn_columns(mask_ref[...].astype(jnp.float32).T).T

    @pl.loop(0, rows // UNROLL)
    def _(k):
        for s in range(UNROLL):
            i = k * UNROLL + s
            zt[i] = jnp.concatenate([turn_columns(z_ref[i]).T, jnp.zeros((width, LANES - cols), jnp.float32)], axis=1)

    pl.semaphore_wait(barrier, n_all - 1)

    def first(indices, local):
        project_rows(indices, local, [zt[i] for i in indices], incoming=False)

    @pl.loop(0, n_chunks)
    def _(r):
        for_rows(r, first)
        send_chunk(r, 0)

    @pl.loop(0, n_updates // 2)
    def _(layer):
        exchange(2 * layer, 0, contract_outgoing, None)
        exchange(2 * layer + 1, 1, contract_incoming, layer < n_updates // 2 - 1)


def solution(mesh):
    n_dap, n_dap2 = mesh.shape["dap"], mesh.shape["dap2"]
    n_all = n_dap * n_dap2
    pair_spec = P(("data", "dap"), "dap2", None)
    mask_spec = P(("data", "dap"), "dap2")

    def local_stack(pair_act, pair_mask, ln_z, w_ab, w_g, ln_x, w_o):
        rows, cols, width = pair_act.shape
        n_updates = w_o.shape[0] * w_o.shape[1]
        full = rows * n_dap
        pitch, stage_pitch = rows + 8, CHUNK + 8
        n_chunks = rows // CHUNK
        flat = [array.reshape(n_updates, *array.shape[2:]) for array in (ln_z, w_ab, w_g, ln_x, w_o)]
        vmem = pl.BlockSpec(memory_space=pltpu.VMEM)
        return pl.pallas_call(
            functools.partial(kernel, n_dap, n_dap2, n_updates),
            out_shape=jax.ShapeDtypeStruct((rows, cols, width), jnp.float32),
            in_specs=[vmem] * 7,
            out_specs=vmem,
            scratch_shapes=[
                pltpu.VMEM((rows, LANES), jnp.float32),
                pltpu.VMEM((6 * width, width), jnp.bfloat16),
                pltpu.VMEM((rows, width, LANES), jnp.float32),
                pltpu.VMEM((rows, width, LANES), jnp.bfloat16),
                pltpu.VMEM((2 * TILES, n_all * stage_pitch, LANES), jnp.float32),
                pltpu.VMEM((n_all, 2 * TILES, rows, LANES), jnp.bfloat16),
                pltpu.VMEM((2, 2 * TILES, full, n_dap2 * LANES), jnp.bfloat16),
                pltpu.VMEM((full, n_dap2 * LANES), jnp.bfloat16),
                pltpu.VMEM((n_dap2, TILES, full, LANES), jnp.float32),
                pltpu.VMEM((TILES, n_all * pitch, LANES), jnp.float32),
                pltpu.VMEM((4, width, LANES), jnp.float32),
                pltpu.SemaphoreType.DMA((n_chunks + 2,)),
                pltpu.SemaphoreType.DMA((2, n_chunks + 2)),
                pltpu.SemaphoreType.DMA((n_chunks,)),
                pltpu.SemaphoreType.DMA((n_chunks,)),
            ],
            compiler_params=pltpu.CompilerParams(collective_id=0, has_side_effects=True, vmem_limit_bytes=60 * 1024 * 1024),
            name="triangle_stack",
        )(pair_act, pair_mask, *flat)

    return jax.shard_map(local_stack, mesh=mesh, in_specs=(pair_spec, mask_spec, P(), P(), P(), P(), P()), out_specs=pair_spec, check_vma=False)
```

```python
import functools

import jax
import jax.numpy as jnp
from jax import lax
from jax.experimental import pallas as pl
from jax.experimental.pallas import tpu as pltpu
from jax.sharding import PartitionSpec as P

LN_EPS = 1e-5
LANES = 128
GROUPS = 4
TILES = 3
CHUNK = 16
UNROLL = 8
BATCH = 3
MESH = pl.DeviceIdType.MESH


def lane_iota(shape):
    return lax.broadcasted_iota(jnp.int32, shape, len(shape) - 1)


def pack_tiles(blocks, cols):
    part = LANES - cols
    lane = lane_iota(blocks[0].shape)
    return [jnp.where(lane < cols, blocks[t], pltpu.roll(blocks[3], cols - part * t, 1)) for t in range(TILES)]


def last_group(tiles, cols):
    part = LANES - cols
    lane = lane_iota(tiles[0].shape)
    moved = [pltpu.roll(tiles[t], part * (t + 1), 1) for t in range(TILES)]
    return jnp.where(lane < part, moved[0], jnp.where(lane < 2 * part, moved[1], moved[2]))


def pack_columns(blocks, cols):
    part = LANES - cols
    lane = lane_iota(blocks[0].shape)
    tiles = []
    for t in range(TILES):
        moved = [block if g == t else pltpu.roll(block, part * (g - t) % LANES, 1) for g, block in enumerate(blocks)]
        tile = moved[GROUPS - 1]
        for g in reversed(range(GROUPS - 1)):
            tile = jnp.where(lane < part * (g + 1), moved[g], tile)
        tiles.append(tile)
    return tiles


def norm_sublanes(values, gain, bias):
    mean = jnp.mean(values, axis=0, keepdims=True)
    centered = values - mean
    variance = jnp.mean(centered * centered, axis=0, keepdims=True)
    return (centered * lax.rsqrt(variance + LN_EPS) * gain + bias).astype(jnp.bfloat16)


def kernel(n_dap, n_dap2, n_updates, z_ref, mask_ref, ln_z_ref, w_ab_ref, w_g_ref, ln_x_ref, w_o_ref, out_ref, m_ref, w_ref, zt, zn, stage, send, recv, bl, xs, xr, lnb,
           send_sem, recv_sem, xsend_sem, xrecv_sem):
    rows, cols, width = z_ref.shape
    n_all = n_dap * n_dap2
    pitch, stage_pitch = xr.shape[1] // n_all, stage.shape[1] // n_all
    per = width // GROUPS
    full = rows * n_dap
    n_chunks = rows // CHUNK
    halves = cols // rows
    my_p, my_q = lax.axis_index("dap"), lax.axis_index("dap2")
    me = my_p * n_dap2 + my_q

    barrier = pltpu.get_barrier_semaphore()

    @pl.loop(1, n_all)
    def _(off):
        peer = lax.rem(me + off, n_all)
        pl.semaphore_signal(barrier, inc=1, device_id={"dap": peer // n_dap2, "dap2": lax.rem(peer, n_dap2)}, device_id_type=MESH)

    def turn_columns(values):
        order = [values[h * rows + s * CHUNK:h * rows + (s + 1) * CHUNK] for s in range(n_chunks) for h in range(halves)]
        return jnp.concatenate(order, axis=0)

    def load_norm(first, norm_ref, update):
        params = norm_ref[update].astype(jnp.float32)
        for k in range(2):
            lnb[first + k] = jnp.broadcast_to(params[k:k + 1], (LANES, width)).T

    def load_projection(update):
        load_norm(0, ln_z_ref, update)
        for kind in range(4):
            turned = w_ab_ref[update, :, kind * width:(kind + 1) * width].T
            for g in range(GROUPS):
                w_ref[g * 4 * per + kind * per:g * 4 * per + (kind + 1) * per, :] = turned[g * per:(g + 1) * per]

    def load_finish(update):
        load_norm(2, ln_x_ref, update)
        w_ref[4 * width:5 * width, :] = w_g_ref[update].T
        w_ref[5 * width:6 * width, :] = w_o_ref[update].T

    def project_rows(indices, local, states, incoming):
        normed = [norm_sublanes(state, lnb[0], lnb[1]) for state in states]
        for i, n_row in zip(indices, normed):
            zn[i] = n_row
        keeps = [m_ref[pl.ds(i, 1), :] for i in indices]
        blocks = [([], []) for _ in indices]
        for g in range(GROUPS):
            weight = w_ref[g * 4 * per:(g + 1) * 4 * per, :]
            for keep, n_row, (a_blocks, b_blocks) in zip(keeps, normed, blocks):
                q = jnp.dot(weight, n_row, preferred_element_type=jnp.float32)
                a_blocks.append(jax.nn.sigmoid(q[per:2 * per]) * q[:per] * keep)
                b_blocks.append(jax.nn.sigmoid(q[3 * per:]) * q[2 * per:3 * per] * keep)
        for k, sides in zip(local, blocks):
            a_pack = pack_columns if incoming else pack_tiles
            for t, tile in enumerate([*pack_tiles(sides[1], cols), *a_pack(sides[0], cols)]):
                stage[t, pl.ds(k, n_all, stride=stage_pitch), :] = tile

    def finish_rows(indices):
        tiles = [[xr[t, pl.ds(i, n_all, stride=pitch), :] for t in range(TILES)] for i in indices]
        x_rows = [jnp.concatenate([*tile, last_group(tile, cols)], axis=0) for tile in tiles]
        gates = [jnp.dot(w_ref[4 * width:5 * width, :], zn[i], preferred_element_type=jnp.float32) for i in indices]
        normed = [norm_sublanes(x_row, lnb[2], lnb[3]) for x_row in x_rows]
        values = [jnp.dot(w_ref[5 * width:6 * width, :], x_norm, preferred_element_type=jnp.float32) for x_norm in normed]
        return [zt[i] + jax.nn.sigmoid(gate) * value for i, gate, value in zip(indices, gates, values)]

    def for_rows(r, body):
        @pl.loop(0, CHUNK // UNROLL)
        def _(k):
            local = [k * UNROLL + s for s in range(UNROLL)]
            body([r * CHUNK + i for i in local], local)

    def to_others(send_to):
        def step(off):
            peer = lax.rem(me + off, n_all)
            send_to(lax.div(peer, n_dap2), lax.rem(peer, n_dap2))

        @pl.loop(0, (n_all - 1) // BATCH)
        def _(k):
            for s in range(BATCH):
                step(1 + k * BATCH + s)

        for off in range((n_all - 1) // BATCH * BATCH + 1, n_all):
            step(off)

    def chunk_rows(p, r):
        return pl.ds(pl.multiple_of(p * rows + r * CHUNK, CHUNK), CHUNK)

    def wait_bytes(ref, sem):
        pltpu.make_async_copy(ref, ref, sem).wait()

    def first_tiles(parity):
        return TILES + parity

    def send_part(parity, part, tiles, first_row, n_rows):
        row = pl.multiple_of(my_p * rows + first_row, CHUNK)
        slot = recv.at[parity, tiles, pl.ds(row, n_rows), pl.ds(pl.multiple_of(my_q * LANES, LANES), LANES)]
        here = pl.ds(pl.multiple_of(first_row, CHUNK), n_rows)
        pltpu.make_async_copy(send.at[me, tiles, here], slot, recv_sem.at[parity, part]).start()

        def send_to(p, q):
            pltpu.make_async_remote_copy(src_ref=send.at[p * n_dap2 + q, tiles, here], dst_ref=slot, send_sem=send_sem.at[part],
                                         recv_sem=recv_sem.at[parity, part], device_id={"dap": p, "dap2": q}, device_id_type=MESH).start()

        to_others(send_to)

    def pack_chunk(r):
        @pl.loop(0, n_all)
        def _(g):
            for t in range(2 * TILES):
                send[g, t, pl.ds(pl.multiple_of(r * CHUNK, CHUNK), CHUNK)] = stage[t, pl.ds(pl.multiple_of(g * stage_pitch, 8), CHUNK), :].astype(jnp.bfloat16)

    def send_chunk(r, parity):
        early, late = first_tiles(parity), 2 * TILES - first_tiles(parity)
        pack_chunk(r)

        @pl.when(r == 0)
        def _():
            send_part(parity, 0, pl.ds(0, 2 * TILES), 0, CHUNK)

        @pl.when(r > 0)
        def _():
            send_part(parity, r, pl.ds(0, early), r * CHUNK, CHUNK)

        @pl.when(r == n_chunks - 1)
        def _():
            send_part(parity, n_chunks, pl.ds(early, late), CHUNK, rows - CHUNK)

    def part_shape(parity, part):
        if part == 0:
            return 2 * TILES, CHUNK
        if part < n_chunks:
            return first_tiles(parity), CHUNK
        return 2 * TILES - first_tiles(parity), rows - CHUNK

    def wait_received(parity, part):
        tiles, n_rows = part_shape(parity, part)
        wait_bytes(recv.at[parity, pl.ds(0, tiles), pl.ds(0, n_dap * n_rows), :], recv_sem.at[parity, part])

    def wait_sent(parity, part):
        tiles, n_rows = part_shape(parity, part)
        wait_bytes(send.at[pl.ds(0, n_all - 1), pl.ds(0, tiles), pl.ds(0, n_rows)], send_sem.at[part])

    def send_x(r):
        def send_rows(part, first_row, n_rows):
            def slots(p, q):
                return (xs.at[q, :, pl.ds(pl.multiple_of(p * rows + first_row, CHUNK), n_rows), :],
                        xr.at[:, pl.ds(pl.multiple_of(me * pitch + first_row, 8), n_rows), :])

            pltpu.make_async_copy(*slots(my_p, my_q), xrecv_sem.at[part]).start()

            def send_to(p, q):
                src, dst = slots(p, q)
                pltpu.make_async_remote_copy(src_ref=src, dst_ref=dst, send_sem=xsend_sem.at[part], recv_sem=xrecv_sem.at[part],
                                             device_id={"dap": p, "dap2": q}, device_id_type=MESH).start()

            to_others(send_to)

        @pl.when(r == 0)
        def _():
            send_rows(0, 0, CHUNK)

        @pl.when(r == n_chunks - 1)
        def _():
            send_rows(1, CHUNK, rows - CHUNK)

    def contract_chunk(r, pair, blocks):
        for k in range(2):
            halved = [block[:, k * LANES:(k + 1) * LANES] for block in blocks]
            for t, tile in enumerate(pack_tiles(halved, cols)):
                for p in range(n_dap):
                    xs[2 * pair + k, t, chunk_rows(p, r), :] = tile[p * CHUNK:(p + 1) * CHUNK]

    def gather_rows(ref, r):
        return jnp.concatenate([ref[chunk_rows(p, r), :] for p in range(n_dap)], axis=0)

    def contract_outgoing(parity):
        def chunk(r):
            @pl.when(r == 1)
            def _():
                wait_received(parity, n_chunks)

            lane = lax.rem(lane_iota((n_dap * CHUNK, n_dap2 * LANES)), LANES)
            a_tiles = [gather_rows(recv.at[parity, TILES + t], r) for t in range(TILES)]
            zero = jnp.zeros_like(a_tiles[0])
            low = [jnp.where(lane < cols, a, zero) for a in a_tiles]
            high = [jnp.where(lane < cols, zero, a) for a in a_tiles]

            @pl.loop(0, n_dap2 // 2)
            def _(pair):
                def b_rows(t):
                    pieces = []
                    for k in range(2):
                        pieces += [recv[parity, t, chunk_rows((2 * pair + k) * halves + h, s), :] for s in range(n_chunks) for h in range(halves)]
                        pieces.append(jnp.zeros((LANES - cols, n_dap2 * LANES), jnp.bfloat16))
                    return jnp.concatenate(pieces, axis=0)

                def dot(a, b):
                    return lax.dot_general(a, b, (((1,), (1,)), ((), ())), preferred_element_type=jnp.float32)

                b_tiles = [b_rows(t) for t in range(TILES)]
                blocks = [dot(low[t], b_tiles[t]) for t in range(TILES)]
                blocks.append(dot(high[0], b_tiles[0]) + dot(high[1], b_tiles[1]) + dot(high[2], b_tiles[2]))
                contract_chunk(r, pair, blocks)

            send_x(r)

        for part in range(n_chunks):
            wait_received(parity, part)
        pl.loop(0, n_chunks)(chunk)

    def contract_incoming(parity):
        def chunk(r):
            @pl.when(r == 1)
            def _():
                wait_received(parity, n_chunks)

            part = LANES - cols
            turned = [recv[parity, TILES + r, :, q * LANES:(q + 1) * LANES].T for q in range(n_dap2)]
            a_all = [jnp.concatenate([a[g * part:(g + 1) * part] for a in turned], axis=0) for g in range(GROUPS)]

            @pl.loop(0, n_dap2 // 2)
            def _(pair):
                lanes = pl.ds(pl.multiple_of(pair * 2 * LANES, LANES), 2 * LANES)
                b_all = [*[recv[parity, t, :, lanes] for t in range(TILES)], bl[:, lanes]]
                contract_chunk(r, pair, [jnp.dot(a, b, preferred_element_type=jnp.float32) for a, b in zip(a_all, b_all)])

            send_x(r)

        @pl.loop(0, n_chunks)
        def _(r):
            @pl.when(r == 0)
            def _():
                wait_received(parity, 0)

            @pl.when(r > 0)
            def _():
                wait_bytes(recv.at[parity, pl.ds(0, first_tiles(parity)), pl.ds(0, n_dap * CHUNK), :], recv_sem.at[parity, r])

            @pl.loop(0, n_dap // 2)
            def _(k):
                for here, q in [(chunk_rows(2 * k + h, r), q) for h in range(2) for q in range(n_dap2)]:
                    lanes = slice(q * LANES, (q + 1) * LANES)
                    tiles = [recv[parity, t, here, lanes].astype(jnp.float32) for t in range(TILES)]
                    bl[here, lanes] = last_group(tiles, cols).astype(jnp.bfloat16)

        pl.loop(0, n_chunks)(chunk)

    def exchange(update, parity, contract, more):
        contract(parity)
        for part in range(n_chunks + 1):
            wait_sent(parity, part)
        load_finish(update)

        def arrived(r):
            for part, n_rows in enumerate((CHUNK, rows - CHUNK)):
                @pl.when(r == part)
                def _():
                    wait_bytes(xs.at[:, :, pl.ds(0, n_dap * n_rows), :], xrecv_sem.at[part])

        def go_on():
            load_projection(update + 1)

            def body(indices, local):
                states = finish_rows(indices)
                for i, state in zip(indices, states):
                    zt[i] = state
                project_rows(indices, local, states, incoming=parity == 0)

            @pl.loop(0, n_chunks)
            def _(r):
                arrived(r)
                for_rows(r, body)
                send_chunk(r, 1 - parity)

        def end():
            @pl.loop(0, n_chunks)
            def _(r):
                arrived(r)

                def body(indices, local):
                    for i, state in zip(indices, finish_rows(indices)):
                        turned = state.T
                        for s in range(n_chunks):
                            for h in range(halves):
                                lane = (s * halves + h) * CHUNK
                                out_ref[i, h * rows + s * CHUNK:h * rows + (s + 1) * CHUNK, :] = turned[lane:lane + CHUNK]

                for_rows(r, body)

        if more is None:
            go_on()
        else:
            pl.when(more)(go_on)
            pl.when(jnp.logical_not(more))(end)
        for part, n_rows in enumerate((CHUNK, rows - CHUNK)):
            wait_bytes(xr.at[:, pl.ds(0, (n_all - 1) * n_rows), :], xsend_sem.at[part])

    load_projection(0)
    m_ref[...] = jnp.zeros((rows, LANES), jnp.float32)
    m_ref[:, :cols] = turn_columns(mask_ref[...].astype(jnp.float32).T).T

    @pl.loop(0, rows // UNROLL)
    def _(k):
        for s in range(UNROLL):
            i = k * UNROLL + s
            zt[i] = jnp.concatenate([turn_columns(z_ref[i]).T, jnp.zeros((width, LANES - cols), jnp.float32)], axis=1)

    pl.semaphore_wait(barrier, n_all - 1)

    def first(indices, local):
        project_rows(indices, local, [zt[i] for i in indices], incoming=False)

    @pl.loop(0, n_chunks)
    def _(r):
        for_rows(r, first)
        send_chunk(r, 0)

    @pl.loop(0, n_updates // 2)
    def _(layer):
        exchange(2 * layer, 0, contract_outgoing, None)
        exchange(2 * layer + 1, 1, contract_incoming, layer < n_updates // 2 - 1)


def solution(mesh):
    n_dap, n_dap2 = mesh.shape["dap"], mesh.shape["dap2"]
    n_all = n_dap * n_dap2
    pair_spec = P(("data", "dap"), "dap2", None)
    mask_spec = P(("data", "dap"), "dap2")

    def local_stack(pair_act, pair_mask, ln_z, w_ab, w_g, ln_x, w_o):
        rows, cols, width = pair_act.shape
        n_updates = w_o.shape[0] * w_o.shape[1]
        full = rows * n_dap
        pitch, stage_pitch = rows + 8, CHUNK + 8
        n_chunks = rows // CHUNK
        flat = [array.reshape(n_updates, *array.shape[2:]) for array in (ln_z, w_ab, w_g, ln_x, w_o)]
        vmem = pl.BlockSpec(memory_space=pltpu.VMEM)
        return pl.pallas_call(
            functools.partial(kernel, n_dap, n_dap2, n_updates),
            out_shape=jax.ShapeDtypeStruct((rows, cols, width), jnp.float32),
            in_specs=[vmem] * 7,
            out_specs=vmem,
            scratch_shapes=[
                pltpu.VMEM((rows, LANES), jnp.float32),
                pltpu.VMEM((6 * width, width), jnp.bfloat16),
                pltpu.VMEM((rows, width, LANES), jnp.float32),
                pltpu.VMEM((rows, width, LANES), jnp.bfloat16),
                pltpu.VMEM((2 * TILES, n_all * stage_pitch, LANES), jnp.float32),
                pltpu.VMEM((n_all, 2 * TILES, rows, LANES), jnp.bfloat16),
                pltpu.VMEM((2, 2 * TILES, full, n_dap2 * LANES), jnp.bfloat16),
                pltpu.VMEM((full, n_dap2 * LANES), jnp.bfloat16),
                pltpu.VMEM((n_dap2, TILES, full, LANES), jnp.float32),
                pltpu.VMEM((TILES, n_all * pitch, LANES), jnp.float32),
                pltpu.VMEM((4, width, LANES), jnp.float32),
                pltpu.SemaphoreType.DMA((n_chunks + 1,)),
                pltpu.SemaphoreType.DMA((2, n_chunks + 1)),
                pltpu.SemaphoreType.DMA((2,)),
                pltpu.SemaphoreType.DMA((2,)),
            ],
            compiler_params=pltpu.CompilerParams(collective_id=0, has_side_effects=True, vmem_limit_bytes=60 * 1024 * 1024),
            name="triangle_stack",
        )(pair_act, pair_mask, *flat)

    return jax.shard_map(local_stack, mesh=mesh, in_specs=(pair_spec, mask_spec, P(), P(), P(), P(), P()), out_specs=pair_spec, check_vma=False)
```

```python
import functools

import jax
import jax.numpy as jnp
from jax import lax
from jax.experimental import pallas as pl
from jax.experimental.pallas import tpu as pltpu
from jax.sharding import PartitionSpec as P

LN_EPS = 1e-5
LANES = 128
GROUPS = 4
TILES = 3
CHUNK = 16
UNROLL = 8
MESH = pl.DeviceIdType.MESH


def lane_iota(shape):
    return lax.broadcasted_iota(jnp.int32, shape, len(shape) - 1)


def pack_tiles(blocks, cols):
    part = LANES - cols
    lane = lane_iota(blocks[0].shape)
    return [jnp.where(lane < cols, blocks[t], pltpu.roll(blocks[3], cols - part * t, 1)) for t in range(TILES)]


def last_group(tiles, cols):
    part = LANES - cols
    lane = lane_iota(tiles[0].shape)
    moved = [pltpu.roll(tiles[t], part * (t + 1), 1) for t in range(TILES)]
    return jnp.where(lane < part, moved[0], jnp.where(lane < 2 * part, moved[1], moved[2]))


def pack_columns(blocks, cols):
    part = LANES - cols
    lane = lane_iota(blocks[0].shape)
    tiles = []
    for t in range(TILES):
        moved = [block if g == t else pltpu.roll(block, part * (g - t) % LANES, 1) for g, block in enumerate(blocks)]
        tile = moved[GROUPS - 1]
        for g in reversed(range(GROUPS - 1)):
            tile = jnp.where(lane < part * (g + 1), moved[g], tile)
        tiles.append(tile)
    return tiles


def norm_sublanes(values, gain, bias):
    mean = jnp.mean(values, axis=0, keepdims=True)
    centered = values - mean
    variance = jnp.mean(centered * centered, axis=0, keepdims=True)
    return (centered * lax.rsqrt(variance + LN_EPS) * gain + bias).astype(jnp.bfloat16)


def kernel(n_dap, n_dap2, n_updates, z_ref, mask_ref, ln_z_ref, w_ab_ref, w_g_ref, ln_x_ref, w_o_ref, out_ref, m_ref, w_ref, zt, zn, stage, send, recv, bl, xs, xr, lnb,
           send_sem, recv_sem, xsend_sem, xrecv_sem):
    rows, cols, width = z_ref.shape
    n_all = n_dap * n_dap2
    pitch, stage_pitch = xr.shape[1] // n_all, stage.shape[1] // n_all
    per = width // GROUPS
    full = rows * n_dap
    n_chunks = rows // CHUNK
    halves = cols // rows
    my_p, my_q = lax.axis_index("dap"), lax.axis_index("dap2")
    me = my_p * n_dap2 + my_q

    barrier = pltpu.get_barrier_semaphore()

    @pl.loop(1, n_all)
    def _(off):
        peer = lax.rem(me + off, n_all)
        pl.semaphore_signal(barrier, inc=1, device_id={"dap": peer // n_dap2, "dap2": lax.rem(peer, n_dap2)}, device_id_type=MESH)

    def turn_columns(values):
        order = [values[h * rows + s * CHUNK:h * rows + (s + 1) * CHUNK] for s in range(n_chunks) for h in range(halves)]
        return jnp.concatenate(order, axis=0)

    def load_norm(first, norm_ref, update):
        params = norm_ref[update].astype(jnp.float32)
        for k in range(2):
            lnb[first + k] = jnp.broadcast_to(params[k:k + 1], (LANES, width)).T

    def load_projection(update):
        load_norm(0, ln_z_ref, update)
        for kind in range(4):
            turned = w_ab_ref[update, :, kind * width:(kind + 1) * width].T
            for g in range(GROUPS):
                w_ref[g * 4 * per + kind * per:g * 4 * per + (kind + 1) * per, :] = turned[g * per:(g + 1) * per]

    def load_finish(update):
        load_norm(2, ln_x_ref, update)
        w_ref[4 * width:5 * width, :] = w_g_ref[update].T
        w_ref[5 * width:6 * width, :] = w_o_ref[update].T

    def project_rows(indices, local, states, incoming):
        normed = [norm_sublanes(state, lnb[0], lnb[1]) for state in states]
        for i, n_row in zip(indices, normed):
            zn[i] = n_row
        keeps = [m_ref[pl.ds(i, 1), :] for i in indices]
        blocks = [([], []) for _ in indices]
        for g in range(GROUPS):
            weight = w_ref[g * 4 * per:(g + 1) * 4 * per, :]
            for keep, n_row, (a_blocks, b_blocks) in zip(keeps, normed, blocks):
                q = jnp.dot(weight, n_row, preferred_element_type=jnp.float32)
                a_blocks.append(jax.nn.sigmoid(q[per:2 * per]) * q[:per] * keep)
                b_blocks.append(jax.nn.sigmoid(q[3 * per:]) * q[2 * per:3 * per] * keep)
        for k, sides in zip(local, blocks):
            a_pack = pack_columns if incoming else pack_tiles
            for t, tile in enumerate([*pack_tiles(sides[1], cols), *a_pack(sides[0], cols)]):
                stage[t, pl.ds(k, n_all, stride=stage_pitch), :] = tile

    def finish_rows(indices):
        tiles = [[xr[t, pl.ds(i, n_all, stride=pitch), :] for t in range(TILES)] for i in indices]
        x_rows = [jnp.concatenate([*tile, last_group(tile, cols)], axis=0) for tile in tiles]
        gates = [jnp.dot(w_ref[4 * width:5 * width, :], zn[i], preferred_element_type=jnp.float32) for i in indices]
        normed = [norm_sublanes(x_row, lnb[2], lnb[3]) for x_row in x_rows]
        values = [jnp.dot(w_ref[5 * width:6 * width, :], x_norm, preferred_element_type=jnp.float32) for x_norm in normed]
        return [zt[i] + jax.nn.sigmoid(gate) * value for i, gate, value in zip(indices, gates, values)]

    def for_rows(r, body):
        @pl.loop(0, CHUNK // UNROLL)
        def _(k):
            local = [k * UNROLL + s for s in range(UNROLL)]
            body([r * CHUNK + i for i in local], local)

    def flip(value, bits, size):
        result, place = 0, 1
        while place < size:
            digit = lax.rem(lax.div(value, place), 2)
            result += place * lax.rem(digit + lax.rem(lax.div(bits, place), 2), 2)
            place *= 2
        return result

    def to_others(send_to):
        cores = 2
        steps = sorted(range(n_dap // cores), key=lambda step: (step == 0, step % 2 == 0, step))

        def column(k, skip):
            q = flip(my_q, k, n_dap2)
            for core in range(cores):
                for step in steps:
                    if not (skip and core == 0 and step == 0):
                        send_to(flip(my_p, jnp.int32(step * cores + core), n_dap), q)

        @pl.loop(0, n_dap2 - 1)
        def _(k):
            column(n_dap2 - 1 - k, False)

        column(jnp.int32(0), True)

    def chunk_rows(p, r):
        return pl.ds(pl.multiple_of(p * rows + r * CHUNK, CHUNK), CHUNK)

    def wait_bytes(ref, sem):
        pltpu.make_async_copy(ref, ref, sem).wait()

    def first_tiles(parity):
        return TILES + parity

    def send_part(parity, part, tiles, first_row, n_rows):
        row = pl.multiple_of(my_p * rows + first_row, CHUNK)
        slot = recv.at[parity, tiles, pl.ds(row, n_rows), pl.ds(pl.multiple_of(my_q * LANES, LANES), LANES)]
        here = pl.ds(pl.multiple_of(first_row, CHUNK), n_rows)
        pltpu.make_async_copy(send.at[me, tiles, here], slot, recv_sem.at[parity, part]).start()

        def send_to(p, q):
            pltpu.make_async_remote_copy(src_ref=send.at[p * n_dap2 + q, tiles, here], dst_ref=slot, send_sem=send_sem.at[part],
                                         recv_sem=recv_sem.at[parity, part], device_id={"dap": p, "dap2": q}, device_id_type=MESH).start()

        to_others(send_to)

    def pack_chunk(r):
        @pl.loop(0, n_all)
        def _(g):
            for t in range(2 * TILES):
                send[g, t, pl.ds(pl.multiple_of(r * CHUNK, CHUNK), CHUNK)] = stage[t, pl.ds(pl.multiple_of(g * stage_pitch, 8), CHUNK), :].astype(jnp.bfloat16)

    def send_chunk(r, parity):
        early, late = first_tiles(parity), 2 * TILES - first_tiles(parity)
        pack_chunk(r)
        send_part(parity, r, pl.ds(0, early), r * CHUNK, CHUNK)

        @pl.when(r == 0)
        def _():
            send_part(parity, n_chunks, pl.ds(early, late), 0, CHUNK)

        @pl.when(r == n_chunks - 1)
        def _():
            send_part(parity, n_chunks + 1, pl.ds(early, late), CHUNK, rows - CHUNK)

    def part_shape(parity, part):
        if part < n_chunks:
            return first_tiles(parity), CHUNK
        return 2 * TILES - first_tiles(parity), CHUNK if part == n_chunks else rows - CHUNK

    def wait_received(parity, part):
        tiles, n_rows = part_shape(parity, part)
        wait_bytes(recv.at[parity, pl.ds(0, tiles), pl.ds(0, n_dap * n_rows), :], recv_sem.at[parity, part])

    def wait_sent(parity, part):
        tiles, n_rows = part_shape(parity, part)
        wait_bytes(send.at[pl.ds(0, n_all - 1), pl.ds(0, tiles), pl.ds(0, n_rows)], send_sem.at[part])

    def send_x(r):
        def slots(p, q):
            return (xs.at[q, :, pl.ds(pl.multiple_of((r * n_dap + p) * CHUNK, CHUNK), CHUNK), :],
                    xr.at[:, pl.ds(pl.multiple_of(me * pitch + r * CHUNK, 8), CHUNK), :])

        pltpu.make_async_copy(*slots(my_p, my_q), xrecv_sem.at[r]).start()

        def send_to(p, q):
            src, dst = slots(p, q)
            pltpu.make_async_remote_copy(src_ref=src, dst_ref=dst, send_sem=xsend_sem.at[r], recv_sem=xrecv_sem.at[r],
                                         device_id={"dap": p, "dap2": q}, device_id_type=MESH).start()

        to_others(send_to)

    def contract_chunk(r, pair, blocks):
        for k in range(2):
            halved = [block[:, k * LANES:(k + 1) * LANES] for block in blocks]
            for t, tile in enumerate(pack_tiles(halved, cols)):
                xs[2 * pair + k, t, pl.ds(pl.multiple_of(r * n_dap * CHUNK, CHUNK), n_dap * CHUNK), :] = tile

    def gather_rows(ref, r):
        return jnp.concatenate([ref[chunk_rows(p, r), :] for p in range(n_dap)], axis=0)

    def contract_outgoing(parity):
        def chunk(r):
            @pl.when(r == 1)
            def _():
                wait_received(parity, n_chunks + 1)

            lane = lax.rem(lane_iota((n_dap * CHUNK, n_dap2 * LANES)), LANES)
            a_tiles = [gather_rows(recv.at[parity, TILES + t], r) for t in range(TILES)]
            zero = jnp.zeros_like(a_tiles[0])
            low = [jnp.where(lane < cols, a, zero) for a in a_tiles]
            high = [jnp.where(lane < cols, zero, a) for a in a_tiles]

            @pl.loop(0, n_dap2 // 2)
            def _(pair):
                def b_rows(t):
                    pieces = []
                    for k in range(2):
                        pieces += [recv[parity, t, chunk_rows((2 * pair + k) * halves + h, s), :] for s in range(n_chunks) for h in range(halves)]
                        pieces.append(jnp.zeros((LANES - cols, n_dap2 * LANES), jnp.bfloat16))
                    return jnp.concatenate(pieces, axis=0)

                def dot(a, b):
                    return lax.dot_general(a, b, (((1,), (1,)), ((), ())), preferred_element_type=jnp.float32)

                b_tiles = [b_rows(t) for t in range(TILES)]
                blocks = [dot(low[t], b_tiles[t]) for t in range(TILES)]
                blocks.append(dot(high[0], b_tiles[0]) + dot(high[1], b_tiles[1]) + dot(high[2], b_tiles[2]))
                contract_chunk(r, pair, blocks)

            send_x(r)

        for part in range(n_chunks + 1):
            wait_received(parity, part)
        pl.loop(0, n_chunks)(chunk)

    def contract_incoming(parity):
        def chunk(r):
            @pl.when(r == 1)
            def _():
                wait_received(parity, n_chunks + 1)

            part = LANES - cols
            turned = [recv[parity, TILES + r, :, q * LANES:(q + 1) * LANES].T for q in range(n_dap2)]
            a_all = [jnp.concatenate([a[g * part:(g + 1) * part] for a in turned], axis=0) for g in range(GROUPS)]

            @pl.loop(0, n_dap2 // 2)
            def _(pair):
                lanes = pl.ds(pl.multiple_of(pair * 2 * LANES, LANES), 2 * LANES)
                b_all = [*[recv[parity, t, :, lanes] for t in range(TILES)], bl[:, lanes]]
                contract_chunk(r, pair, [jnp.dot(a, b, preferred_element_type=jnp.float32) for a, b in zip(a_all, b_all)])

            send_x(r)

        @pl.loop(0, n_chunks)
        def _(r):
            wait_bytes(recv.at[parity, pl.ds(0, first_tiles(parity)), pl.ds(0, n_dap * CHUNK), :], recv_sem.at[parity, r])

            @pl.loop(0, n_dap // 2)
            def _(k):
                for here, q in [(chunk_rows(2 * k + h, r), q) for h in range(2) for q in range(n_dap2)]:
                    lanes = slice(q * LANES, (q + 1) * LANES)
                    tiles = [recv[parity, t, here, lanes].astype(jnp.float32) for t in range(TILES)]
                    bl[here, lanes] = last_group(tiles, cols).astype(jnp.bfloat16)

        wait_received(parity, n_chunks)
        pl.loop(0, n_chunks)(chunk)

    def exchange(update, parity, contract, more):
        contract(parity)
        for part in range(n_chunks + 2):
            wait_sent(parity, part)
        load_finish(update)

        def arrived(r):
            wait_bytes(xs.at[:, :, pl.ds(0, n_dap * CHUNK), :], xrecv_sem.at[r])

        def go_on():
            load_projection(update + 1)

            def body(indices, local):
                states = finish_rows(indices)
                for i, state in zip(indices, states):
                    zt[i] = state
                project_rows(indices, local, states, incoming=parity == 0)

            @pl.loop(0, n_chunks)
            def _(r):
                arrived(r)
                for_rows(r, body)
                send_chunk(r, 1 - parity)

        def end():
            @pl.loop(0, n_chunks)
            def _(r):
                arrived(r)

                def body(indices, local):
                    for i, state in zip(indices, finish_rows(indices)):
                        turned = state.T
                        for s in range(n_chunks):
                            for h in range(halves):
                                lane = (s * halves + h) * CHUNK
                                out_ref[i, h * rows + s * CHUNK:h * rows + (s + 1) * CHUNK, :] = turned[lane:lane + CHUNK]

                for_rows(r, body)

        if more is None:
            go_on()
        else:
            pl.when(more)(go_on)
            pl.when(jnp.logical_not(more))(end)
        for r in range(n_chunks):
            wait_bytes(xr.at[:, pl.ds(0, (n_all - 1) * CHUNK), :], xsend_sem.at[r])

    load_projection(0)
    m_ref[...] = jnp.zeros((rows, LANES), jnp.float32)
    m_ref[:, :cols] = turn_columns(mask_ref[...].astype(jnp.float32).T).T

    @pl.loop(0, rows // UNROLL)
    def _(k):
        for s in range(UNROLL):
            i = k * UNROLL + s
            zt[i] = jnp.concatenate([turn_columns(z_ref[i]).T, jnp.zeros((width, LANES - cols), jnp.float32)], axis=1)

    pl.semaphore_wait(barrier, n_all - 1)

    def first(indices, local):
        project_rows(indices, local, [zt[i] for i in indices], incoming=False)

    @pl.loop(0, n_chunks)
    def _(r):
        for_rows(r, first)
        send_chunk(r, 0)

    @pl.loop(0, n_updates // 2)
    def _(layer):
        exchange(2 * layer, 0, contract_outgoing, None)
        exchange(2 * layer + 1, 1, contract_incoming, layer < n_updates // 2 - 1)


def solution(mesh):
    n_dap, n_dap2 = mesh.shape["dap"], mesh.shape["dap2"]
    n_all = n_dap * n_dap2
    pair_spec = P(("data", "dap"), "dap2", None)
    mask_spec = P(("data", "dap"), "dap2")

    def local_stack(pair_act, pair_mask, ln_z, w_ab, w_g, ln_x, w_o):
        rows, cols, width = pair_act.shape
        n_updates = w_o.shape[0] * w_o.shape[1]
        full = rows * n_dap
        pitch, stage_pitch = rows + 8, CHUNK + 8
        n_chunks = rows // CHUNK
        flat = [array.reshape(n_updates, *array.shape[2:]) for array in (ln_z, w_ab, w_g, ln_x, w_o)]
        vmem = pl.BlockSpec(memory_space=pltpu.VMEM)
        return pl.pallas_call(
            functools.partial(kernel, n_dap, n_dap2, n_updates),
            out_shape=jax.ShapeDtypeStruct((rows, cols, width), jnp.float32),
            in_specs=[vmem] * 7,
            out_specs=vmem,
            scratch_shapes=[
                pltpu.VMEM((rows, LANES), jnp.float32),
                pltpu.VMEM((6 * width, width), jnp.bfloat16),
                pltpu.VMEM((rows, width, LANES), jnp.float32),
                pltpu.VMEM((rows, width, LANES), jnp.bfloat16),
                pltpu.VMEM((2 * TILES, n_all * stage_pitch, LANES), jnp.float32),
                pltpu.VMEM((n_all, 2 * TILES, rows, LANES), jnp.bfloat16),
                pltpu.VMEM((2, 2 * TILES, full, n_dap2 * LANES), jnp.bfloat16),
                pltpu.VMEM((full, n_dap2 * LANES), jnp.bfloat16),
                pltpu.VMEM((n_dap2, TILES, full, LANES), jnp.float32),
                pltpu.VMEM((TILES, n_all * pitch, LANES), jnp.float32),
                pltpu.VMEM((4, width, LANES), jnp.float32),
                pltpu.SemaphoreType.DMA((n_chunks + 2,)),
                pltpu.SemaphoreType.DMA((2, n_chunks + 2)),
                pltpu.SemaphoreType.DMA((n_chunks,)),
                pltpu.SemaphoreType.DMA((n_chunks,)),
            ],
            compiler_params=pltpu.CompilerParams(collective_id=0, has_side_effects=True, vmem_limit_bytes=60 * 1024 * 1024),
            name="triangle_stack",
        )(pair_act, pair_mask, *flat)

    return jax.shard_map(local_stack, mesh=mesh, in_specs=(pair_spec, mask_spec, P(), P(), P(), P(), P()), out_specs=pair_spec, check_vma=False)
```

```python
import functools
import math

import jax
import jax.numpy as jnp
from jax import lax
from jax.experimental import pallas as pl
from jax.experimental.pallas import tpu as pltpu
from jax.sharding import PartitionSpec as P

LN_EPS = 1e-5
LANES = 128
GROUPS = 4
TILES = 3
CHUNK = 16
UNROLL = 8
BATCH = 3
STRIDE = 13
MESH = pl.DeviceIdType.MESH


def lane_iota(shape):
    return lax.broadcasted_iota(jnp.int32, shape, len(shape) - 1)


def pack_tiles(blocks, cols):
    part = LANES - cols
    lane = lane_iota(blocks[0].shape)
    return [jnp.where(lane < cols, blocks[t], pltpu.roll(blocks[3], cols - part * t, 1)) for t in range(TILES)]


def last_group(tiles, cols):
    part = LANES - cols
    lane = lane_iota(tiles[0].shape)
    moved = [pltpu.roll(tiles[t], part * (t + 1), 1) for t in range(TILES)]
    return jnp.where(lane < part, moved[0], jnp.where(lane < 2 * part, moved[1], moved[2]))


def pack_columns(blocks, cols):
    part = LANES - cols
    lane = lane_iota(blocks[0].shape)
    tiles = []
    for t in range(TILES):
        moved = [block if g == t else pltpu.roll(block, part * (g - t) % LANES, 1) for g, block in enumerate(blocks)]
        tile = moved[GROUPS - 1]
        for g in reversed(range(GROUPS - 1)):
            tile = jnp.where(lane < part * (g + 1), moved[g], tile)
        tiles.append(tile)
    return tiles


def norm_sublanes(values, gain, bias):
    mean = jnp.mean(values, axis=0, keepdims=True)
    centered = values - mean
    variance = jnp.mean(centered * centered, axis=0, keepdims=True)
    return (centered * lax.rsqrt(variance + LN_EPS) * gain + bias).astype(jnp.bfloat16)


def kernel(n_dap, n_dap2, n_updates, z_ref, mask_ref, ln_z_ref, w_ab_ref, w_g_ref, ln_x_ref, w_o_ref, out_ref, m_ref, w_ref, zt, zn, stage, send, recv, bl, xs, xr, lnb,
           send_sem, recv_sem, xsend_sem, xrecv_sem):
    rows, cols, width = z_ref.shape
    n_all = n_dap * n_dap2
    pitch, stage_pitch = xr.shape[1] // n_all, stage.shape[1] // n_all
    per = width // GROUPS
    full = rows * n_dap
    n_chunks = rows // CHUNK
    halves = cols // rows
    my_p, my_q = lax.axis_index("dap"), lax.axis_index("dap2")
    me = my_p * n_dap2 + my_q

    barrier = pltpu.get_barrier_semaphore()

    @pl.loop(1, n_all)
    def _(off):
        peer = lax.rem(me + off, n_all)
        pl.semaphore_signal(barrier, inc=1, device_id={"dap": peer // n_dap2, "dap2": lax.rem(peer, n_dap2)}, device_id_type=MESH)

    def turn_columns(values):
        order = [values[h * rows + s * CHUNK:h * rows + (s + 1) * CHUNK] for s in range(n_chunks) for h in range(halves)]
        return jnp.concatenate(order, axis=0)

    def load_norm(first, norm_ref, update):
        params = norm_ref[update].astype(jnp.float32)
        for k in range(2):
            lnb[first + k] = jnp.broadcast_to(params[k:k + 1], (LANES, width)).T

    def load_projection(update):
        load_norm(0, ln_z_ref, update)
        for kind in range(4):
            turned = w_ab_ref[update, :, kind * width:(kind + 1) * width].T
            for g in range(GROUPS):
                w_ref[g * 4 * per + kind * per:g * 4 * per + (kind + 1) * per, :] = turned[g * per:(g + 1) * per]

    def load_finish(update):
        load_norm(2, ln_x_ref, update)
        w_ref[4 * width:5 * width, :] = w_g_ref[update].T
        w_ref[5 * width:6 * width, :] = w_o_ref[update].T

    def project_rows(indices, local, states, incoming):
        normed = [norm_sublanes(state, lnb[0], lnb[1]) for state in states]
        for i, n_row in zip(indices, normed):
            zn[i] = n_row
        keeps = [m_ref[pl.ds(i, 1), :] for i in indices]
        blocks = [([], []) for _ in indices]
        for g in range(GROUPS):
            weight = w_ref[g * 4 * per:(g + 1) * 4 * per, :]
            for keep, n_row, (a_blocks, b_blocks) in zip(keeps, normed, blocks):
                q = jnp.dot(weight, n_row, preferred_element_type=jnp.float32)
                a_blocks.append(jax.nn.sigmoid(q[per:2 * per]) * q[:per] * keep)
                b_blocks.append(jax.nn.sigmoid(q[3 * per:]) * q[2 * per:3 * per] * keep)
        for k, sides in zip(local, blocks):
            a_pack = pack_columns if incoming else pack_tiles
            for t, tile in enumerate([*pack_tiles(sides[1], cols), *a_pack(sides[0], cols)]):
                stage[t, pl.ds(k, n_all, stride=stage_pitch), :] = tile

    def finish_rows(indices):
        tiles = [[xr[t, pl.ds(i, n_all, stride=pitch), :] for t in range(TILES)] for i in indices]
        x_rows = [jnp.concatenate([*tile, last_group(tile, cols)], axis=0) for tile in tiles]
        gates = [jnp.dot(w_ref[4 * width:5 * width, :], zn[i], preferred_element_type=jnp.float32) for i in indices]
        normed = [norm_sublanes(x_row, lnb[2], lnb[3]) for x_row in x_rows]
        values = [jnp.dot(w_ref[5 * width:6 * width, :], x_norm, preferred_element_type=jnp.float32) for x_norm in normed]
        return [zt[i] + jax.nn.sigmoid(gate) * value for i, gate, value in zip(indices, gates, values)]

    def for_rows(r, body):
        @pl.loop(0, CHUNK // UNROLL)
        def _(k):
            local = [k * UNROLL + s for s in range(UNROLL)]
            body([r * CHUNK + i for i in local], local)

    def to_others(send_to):
        assert math.gcd(STRIDE, n_all) == 1
        def step(off):
            peer = lax.rem(me + off * STRIDE, n_all)
            send_to(lax.div(peer, n_dap2), lax.rem(peer, n_dap2))

        @pl.loop(0, (n_all - 1) // BATCH)
        def _(k):
            for s in range(BATCH):
                step(1 + k * BATCH + s)

        for off in range((n_all - 1) // BATCH * BATCH + 1, n_all):
            step(off)

    def chunk_rows(p, r):
        return pl.ds(pl.multiple_of(p * rows + r * CHUNK, CHUNK), CHUNK)

    def wait_bytes(ref, sem):
        pltpu.make_async_copy(ref, ref, sem).wait()

    def first_tiles(parity):
        return TILES + parity

    def send_part(parity, part, tiles, first_row, n_rows):
        row = pl.multiple_of(my_p * rows + first_row, CHUNK)
        slot = recv.at[parity, tiles, pl.ds(row, n_rows), pl.ds(pl.multiple_of(my_q * LANES, LANES), LANES)]
        here = pl.ds(pl.multiple_of(first_row, CHUNK), n_rows)
        pltpu.make_async_copy(send.at[me, tiles, here], slot, recv_sem.at[parity, part]).start()

        def send_to(p, q):
            pltpu.make_async_remote_copy(src_ref=send.at[p * n_dap2 + q, tiles, here], dst_ref=slot, send_sem=send_sem.at[part],
                                         recv_sem=recv_sem.at[parity, part], device_id={"dap": p, "dap2": q}, device_id_type=MESH).start()

        to_others(send_to)

    def pack_chunk(r):
        @pl.loop(0, n_all)
        def _(g):
            for t in range(2 * TILES):
                send[g, t, pl.ds(pl.multiple_of(r * CHUNK, CHUNK), CHUNK)] = stage[t, pl.ds(pl.multiple_of(g * stage_pitch, 8), CHUNK), :].astype(jnp.bfloat16)

    def send_chunk(r, parity):
        early, late = first_tiles(parity), 2 * TILES - first_tiles(parity)
        pack_chunk(r)
        send_part(parity, r, pl.ds(0, early), r * CHUNK, CHUNK)

        @pl.when(r == 0)
        def _():
            send_part(parity, n_chunks, pl.ds(early, late), 0, CHUNK)

        @pl.when(r == n_chunks - 1)
        def _():
            send_part(parity, n_chunks + 1, pl.ds(early, late), CHUNK, rows - CHUNK)

    def part_shape(parity, part):
        if part < n_chunks:
            return first_tiles(parity), CHUNK
        return 2 * TILES - first_tiles(parity), CHUNK if part == n_chunks else rows - CHUNK

    def wait_received(parity, part):
        tiles, n_rows = part_shape(parity, part)
        wait_bytes(recv.at[parity, pl.ds(0, tiles), pl.ds(0, n_dap * n_rows), :], recv_sem.at[parity, part])

    def wait_sent(parity, part):
        tiles, n_rows = part_shape(parity, part)
        wait_bytes(send.at[pl.ds(0, n_all - 1), pl.ds(0, tiles), pl.ds(0, n_rows)], send_sem.at[part])

    def send_x(r):
        def slots(p, q):
            return (xs.at[q, :, pl.ds(pl.multiple_of((r * n_dap + p) * CHUNK, CHUNK), CHUNK), :],
                    xr.at[:, pl.ds(pl.multiple_of(me * pitch + r * CHUNK, 8), CHUNK), :])

        pltpu.make_async_copy(*slots(my_p, my_q), xrecv_sem.at[r]).start()

        def send_to(p, q):
            src, dst = slots(p, q)
            pltpu.make_async_remote_copy(src_ref=src, dst_ref=dst, send_sem=xsend_sem.at[r], recv_sem=xrecv_sem.at[r],
                                         device_id={"dap": p, "dap2": q}, device_id_type=MESH).start()

        to_others(send_to)

    def contract_chunk(r, pair, blocks):
        for k in range(2):
            halved = [block[:, k * LANES:(k + 1) * LANES] for block in blocks]
            for t, tile in enumerate(pack_tiles(halved, cols)):
                xs[2 * pair + k, t, pl.ds(pl.multiple_of(r * n_dap * CHUNK, CHUNK), n_dap * CHUNK), :] = tile

    def gather_rows(ref, r):
        return jnp.concatenate([ref[chunk_rows(p, r), :] for p in range(n_dap)], axis=0)

    def contract_outgoing(parity):
        def chunk(r):
            @pl.when(r == 1)
            def _():
                wait_received(parity, n_chunks + 1)

            lane = lax.rem(lane_iota((n_dap * CHUNK, n_dap2 * LANES)), LANES)
            a_tiles = [gather_rows(recv.at[parity, TILES + t], r) for t in range(TILES)]
            zero = jnp.zeros_like(a_tiles[0])
            low = [jnp.where(lane < cols, a, zero) for a in a_tiles]
            high = [jnp.where(lane < cols, zero, a) for a in a_tiles]

            @pl.loop(0, n_dap2 // 2)
            def _(pair):
                def b_rows(t):
                    pieces = []
                    for k in range(2):
                        pieces += [recv[parity, t, chunk_rows((2 * pair + k) * halves + h, s), :] for s in range(n_chunks) for h in range(halves)]
                        pieces.append(jnp.zeros((LANES - cols, n_dap2 * LANES), jnp.bfloat16))
                    return jnp.concatenate(pieces, axis=0)

                def dot(a, b):
                    return lax.dot_general(a, b, (((1,), (1,)), ((), ())), preferred_element_type=jnp.float32)

                b_tiles = [b_rows(t) for t in range(TILES)]
                blocks = [dot(low[t], b_tiles[t]) for t in range(TILES)]
                blocks.append(dot(high[0], b_tiles[0]) + dot(high[1], b_tiles[1]) + dot(high[2], b_tiles[2]))
                contract_chunk(r, pair, blocks)

            send_x(r)

        for part in range(n_chunks + 1):
            wait_received(parity, part)
        pl.loop(0, n_chunks)(chunk)

    def contract_incoming(parity):
        def chunk(r):
            @pl.when(r == 1)
            def _():
                wait_received(parity, n_chunks + 1)

            part = LANES - cols
            turned = [recv[parity, TILES + r, :, q * LANES:(q + 1) * LANES].T for q in range(n_dap2)]
            a_all = [jnp.concatenate([a[g * part:(g + 1) * part] for a in turned], axis=0) for g in range(GROUPS)]

            @pl.loop(0, n_dap2 // 2)
            def _(pair):
                lanes = pl.ds(pl.multiple_of(pair * 2 * LANES, LANES), 2 * LANES)
                b_all = [*[recv[parity, t, :, lanes] for t in range(TILES)], bl[:, lanes]]
                contract_chunk(r, pair, [jnp.dot(a, b, preferred_element_type=jnp.float32) for a, b in zip(a_all, b_all)])

            send_x(r)

        @pl.loop(0, n_chunks)
        def _(r):
            wait_bytes(recv.at[parity, pl.ds(0, first_tiles(parity)), pl.ds(0, n_dap * CHUNK), :], recv_sem.at[parity, r])

            @pl.loop(0, n_dap // 2)
            def _(k):
                for here, q in [(chunk_rows(2 * k + h, r), q) for h in range(2) for q in range(n_dap2)]:
                    lanes = slice(q * LANES, (q + 1) * LANES)
                    tiles = [recv[parity, t, here, lanes].astype(jnp.float32) for t in range(TILES)]
                    bl[here, lanes] = last_group(tiles, cols).astype(jnp.bfloat16)

        wait_received(parity, n_chunks)
        pl.loop(0, n_chunks)(chunk)

    def exchange(update, parity, contract, more):
        contract(parity)
        for part in range(n_chunks + 2):
            wait_sent(parity, part)
        load_finish(update)

        def arrived(r):
            wait_bytes(xs.at[:, :, pl.ds(0, n_dap * CHUNK), :], xrecv_sem.at[r])

        def go_on():
            load_projection(update + 1)

            def body(indices, local):
                states = finish_rows(indices)
                for i, state in zip(indices, states):
                    zt[i] = state
                project_rows(indices, local, states, incoming=parity == 0)

            @pl.loop(0, n_chunks)
            def _(r):
                arrived(r)
                for_rows(r, body)
                send_chunk(r, 1 - parity)

        def end():
            @pl.loop(0, n_chunks)
            def _(r):
                arrived(r)

                def body(indices, local):
                    for i, state in zip(indices, finish_rows(indices)):
                        turned = state.T
                        for s in range(n_chunks):
                            for h in range(halves):
                                lane = (s * halves + h) * CHUNK
                                out_ref[i, h * rows + s * CHUNK:h * rows + (s + 1) * CHUNK, :] = turned[lane:lane + CHUNK]

                for_rows(r, body)

        if more is None:
            go_on()
        else:
            pl.when(more)(go_on)
            pl.when(jnp.logical_not(more))(end)
        for r in range(n_chunks):
            wait_bytes(xr.at[:, pl.ds(0, (n_all - 1) * CHUNK), :], xsend_sem.at[r])

    load_projection(0)
    m_ref[...] = jnp.zeros((rows, LANES), jnp.float32)
    m_ref[:, :cols] = turn_columns(mask_ref[...].astype(jnp.float32).T).T

    @pl.loop(0, rows // UNROLL)
    def _(k):
        for s in range(UNROLL):
            i = k * UNROLL + s
            zt[i] = jnp.concatenate([turn_columns(z_ref[i]).T, jnp.zeros((width, LANES - cols), jnp.float32)], axis=1)

    pl.semaphore_wait(barrier, n_all - 1)

    def first(indices, local):
        project_rows(indices, local, [zt[i] for i in indices], incoming=False)

    @pl.loop(0, n_chunks)
    def _(r):
        for_rows(r, first)
        send_chunk(r, 0)

    @pl.loop(0, n_updates // 2)
    def _(layer):
        exchange(2 * layer, 0, contract_outgoing, None)
        exchange(2 * layer + 1, 1, contract_incoming, layer < n_updates // 2 - 1)


def solution(mesh):
    n_dap, n_dap2 = mesh.shape["dap"], mesh.shape["dap2"]
    n_all = n_dap * n_dap2
    pair_spec = P(("data", "dap"), "dap2", None)
    mask_spec = P(("data", "dap"), "dap2")

    def local_stack(pair_act, pair_mask, ln_z, w_ab, w_g, ln_x, w_o):
        rows, cols, width = pair_act.shape
        n_updates = w_o.shape[0] * w_o.shape[1]
        full = rows * n_dap
        pitch, stage_pitch = rows + 8, CHUNK + 8
        n_chunks = rows // CHUNK
        flat = [array.reshape(n_updates, *array.shape[2:]) for array in (ln_z, w_ab, w_g, ln_x, w_o)]
        vmem = pl.BlockSpec(memory_space=pltpu.VMEM)
        return pl.pallas_call(
            functools.partial(kernel, n_dap, n_dap2, n_updates),
            out_shape=jax.ShapeDtypeStruct((rows, cols, width), jnp.float32),
            in_specs=[vmem] * 7,
            out_specs=vmem,
            scratch_shapes=[
                pltpu.VMEM((rows, LANES), jnp.float32),
                pltpu.VMEM((6 * width, width), jnp.bfloat16),
                pltpu.VMEM((rows, width, LANES), jnp.float32),
                pltpu.VMEM((rows, width, LANES), jnp.bfloat16),
                pltpu.VMEM((2 * TILES, n_all * stage_pitch, LANES), jnp.float32),
                pltpu.VMEM((n_all, 2 * TILES, rows, LANES), jnp.bfloat16),
                pltpu.VMEM((2, 2 * TILES, full, n_dap2 * LANES), jnp.bfloat16),
                pltpu.VMEM((full, n_dap2 * LANES), jnp.bfloat16),
                pltpu.VMEM((n_dap2, TILES, full, LANES), jnp.float32),
                pltpu.VMEM((TILES, n_all * pitch, LANES), jnp.float32),
                pltpu.VMEM((4, width, LANES), jnp.float32),
                pltpu.SemaphoreType.DMA((n_chunks + 2,)),
                pltpu.SemaphoreType.DMA((2, n_chunks + 2)),
                pltpu.SemaphoreType.DMA((n_chunks,)),
                pltpu.SemaphoreType.DMA((n_chunks,)),
            ],
            compiler_params=pltpu.CompilerParams(collective_id=0, has_side_effects=True, vmem_limit_bytes=60 * 1024 * 1024),
            name="triangle_stack",
        )(pair_act, pair_mask, *flat)

    return jax.shard_map(local_stack, mesh=mesh, in_specs=(pair_spec, mask_spec, P(), P(), P(), P(), P()), out_specs=pair_spec, check_vma=False)
```

```python
import functools

import jax
import jax.numpy as jnp
from jax import lax
from jax.experimental import pallas as pl
from jax.experimental.pallas import tpu as pltpu
from jax.sharding import PartitionSpec as P

LN_EPS = 1e-5
LANES = 128
GROUPS = 4
TILES = 3
CHUNK = 16
UNROLL = 8
BATCH = 3
MESH = pl.DeviceIdType.MESH


def lane_iota(shape):
    return lax.broadcasted_iota(jnp.int32, shape, len(shape) - 1)


def pack_tiles(blocks, cols):
    part = LANES - cols
    lane = lane_iota(blocks[0].shape)
    return [jnp.where(lane < cols, blocks[t], pltpu.roll(blocks[3], cols - part * t, 1)) for t in range(TILES)]


def last_group(tiles, cols):
    part = LANES - cols
    lane = lane_iota(tiles[0].shape)
    moved = [pltpu.roll(tiles[t], part * (t + 1), 1) for t in range(TILES)]
    return jnp.where(lane < part, moved[0], jnp.where(lane < 2 * part, moved[1], moved[2]))


def pack_columns(blocks, cols):
    part = LANES - cols
    lane = lane_iota(blocks[0].shape)
    tiles = []
    for t in range(TILES):
        moved = [block if g == t else pltpu.roll(block, part * (g - t) % LANES, 1) for g, block in enumerate(blocks)]
        tile = moved[GROUPS - 1]
        for g in reversed(range(GROUPS - 1)):
            tile = jnp.where(lane < part * (g + 1), moved[g], tile)
        tiles.append(tile)
    return tiles


def norm_sublanes(values, gain, bias):
    mean = jnp.mean(values, axis=0, keepdims=True)
    centered = values - mean
    variance = jnp.mean(centered * centered, axis=0, keepdims=True)
    return (centered * lax.rsqrt(variance + LN_EPS) * gain + bias).astype(jnp.bfloat16)


def kernel(n_dap, n_dap2, n_updates, z_ref, mask_ref, ln_z_ref, w_ab_ref, w_g_ref, ln_x_ref, w_o_ref, out_ref, m_ref, w_ref, zt, zn, stage, send, recv, bl, xs, xr, lnb,
           send_sem, recv_sem, xsend_sem, xrecv_sem):
    rows, cols, width = z_ref.shape
    n_all = n_dap * n_dap2
    pitch, stage_pitch = xr.shape[1] // n_all, stage.shape[1] // n_all
    per = width // GROUPS
    full = rows * n_dap
    n_chunks = rows // CHUNK
    halves = cols // rows
    my_p, my_q = lax.axis_index("dap"), lax.axis_index("dap2")
    me = my_p * n_dap2 + my_q

    barrier = pltpu.get_barrier_semaphore()

    @pl.loop(1, n_all)
    def _(off):
        peer = lax.rem(me + off, n_all)
        pl.semaphore_signal(barrier, inc=1, device_id={"dap": peer // n_dap2, "dap2": lax.rem(peer, n_dap2)}, device_id_type=MESH)

    def turn_columns(values):
        order = [values[h * rows + s * CHUNK:h * rows + (s + 1) * CHUNK] for s in range(n_chunks) for h in range(halves)]
        return jnp.concatenate(order, axis=0)

    def load_norm(first, norm_ref, update):
        params = norm_ref[update].astype(jnp.float32)
        for k in range(2):
            lnb[first + k] = jnp.broadcast_to(params[k:k + 1], (LANES, width)).T

    def load_projection(update):
        load_norm(0, ln_z_ref, update)
        for kind in range(4):
            turned = w_ab_ref[update, :, kind * width:(kind + 1) * width].T
            for g in range(GROUPS):
                w_ref[g * 4 * per + kind * per:g * 4 * per + (kind + 1) * per, :] = turned[g * per:(g + 1) * per]

    def load_finish(update):
        load_norm(2, ln_x_ref, update)
        w_ref[4 * width:5 * width, :] = w_g_ref[update].T
        w_ref[5 * width:6 * width, :] = w_o_ref[update].T

    def project_rows(indices, local, states, incoming):
        normed = [norm_sublanes(state, lnb[0], lnb[1]) for state in states]
        for i, n_row in zip(indices, normed):
            zn[i] = n_row
        keeps = [m_ref[pl.ds(i, 1), :] for i in indices]
        blocks = [([], []) for _ in indices]
        for g in range(GROUPS):
            weight = w_ref[g * 4 * per:(g + 1) * 4 * per, :]
            for keep, n_row, (a_blocks, b_blocks) in zip(keeps, normed, blocks):
                q = jnp.dot(weight, n_row, preferred_element_type=jnp.float32)
                a_blocks.append(jax.nn.sigmoid(q[per:2 * per]) * q[:per] * keep)
                b_blocks.append(jax.nn.sigmoid(q[3 * per:]) * q[2 * per:3 * per] * keep)
        for k, sides in zip(local, blocks):
            a_pack = pack_columns if incoming else pack_tiles
            for t, tile in enumerate([*pack_tiles(sides[1], cols), *a_pack(sides[0], cols)]):
                stage[t, pl.ds(k, n_all, stride=stage_pitch), :] = tile

    def finish_rows(indices):
        tiles = [[xr[t, pl.ds(i, n_all, stride=pitch), :] for t in range(TILES)] for i in indices]
        x_rows = [jnp.concatenate([*tile, last_group(tile, cols)], axis=0) for tile in tiles]
        gates = [jnp.dot(w_ref[4 * width:5 * width, :], zn[i], preferred_element_type=jnp.float32) for i in indices]
        normed = [norm_sublanes(x_row, lnb[2], lnb[3]) for x_row in x_rows]
        values = [jnp.dot(w_ref[5 * width:6 * width, :], x_norm, preferred_element_type=jnp.float32) for x_norm in normed]
        return [zt[i] + jax.nn.sigmoid(gate) * value for i, gate, value in zip(indices, gates, values)]

    def for_rows(r, body):
        @pl.loop(0, CHUNK // UNROLL)
        def _(k):
            local = [k * UNROLL + s for s in range(UNROLL)]
            body([r * CHUNK + i for i in local], local)

    def to_others(send_to):
        half = n_all // 2

        def step(off):
            peer = lax.rem(me + off, n_all)
            send_to(lax.div(peer, n_dap2), lax.rem(peer, n_dap2))

        step(half)

        @pl.loop(0, (half - 1) // BATCH)
        def _(k):
            for s in range(1, BATCH + 1):
                step(half + (k * BATCH + s))
                step(half - (k * BATCH + s))

        for off in range((half - 1) // BATCH * BATCH + 1, half):
            step(half + off)
            step(half - off)

    def chunk_rows(p, r):
        return pl.ds(pl.multiple_of(p * rows + r * CHUNK, CHUNK), CHUNK)

    def wait_bytes(ref, sem):
        pltpu.make_async_copy(ref, ref, sem).wait()

    def first_tiles(parity):
        return TILES + parity

    def send_part(parity, part, tiles, first_row, n_rows):
        row = pl.multiple_of(my_p * rows + first_row, CHUNK)
        slot = recv.at[parity, tiles, pl.ds(row, n_rows), pl.ds(pl.multiple_of(my_q * LANES, LANES), LANES)]
        here = pl.ds(pl.multiple_of(first_row, CHUNK), n_rows)
        pltpu.make_async_copy(send.at[me, tiles, here], slot, recv_sem.at[parity, part]).start()

        def send_to(p, q):
            pltpu.make_async_remote_copy(src_ref=send.at[p * n_dap2 + q, tiles, here], dst_ref=slot, send_sem=send_sem.at[part],
                                         recv_sem=recv_sem.at[parity, part], device_id={"dap": p, "dap2": q}, device_id_type=MESH).start()

        to_others(send_to)

    def pack_chunk(r):
        @pl.loop(0, n_all)
        def _(g):
            for t in range(2 * TILES):
                send[g, t, pl.ds(pl.multiple_of(r * CHUNK, CHUNK), CHUNK)] = stage[t, pl.ds(pl.multiple_of(g * stage_pitch, 8), CHUNK), :].astype(jnp.bfloat16)

    def send_chunk(r, parity):
        early, late = first_tiles(parity), 2 * TILES - first_tiles(parity)
        pack_chunk(r)
        send_part(parity, r, pl.ds(0, early), r * CHUNK, CHUNK)

        @pl.when(r == 0)
        def _():
            send_part(parity, n_chunks, pl.ds(early, late), 0, CHUNK)

        @pl.when(r == n_chunks - 1)
        def _():
            send_part(parity, n_chunks + 1, pl.ds(early, late), CHUNK, rows - CHUNK)

    def part_shape(parity, part):
        if part < n_chunks:
            return first_tiles(parity), CHUNK
        return 2 * TILES - first_tiles(parity), CHUNK if part == n_chunks else rows - CHUNK

    def wait_received(parity, part):
        tiles, n_rows = part_shape(parity, part)
        wait_bytes(recv.at[parity, pl.ds(0, tiles), pl.ds(0, n_dap * n_rows), :], recv_sem.at[parity, part])

    def wait_sent(parity, part):
        tiles, n_rows = part_shape(parity, part)
        wait_bytes(send.at[pl.ds(0, n_all - 1), pl.ds(0, tiles), pl.ds(0, n_rows)], send_sem.at[part])

    def send_x(r):
        def slots(p, q):
            return (xs.at[q, :, pl.ds(pl.multiple_of((r * n_dap + p) * CHUNK, CHUNK), CHUNK), :],
                    xr.at[:, pl.ds(pl.multiple_of(me * pitch + r * CHUNK, 8), CHUNK), :])

        pltpu.make_async_copy(*slots(my_p, my_q), xrecv_sem.at[r]).start()

        def send_to(p, q):
            src, dst = slots(p, q)
            pltpu.make_async_remote_copy(src_ref=src, dst_ref=dst, send_sem=xsend_sem.at[r], recv_sem=xrecv_sem.at[r],
                                         device_id={"dap": p, "dap2": q}, device_id_type=MESH).start()

        to_others(send_to)

    def contract_chunk(r, pair, blocks):
        for k in range(2):
            halved = [block[:, k * LANES:(k + 1) * LANES] for block in blocks]
            for t, tile in enumerate(pack_tiles(halved, cols)):
                xs[2 * pair + k, t, pl.ds(pl.multiple_of(r * n_dap * CHUNK, CHUNK), n_dap * CHUNK), :] = tile

    def gather_rows(ref, r):
        return jnp.concatenate([ref[chunk_rows(p, r), :] for p in range(n_dap)], axis=0)

    def contract_outgoing(parity):
        def chunk(r):
            @pl.when(r == 1)
            def _():
                wait_received(parity, n_chunks + 1)

            lane = lax.rem(lane_iota((n_dap * CHUNK, n_dap2 * LANES)), LANES)
            a_tiles = [gather_rows(recv.at[parity, TILES + t], r) for t in range(TILES)]
            zero = jnp.zeros_like(a_tiles[0])
            low = [jnp.where(lane < cols, a, zero) for a in a_tiles]
            high = [jnp.where(lane < cols, zero, a) for a in a_tiles]

            @pl.loop(0, n_dap2 // 2)
            def _(pair):
                def b_rows(t):
                    pieces = []
                    for k in range(2):
                        pieces += [recv[parity, t, chunk_rows((2 * pair + k) * halves + h, s), :] for s in range(n_chunks) for h in range(halves)]
                        pieces.append(jnp.zeros((LANES - cols, n_dap2 * LANES), jnp.bfloat16))
                    return jnp.concatenate(pieces, axis=0)

                def dot(a, b):
                    return lax.dot_general(a, b, (((1,), (1,)), ((), ())), preferred_element_type=jnp.float32)

                b_tiles = [b_rows(t) for t in range(TILES)]
                blocks = [dot(low[t], b_tiles[t]) for t in range(TILES)]
                blocks.append(dot(high[0], b_tiles[0]) + dot(high[1], b_tiles[1]) + dot(high[2], b_tiles[2]))
                contract_chunk(r, pair, blocks)

            send_x(r)

        for part in range(n_chunks + 1):
            wait_received(parity, part)
        pl.loop(0, n_chunks)(chunk)

    def contract_incoming(parity):
        def chunk(r):
            @pl.when(r == 1)
            def _():
                wait_received(parity, n_chunks + 1)

            part = LANES - cols
            turned = [recv[parity, TILES + r, :, q * LANES:(q + 1) * LANES].T for q in range(n_dap2)]
            a_all = [jnp.concatenate([a[g * part:(g + 1) * part] for a in turned], axis=0) for g in range(GROUPS)]

            @pl.loop(0, n_dap2 // 2)
            def _(pair):
                lanes = pl.ds(pl.multiple_of(pair * 2 * LANES, LANES), 2 * LANES)
                b_all = [*[recv[parity, t, :, lanes] for t in range(TILES)], bl[:, lanes]]
                contract_chunk(r, pair, [jnp.dot(a, b, preferred_element_type=jnp.float32) for a, b in zip(a_all, b_all)])

            send_x(r)

        @pl.loop(0, n_chunks)
        def _(r):
            wait_bytes(recv.at[parity, pl.ds(0, first_tiles(parity)), pl.ds(0, n_dap * CHUNK), :], recv_sem.at[parity, r])

            @pl.loop(0, n_dap // 2)
            def _(k):
                for here, q in [(chunk_rows(2 * k + h, r), q) for h in range(2) for q in range(n_dap2)]:
                    lanes = slice(q * LANES, (q + 1) * LANES)
                    tiles = [recv[parity, t, here, lanes].astype(jnp.float32) for t in range(TILES)]
                    bl[here, lanes] = last_group(tiles, cols).astype(jnp.bfloat16)

        wait_received(parity, n_chunks)
        pl.loop(0, n_chunks)(chunk)

    def exchange(update, parity, contract, more):
        contract(parity)
        for part in range(n_chunks + 2):
            wait_sent(parity, part)
        load_finish(update)

        def arrived(r):
            wait_bytes(xs.at[:, :, pl.ds(0, n_dap * CHUNK), :], xrecv_sem.at[r])

        def go_on():
            load_projection(update + 1)

            def body(indices, local):
                states = finish_rows(indices)
                for i, state in zip(indices, states):
                    zt[i] = state
                project_rows(indices, local, states, incoming=parity == 0)

            @pl.loop(0, n_chunks)
            def _(r):
                arrived(r)
                for_rows(r, body)
                send_chunk(r, 1 - parity)

        def end():
            @pl.loop(0, n_chunks)
            def _(r):
                arrived(r)

                def body(indices, local):
                    for i, state in zip(indices, finish_rows(indices)):
                        turned = state.T
                        for s in range(n_chunks):
                            for h in range(halves):
                                lane = (s * halves + h) * CHUNK
                                out_ref[i, h * rows + s * CHUNK:h * rows + (s + 1) * CHUNK, :] = turned[lane:lane + CHUNK]

                for_rows(r, body)

        if more is None:
            go_on()
        else:
            pl.when(more)(go_on)
            pl.when(jnp.logical_not(more))(end)
        for r in range(n_chunks):
            wait_bytes(xr.at[:, pl.ds(0, (n_all - 1) * CHUNK), :], xsend_sem.at[r])

    load_projection(0)
    m_ref[...] = jnp.zeros((rows, LANES), jnp.float32)
    m_ref[:, :cols] = turn_columns(mask_ref[...].astype(jnp.float32).T).T

    @pl.loop(0, rows // UNROLL)
    def _(k):
        for s in range(UNROLL):
            i = k * UNROLL + s
            zt[i] = jnp.concatenate([turn_columns(z_ref[i]).T, jnp.zeros((width, LANES - cols), jnp.float32)], axis=1)

    pl.semaphore_wait(barrier, n_all - 1)

    def first(indices, local):
        project_rows(indices, local, [zt[i] for i in indices], incoming=False)

    @pl.loop(0, n_chunks)
    def _(r):
        for_rows(r, first)
        send_chunk(r, 0)

    @pl.loop(0, n_updates // 2)
    def _(layer):
        exchange(2 * layer, 0, contract_outgoing, None)
        exchange(2 * layer + 1, 1, contract_incoming, layer < n_updates // 2 - 1)


def solution(mesh):
    n_dap, n_dap2 = mesh.shape["dap"], mesh.shape["dap2"]
    n_all = n_dap * n_dap2
    pair_spec = P(("data", "dap"), "dap2", None)
    mask_spec = P(("data", "dap"), "dap2")

    def local_stack(pair_act, pair_mask, ln_z, w_ab, w_g, ln_x, w_o):
        rows, cols, width = pair_act.shape
        n_updates = w_o.shape[0] * w_o.shape[1]
        full = rows * n_dap
        pitch, stage_pitch = rows + 8, CHUNK + 8
        n_chunks = rows // CHUNK
        flat = [array.reshape(n_updates, *array.shape[2:]) for array in (ln_z, w_ab, w_g, ln_x, w_o)]
        vmem = pl.BlockSpec(memory_space=pltpu.VMEM)
        return pl.pallas_call(
            functools.partial(kernel, n_dap, n_dap2, n_updates),
            out_shape=jax.ShapeDtypeStruct((rows, cols, width), jnp.float32),
            in_specs=[vmem] * 7,
            out_specs=vmem,
            scratch_shapes=[
                pltpu.VMEM((rows, LANES), jnp.float32),
                pltpu.VMEM((6 * width, width), jnp.bfloat16),
                pltpu.VMEM((rows, width, LANES), jnp.float32),
                pltpu.VMEM((rows, width, LANES), jnp.bfloat16),
                pltpu.VMEM((2 * TILES, n_all * stage_pitch, LANES), jnp.float32),
                pltpu.VMEM((n_all, 2 * TILES, rows, LANES), jnp.bfloat16),
                pltpu.VMEM((2, 2 * TILES, full, n_dap2 * LANES), jnp.bfloat16),
                pltpu.VMEM((full, n_dap2 * LANES), jnp.bfloat16),
                pltpu.VMEM((n_dap2, TILES, full, LANES), jnp.float32),
                pltpu.VMEM((TILES, n_all * pitch, LANES), jnp.float32),
                pltpu.VMEM((4, width, LANES), jnp.float32),
                pltpu.SemaphoreType.DMA((n_chunks + 2,)),
                pltpu.SemaphoreType.DMA((2, n_chunks + 2)),
                pltpu.SemaphoreType.DMA((n_chunks,)),
                pltpu.SemaphoreType.DMA((n_chunks,)),
            ],
            compiler_params=pltpu.CompilerParams(collective_id=0, has_side_effects=True, vmem_limit_bytes=60 * 1024 * 1024),
            name="triangle_stack",
        )(pair_act, pair_mask, *flat)

    return jax.shard_map(local_stack, mesh=mesh, in_specs=(pair_spec, mask_spec, P(), P(), P(), P(), P()), out_specs=pair_spec, check_vma=False)
```

```python
import functools

import jax
import jax.numpy as jnp
from jax import lax
from jax.experimental import pallas as pl
from jax.experimental.pallas import tpu as pltpu
from jax.sharding import PartitionSpec as P

LN_EPS = 1e-5
LANES = 128
GROUPS = 4
TILES = 3
CHUNK = 16
UNROLL = 8
BATCH = 3
MESH = pl.DeviceIdType.MESH


def lane_iota(shape):
    return lax.broadcasted_iota(jnp.int32, shape, len(shape) - 1)


def pack_tiles(blocks, cols):
    part = LANES - cols
    lane = lane_iota(blocks[0].shape)
    return [jnp.where(lane < cols, blocks[t], pltpu.roll(blocks[3], cols - part * t, 1)) for t in range(TILES)]


def last_group(tiles, cols):
    part = LANES - cols
    lane = lane_iota(tiles[0].shape)
    moved = [pltpu.roll(tiles[t], part * (t + 1), 1) for t in range(TILES)]
    return jnp.where(lane < part, moved[0], jnp.where(lane < 2 * part, moved[1], moved[2]))


def pack_columns(blocks, cols):
    part = LANES - cols
    lane = lane_iota(blocks[0].shape)
    tiles = []
    for t in range(TILES):
        moved = [block if g == t else pltpu.roll(block, part * (g - t) % LANES, 1) for g, block in enumerate(blocks)]
        tile = moved[GROUPS - 1]
        for g in reversed(range(GROUPS - 1)):
            tile = jnp.where(lane < part * (g + 1), moved[g], tile)
        tiles.append(tile)
    return tiles


def norm_sublanes(values, gain, bias):
    mean = jnp.mean(values, axis=0, keepdims=True)
    centered = values - mean
    variance = jnp.mean(centered * centered, axis=0, keepdims=True)
    return (centered * lax.rsqrt(variance + LN_EPS) * gain + bias).astype(jnp.bfloat16)


def kernel(n_dap, n_dap2, n_updates, z_ref, mask_ref, ln_z_ref, w_ab_ref, w_g_ref, ln_x_ref, w_o_ref, out_ref, m_ref, w_ref, zt, zn, stage, send, recv, bl, xs, xr, lnb,
           send_sem, recv_sem, xsend_sem, xrecv_sem):
    rows, cols, width = z_ref.shape
    n_all = n_dap * n_dap2
    pitch, stage_pitch = xr.shape[1] // n_all, stage.shape[1] // n_all
    per = width // GROUPS
    full = rows * n_dap
    n_chunks = rows // CHUNK
    halves = cols // rows
    my_p, my_q = lax.axis_index("dap"), lax.axis_index("dap2")
    me = my_p * n_dap2 + my_q

    barrier = pltpu.get_barrier_semaphore()

    @pl.loop(1, n_all)
    def _(off):
        peer = lax.rem(me + off, n_all)
        pl.semaphore_signal(barrier, inc=1, device_id={"dap": peer // n_dap2, "dap2": lax.rem(peer, n_dap2)}, device_id_type=MESH)

    def turn_columns(values):
        order = [values[h * rows + s * CHUNK:h * rows + (s + 1) * CHUNK] for s in range(n_chunks) for h in range(halves)]
        return jnp.concatenate(order, axis=0)

    def load_norm(first, norm_ref, update):
        params = norm_ref[update].astype(jnp.float32)
        for k in range(2):
            lnb[first + k] = jnp.broadcast_to(params[k:k + 1], (LANES, width)).T

    def load_projection(update):
        load_norm(0, ln_z_ref, update)
        for kind in range(4):
            turned = w_ab_ref[update, :, kind * width:(kind + 1) * width].T
            for g in range(GROUPS):
                w_ref[g * 4 * per + kind * per:g * 4 * per + (kind + 1) * per, :] = turned[g * per:(g + 1) * per]

    def load_finish(update):
        load_norm(2, ln_x_ref, update)
        w_ref[4 * width:5 * width, :] = w_g_ref[update].T
        w_ref[5 * width:6 * width, :] = w_o_ref[update].T

    def project_rows(indices, local, states, incoming):
        normed = [norm_sublanes(state, lnb[0], lnb[1]) for state in states]
        for i, n_row in zip(indices, normed):
            zn[i] = n_row
        keeps = [m_ref[pl.ds(i, 1), :] for i in indices]
        blocks = [([], []) for _ in indices]
        for g in range(GROUPS):
            weight = w_ref[g * 4 * per:(g + 1) * 4 * per, :]
            for keep, n_row, (a_blocks, b_blocks) in zip(keeps, normed, blocks):
                q = jnp.dot(weight, n_row, preferred_element_type=jnp.float32)
                a_blocks.append(jax.nn.sigmoid(q[per:2 * per]) * q[:per] * keep)
                b_blocks.append(jax.nn.sigmoid(q[3 * per:]) * q[2 * per:3 * per] * keep)
        for k, sides in zip(local, blocks):
            a_pack = pack_columns if incoming else pack_tiles
            for t, tile in enumerate([*pack_tiles(sides[1], cols), *a_pack(sides[0], cols)]):
                stage[t, pl.ds(k, n_all, stride=stage_pitch), :] = tile

    def finish_rows(indices):
        tiles = [[xr[t, pl.ds(i, n_all, stride=pitch), :] for t in range(TILES)] for i in indices]
        x_rows = [jnp.concatenate([*tile, last_group(tile, cols)], axis=0) for tile in tiles]
        gates = [jnp.dot(w_ref[4 * width:5 * width, :], zn[i], preferred_element_type=jnp.float32) for i in indices]
        normed = [norm_sublanes(x_row, lnb[2], lnb[3]) for x_row in x_rows]
        values = [jnp.dot(w_ref[5 * width:6 * width, :], x_norm, preferred_element_type=jnp.float32) for x_norm in normed]
        return [zt[i] + jax.nn.sigmoid(gate) * value for i, gate, value in zip(indices, gates, values)]

    def for_rows(r, body):
        @pl.loop(0, CHUNK // UNROLL)
        def _(k):
            local = [k * UNROLL + s for s in range(UNROLL)]
            body([r * CHUNK + i for i in local], local)

    def to_others(send_to):
        odd = lax.rem(my_p, 2)

        def step(off):
            peer = lax.rem(me + off + odd * (n_all - 2 * off), n_all)
            send_to(lax.div(peer, n_dap2), lax.rem(peer, n_dap2))

        @pl.loop(0, (n_all - 1) // BATCH)
        def _(k):
            for s in range(BATCH):
                step(1 + k * BATCH + s)

        for off in range((n_all - 1) // BATCH * BATCH + 1, n_all):
            step(off)

    def chunk_rows(p, r):
        return pl.ds(pl.multiple_of(p * rows + r * CHUNK, CHUNK), CHUNK)

    def wait_bytes(ref, sem):
        pltpu.make_async_copy(ref, ref, sem).wait()

    def first_tiles(parity):
        return TILES + parity

    def send_part(parity, part, tiles, first_row, n_rows):
        row = pl.multiple_of(my_p * rows + first_row, CHUNK)
        slot = recv.at[parity, tiles, pl.ds(row, n_rows), pl.ds(pl.multiple_of(my_q * LANES, LANES), LANES)]
        here = pl.ds(pl.multiple_of(first_row, CHUNK), n_rows)
        pltpu.make_async_copy(send.at[me, tiles, here], slot, recv_sem.at[parity, part]).start()

        def send_to(p, q):
            pltpu.make_async_remote_copy(src_ref=send.at[p * n_dap2 + q, tiles, here], dst_ref=slot, send_sem=send_sem.at[part],
                                         recv_sem=recv_sem.at[parity, part], device_id={"dap": p, "dap2": q}, device_id_type=MESH).start()

        to_others(send_to)

    def pack_chunk(r):
        @pl.loop(0, n_all)
        def _(g):
            for t in range(2 * TILES):
                send[g, t, pl.ds(pl.multiple_of(r * CHUNK, CHUNK), CHUNK)] = stage[t, pl.ds(pl.multiple_of(g * stage_pitch, 8), CHUNK), :].astype(jnp.bfloat16)

    def send_chunk(r, parity):
        early, late = first_tiles(parity), 2 * TILES - first_tiles(parity)
        pack_chunk(r)
        send_part(parity, r, pl.ds(0, early), r * CHUNK, CHUNK)

        @pl.when(r == 0)
        def _():
            send_part(parity, n_chunks, pl.ds(early, late), 0, CHUNK)

        @pl.when(r == n_chunks - 1)
        def _():
            send_part(parity, n_chunks + 1, pl.ds(early, late), CHUNK, rows - CHUNK)

    def part_shape(parity, part):
        if part < n_chunks:
            return first_tiles(parity), CHUNK
        return 2 * TILES - first_tiles(parity), CHUNK if part == n_chunks else rows - CHUNK

    def wait_received(parity, part):
        tiles, n_rows = part_shape(parity, part)
        wait_bytes(recv.at[parity, pl.ds(0, tiles), pl.ds(0, n_dap * n_rows), :], recv_sem.at[parity, part])

    def wait_sent(parity, part):
        tiles, n_rows = part_shape(parity, part)
        wait_bytes(send.at[pl.ds(0, n_all - 1), pl.ds(0, tiles), pl.ds(0, n_rows)], send_sem.at[part])

    def send_x(r):
        def slots(p, q):
            return (xs.at[q, :, pl.ds(pl.multiple_of((r * n_dap + p) * CHUNK, CHUNK), CHUNK), :],
                    xr.at[:, pl.ds(pl.multiple_of(me * pitch + r * CHUNK, 8), CHUNK), :])

        pltpu.make_async_copy(*slots(my_p, my_q), xrecv_sem.at[r]).start()

        def send_to(p, q):
            src, dst = slots(p, q)
            pltpu.make_async_remote_copy(src_ref=src, dst_ref=dst, send_sem=xsend_sem.at[r], recv_sem=xrecv_sem.at[r],
                                         device_id={"dap": p, "dap2": q}, device_id_type=MESH).start()

        to_others(send_to)

    def contract_chunk(r, pair, blocks):
        for k in range(2):
            halved = [block[:, k * LANES:(k + 1) * LANES] for block in blocks]
            for t, tile in enumerate(pack_tiles(halved, cols)):
                xs[2 * pair + k, t, pl.ds(pl.multiple_of(r * n_dap * CHUNK, CHUNK), n_dap * CHUNK), :] = tile

    def gather_rows(ref, r):
        return jnp.concatenate([ref[chunk_rows(p, r), :] for p in range(n_dap)], axis=0)

    def contract_outgoing(parity):
        def chunk(r):
            @pl.when(r == 1)
            def _():
                wait_received(parity, n_chunks + 1)

            lane = lax.rem(lane_iota((n_dap * CHUNK, n_dap2 * LANES)), LANES)
            a_tiles = [gather_rows(recv.at[parity, TILES + t], r) for t in range(TILES)]
            zero = jnp.zeros_like(a_tiles[0])
            low = [jnp.where(lane < cols, a, zero) for a in a_tiles]
            high = [jnp.where(lane < cols, zero, a) for a in a_tiles]

            @pl.loop(0, n_dap2 // 2)
            def _(pair):
                def b_rows(t):
                    pieces = []
                    for k in range(2):
                        pieces += [recv[parity, t, chunk_rows((2 * pair + k) * halves + h, s), :] for s in range(n_chunks) for h in range(halves)]
                        pieces.append(jnp.zeros((LANES - cols, n_dap2 * LANES), jnp.bfloat16))
                    return jnp.concatenate(pieces, axis=0)

                def dot(a, b):
                    return lax.dot_general(a, b, (((1,), (1,)), ((), ())), preferred_element_type=jnp.float32)

                b_tiles = [b_rows(t) for t in range(TILES)]
                blocks = [dot(low[t], b_tiles[t]) for t in range(TILES)]
                blocks.append(dot(high[0], b_tiles[0]) + dot(high[1], b_tiles[1]) + dot(high[2], b_tiles[2]))
                contract_chunk(r, pair, blocks)

            send_x(r)

        for part in range(n_chunks + 1):
            wait_received(parity, part)
        pl.loop(0, n_chunks)(chunk)

    def contract_incoming(parity):
        def chunk(r):
            @pl.when(r == 1)
            def _():
                wait_received(parity, n_chunks + 1)

            part = LANES - cols
            turned = [recv[parity, TILES + r, :, q * LANES:(q + 1) * LANES].T for q in range(n_dap2)]
            a_all = [jnp.concatenate([a[g * part:(g + 1) * part] for a in turned], axis=0) for g in range(GROUPS)]

            @pl.loop(0, n_dap2 // 2)
            def _(pair):
                lanes = pl.ds(pl.multiple_of(pair * 2 * LANES, LANES), 2 * LANES)
                b_all = [*[recv[parity, t, :, lanes] for t in range(TILES)], bl[:, lanes]]
                contract_chunk(r, pair, [jnp.dot(a, b, preferred_element_type=jnp.float32) for a, b in zip(a_all, b_all)])

            send_x(r)

        @pl.loop(0, n_chunks)
        def _(r):
            wait_bytes(recv.at[parity, pl.ds(0, first_tiles(parity)), pl.ds(0, n_dap * CHUNK), :], recv_sem.at[parity, r])

            @pl.loop(0, n_dap // 2)
            def _(k):
                for here, q in [(chunk_rows(2 * k + h, r), q) for h in range(2) for q in range(n_dap2)]:
                    lanes = slice(q * LANES, (q + 1) * LANES)
                    tiles = [recv[parity, t, here, lanes].astype(jnp.float32) for t in range(TILES)]
                    bl[here, lanes] = last_group(tiles, cols).astype(jnp.bfloat16)

        wait_received(parity, n_chunks)
        pl.loop(0, n_chunks)(chunk)

    def exchange(update, parity, contract, more):
        contract(parity)
        for part in range(n_chunks + 2):
            wait_sent(parity, part)
        load_finish(update)

        def arrived(r):
            wait_bytes(xs.at[:, :, pl.ds(0, n_dap * CHUNK), :], xrecv_sem.at[r])

        def go_on():
            load_projection(update + 1)

            def body(indices, local):
                states = finish_rows(indices)
                for i, state in zip(indices, states):
                    zt[i] = state
                project_rows(indices, local, states, incoming=parity == 0)

            @pl.loop(0, n_chunks)
            def _(r):
                arrived(r)
                for_rows(r, body)
                send_chunk(r, 1 - parity)

        def end():
            @pl.loop(0, n_chunks)
            def _(r):
                arrived(r)

                def body(indices, local):
                    for i, state in zip(indices, finish_rows(indices)):
                        turned = state.T
                        for s in range(n_chunks):
                            for h in range(halves):
                                lane = (s * halves + h) * CHUNK
                                out_ref[i, h * rows + s * CHUNK:h * rows + (s + 1) * CHUNK, :] = turned[lane:lane + CHUNK]

                for_rows(r, body)

        if more is None:
            go_on()
        else:
            pl.when(more)(go_on)
            pl.when(jnp.logical_not(more))(end)
        for r in range(n_chunks):
            wait_bytes(xr.at[:, pl.ds(0, (n_all - 1) * CHUNK), :], xsend_sem.at[r])

    load_projection(0)
    m_ref[...] = jnp.zeros((rows, LANES), jnp.float32)
    m_ref[:, :cols] = turn_columns(mask_ref[...].astype(jnp.float32).T).T

    @pl.loop(0, rows // UNROLL)
    def _(k):
        for s in range(UNROLL):
            i = k * UNROLL + s
            zt[i] = jnp.concatenate([turn_columns(z_ref[i]).T, jnp.zeros((width, LANES - cols), jnp.float32)], axis=1)

    pl.semaphore_wait(barrier, n_all - 1)

    def first(indices, local):
        project_rows(indices, local, [zt[i] for i in indices], incoming=False)

    @pl.loop(0, n_chunks)
    def _(r):
        for_rows(r, first)
        send_chunk(r, 0)

    @pl.loop(0, n_updates // 2)
    def _(layer):
        exchange(2 * layer, 0, contract_outgoing, None)
        exchange(2 * layer + 1, 1, contract_incoming, layer < n_updates // 2 - 1)


def solution(mesh):
    n_dap, n_dap2 = mesh.shape["dap"], mesh.shape["dap2"]
    n_all = n_dap * n_dap2
    pair_spec = P(("data", "dap"), "dap2", None)
    mask_spec = P(("data", "dap"), "dap2")

    def local_stack(pair_act, pair_mask, ln_z, w_ab, w_g, ln_x, w_o):
        rows, cols, width = pair_act.shape
        n_updates = w_o.shape[0] * w_o.shape[1]
        full = rows * n_dap
        pitch, stage_pitch = rows + 8, CHUNK + 8
        n_chunks = rows // CHUNK
        flat = [array.reshape(n_updates, *array.shape[2:]) for array in (ln_z, w_ab, w_g, ln_x, w_o)]
        vmem = pl.BlockSpec(memory_space=pltpu.VMEM)
        return pl.pallas_call(
            functools.partial(kernel, n_dap, n_dap2, n_updates),
            out_shape=jax.ShapeDtypeStruct((rows, cols, width), jnp.float32),
            in_specs=[vmem] * 7,
            out_specs=vmem,
            scratch_shapes=[
                pltpu.VMEM((rows, LANES), jnp.float32),
                pltpu.VMEM((6 * width, width), jnp.bfloat16),
                pltpu.VMEM((rows, width, LANES), jnp.float32),
                pltpu.VMEM((rows, width, LANES), jnp.bfloat16),
                pltpu.VMEM((2 * TILES, n_all * stage_pitch, LANES), jnp.float32),
                pltpu.VMEM((n_all, 2 * TILES, rows, LANES), jnp.bfloat16),
                pltpu.VMEM((2, 2 * TILES, full, n_dap2 * LANES), jnp.bfloat16),
                pltpu.VMEM((full, n_dap2 * LANES), jnp.bfloat16),
                pltpu.VMEM((n_dap2, TILES, full, LANES), jnp.float32),
                pltpu.VMEM((TILES, n_all * pitch, LANES), jnp.float32),
                pltpu.VMEM((4, width, LANES), jnp.float32),
                pltpu.SemaphoreType.DMA((n_chunks + 2,)),
                pltpu.SemaphoreType.DMA((2, n_chunks + 2)),
                pltpu.SemaphoreType.DMA((n_chunks,)),
                pltpu.SemaphoreType.DMA((n_chunks,)),
            ],
            compiler_params=pltpu.CompilerParams(collective_id=0, has_side_effects=True, vmem_limit_bytes=60 * 1024 * 1024),
            name="triangle_stack",
        )(pair_act, pair_mask, *flat)

    return jax.shard_map(local_stack, mesh=mesh, in_specs=(pair_spec, mask_spec, P(), P(), P(), P(), P()), out_specs=pair_spec, check_vma=False)
```

```python
import functools

import jax
import jax.numpy as jnp
from jax import lax
from jax.experimental import pallas as pl
from jax.experimental.pallas import tpu as pltpu
from jax.sharding import PartitionSpec as P

LN_EPS = 1e-5
LANES = 128
GROUPS = 4
TILES = 3
CHUNK = 16
UNROLL = 8
BATCH = 3
MESH = pl.DeviceIdType.MESH


def lane_iota(shape):
    return lax.broadcasted_iota(jnp.int32, shape, len(shape) - 1)


def pack_tiles(blocks, cols):
    part = LANES - cols
    lane = lane_iota(blocks[0].shape)
    return [jnp.where(lane < cols, blocks[t], pltpu.roll(blocks[3], cols - part * t, 1)) for t in range(TILES)]


def last_group(tiles, cols):
    part = LANES - cols
    lane = lane_iota(tiles[0].shape)
    moved = [pltpu.roll(tiles[t], part * (t + 1), 1) for t in range(TILES)]
    return jnp.where(lane < part, moved[0], jnp.where(lane < 2 * part, moved[1], moved[2]))


def pack_columns(blocks, cols):
    part = LANES - cols
    lane = lane_iota(blocks[0].shape)
    tiles = []
    for t in range(TILES):
        moved = [block if g == t else pltpu.roll(block, part * (g - t) % LANES, 1) for g, block in enumerate(blocks)]
        tile = moved[GROUPS - 1]
        for g in reversed(range(GROUPS - 1)):
            tile = jnp.where(lane < part * (g + 1), moved[g], tile)
        tiles.append(tile)
    return tiles


def norm_sublanes(values, gain, bias):
    mean = jnp.mean(values, axis=0, keepdims=True)
    centered = values - mean
    variance = jnp.mean(centered * centered, axis=0, keepdims=True)
    return (centered * lax.rsqrt(variance + LN_EPS) * gain + bias).astype(jnp.bfloat16)


def kernel(n_dap, n_dap2, n_updates, z_ref, mask_ref, ln_z_ref, w_ab_ref, w_g_ref, ln_x_ref, w_o_ref, out_ref, m_ref, w_ref, zt, zn, stage, send, recv, bl, xs, xr, lnb,
           send_sem, recv_sem, xsend_sem, xrecv_sem):
    rows, cols, width = z_ref.shape
    n_all = n_dap * n_dap2
    pitch, stage_pitch = xr.shape[1] // n_all, stage.shape[1] // n_all
    per = width // GROUPS
    full = rows * n_dap
    n_chunks = rows // CHUNK
    halves = cols // rows
    my_p, my_q = lax.axis_index("dap"), lax.axis_index("dap2")
    me = my_p * n_dap2 + my_q

    barrier = pltpu.get_barrier_semaphore()

    @pl.loop(1, n_all)
    def _(off):
        peer = lax.rem(me + off, n_all)
        pl.semaphore_signal(barrier, inc=1, device_id={"dap": peer // n_dap2, "dap2": lax.rem(peer, n_dap2)}, device_id_type=MESH)

    def turn_columns(values):
        order = [values[h * rows + s * CHUNK:h * rows + (s + 1) * CHUNK] for s in range(n_chunks) for h in range(halves)]
        return jnp.concatenate(order, axis=0)

    def load_norm(first, norm_ref, update):
        params = norm_ref[update].astype(jnp.float32)
        for k in range(2):
            lnb[first + k] = jnp.broadcast_to(params[k:k + 1], (LANES, width)).T

    def load_projection(update):
        load_norm(0, ln_z_ref, update)
        for kind in range(4):
            turned = w_ab_ref[update, :, kind * width:(kind + 1) * width].T
            for g in range(GROUPS):
                w_ref[g * 4 * per + kind * per:g * 4 * per + (kind + 1) * per, :] = turned[g * per:(g + 1) * per]

    def load_finish(update):
        load_norm(2, ln_x_ref, update)
        w_ref[4 * width:5 * width, :] = w_g_ref[update].T
        w_ref[5 * width:6 * width, :] = w_o_ref[update].T

    def project_rows(indices, local, states, incoming):
        normed = [norm_sublanes(state, lnb[0], lnb[1]) for state in states]
        for i, n_row in zip(indices, normed):
            zn[i] = n_row
        keeps = [m_ref[pl.ds(i, 1), :] for i in indices]
        blocks = [([], []) for _ in indices]
        for g in range(GROUPS):
            weight = w_ref[g * 4 * per:(g + 1) * 4 * per, :]
            for keep, n_row, (a_blocks, b_blocks) in zip(keeps, normed, blocks):
                q = jnp.dot(weight, n_row, preferred_element_type=jnp.float32)
                a_blocks.append(jax.nn.sigmoid(q[per:2 * per]) * q[:per] * keep)
                b_blocks.append(jax.nn.sigmoid(q[3 * per:]) * q[2 * per:3 * per] * keep)
        for k, sides in zip(local, blocks):
            a_pack = pack_columns if incoming else pack_tiles
            for t, tile in enumerate([*pack_tiles(sides[1], cols), *a_pack(sides[0], cols)]):
                stage[t, pl.ds(k, n_all, stride=stage_pitch), :] = tile

    def finish_rows(indices):
        tiles = [[xr[t, pl.ds(i, n_all, stride=pitch), :] for t in range(TILES)] for i in indices]
        x_rows = [jnp.concatenate([*tile, last_group(tile, cols)], axis=0) for tile in tiles]
        gates = [jnp.dot(w_ref[4 * width:5 * width, :], zn[i], preferred_element_type=jnp.float32) for i in indices]
        normed = [norm_sublanes(x_row, lnb[2], lnb[3]) for x_row in x_rows]
        values = [jnp.dot(w_ref[5 * width:6 * width, :], x_norm, preferred_element_type=jnp.float32) for x_norm in normed]
        return [zt[i] + jax.nn.sigmoid(gate) * value for i, gate, value in zip(indices, gates, values)]

    def for_rows(r, body):
        @pl.loop(0, CHUNK // UNROLL)
        def _(k):
            local = [k * UNROLL + s for s in range(UNROLL)]
            body([r * CHUNK + i for i in local], local)

    def to_others(send_to):
        odd = lax.rem(my_p, 2)

        def step(off):
            peer = lax.rem(me + off + odd * (n_all - 2 * off), n_all)
            send_to(lax.div(peer, n_dap2), lax.rem(peer, n_dap2))

        @pl.loop(0, (n_all - 1) // BATCH)
        def _(k):
            for s in range(BATCH):
                step(1 + k * BATCH + s)

        for off in range((n_all - 1) // BATCH * BATCH + 1, n_all):
            step(off)

    def chunk_rows(p, r):
        return pl.ds(pl.multiple_of(p * rows + r * CHUNK, CHUNK), CHUNK)

    def wait_bytes(ref, sem):
        pltpu.make_async_copy(ref, ref, sem).wait()

    def first_tiles(parity):
        return TILES + parity

    def send_part(parity, part, tiles, first_row, n_rows):
        row = pl.multiple_of(my_p * rows + first_row, CHUNK)
        slot = recv.at[parity, tiles, pl.ds(row, n_rows), pl.ds(pl.multiple_of(my_q * LANES, LANES), LANES)]
        here = pl.ds(pl.multiple_of(first_row, CHUNK), n_rows)
        pltpu.make_async_copy(send.at[me, tiles, here], slot, recv_sem.at[parity, part]).start()

        def send_to(p, q):
            pltpu.make_async_remote_copy(src_ref=send.at[p * n_dap2 + q, tiles, here], dst_ref=slot, send_sem=send_sem.at[part],
                                         recv_sem=recv_sem.at[parity, part], device_id={"dap": p, "dap2": q}, device_id_type=MESH).start()

        to_others(send_to)

    def pack_chunk(r):
        @pl.loop(0, n_all)
        def _(g):
            for t in range(2 * TILES):
                send[g, t, pl.ds(pl.multiple_of(r * CHUNK, CHUNK), CHUNK)] = stage[t, pl.ds(pl.multiple_of(g * stage_pitch, 8), CHUNK), :].astype(jnp.bfloat16)

    def send_chunk(r, parity):
        early, late = first_tiles(parity), 2 * TILES - first_tiles(parity)
        pack_chunk(r)
        send_part(parity, r, pl.ds(0, early), r * CHUNK, CHUNK)

        if n_chunks in parts_of(parity):
            @pl.when(r == 0)
            def _():
                send_part(parity, n_chunks, pl.ds(early, late), 0, CHUNK)

        @pl.when(r == n_chunks - 1)
        def _():
            send_part(parity, n_chunks + 1, pl.ds(early, late), rows - late_rows(parity), late_rows(parity))

    def late_rows(parity):
        return rows if parity else rows - CHUNK

    def parts_of(parity):
        return [part for part in range(n_chunks + 2) if not (parity and part == n_chunks)]

    def part_shape(parity, part):
        if part < n_chunks:
            return first_tiles(parity), CHUNK
        return 2 * TILES - first_tiles(parity), CHUNK if part == n_chunks else late_rows(parity)

    def wait_received(parity, part):
        tiles, n_rows = part_shape(parity, part)
        wait_bytes(recv.at[parity, pl.ds(0, tiles), pl.ds(0, n_dap * n_rows), :], recv_sem.at[parity, part])

    def wait_sent(parity, part):
        tiles, n_rows = part_shape(parity, part)
        wait_bytes(send.at[pl.ds(0, n_all - 1), pl.ds(0, tiles), pl.ds(0, n_rows)], send_sem.at[part])

    def send_x(r):
        def slots(p, q):
            return (xs.at[q, :, pl.ds(pl.multiple_of((r * n_dap + p) * CHUNK, CHUNK), CHUNK), :],
                    xr.at[:, pl.ds(pl.multiple_of(me * pitch + r * CHUNK, 8), CHUNK), :])

        pltpu.make_async_copy(*slots(my_p, my_q), xrecv_sem.at[r]).start()

        def send_to(p, q):
            src, dst = slots(p, q)
            pltpu.make_async_remote_copy(src_ref=src, dst_ref=dst, send_sem=xsend_sem.at[r], recv_sem=xrecv_sem.at[r],
                                         device_id={"dap": p, "dap2": q}, device_id_type=MESH).start()

        to_others(send_to)

    def contract_chunk(r, pair, blocks):
        for k in range(2):
            halved = [block[:, k * LANES:(k + 1) * LANES] for block in blocks]
            for t, tile in enumerate(pack_tiles(halved, cols)):
                xs[2 * pair + k, t, pl.ds(pl.multiple_of(r * n_dap * CHUNK, CHUNK), n_dap * CHUNK), :] = tile

    def gather_rows(ref, r):
        return jnp.concatenate([ref[chunk_rows(p, r), :] for p in range(n_dap)], axis=0)

    def contract_outgoing(parity):
        def chunk(r):
            @pl.when(r == 1)
            def _():
                wait_received(parity, n_chunks + 1)

            lane = lax.rem(lane_iota((n_dap * CHUNK, n_dap2 * LANES)), LANES)
            a_tiles = [gather_rows(recv.at[parity, TILES + t], r) for t in range(TILES)]
            zero = jnp.zeros_like(a_tiles[0])
            low = [jnp.where(lane < cols, a, zero) for a in a_tiles]
            high = [jnp.where(lane < cols, zero, a) for a in a_tiles]

            @pl.loop(0, n_dap2 // 2)
            def _(pair):
                def b_rows(t):
                    pieces = []
                    for k in range(2):
                        pieces += [recv[parity, t, chunk_rows((2 * pair + k) * halves + h, s), :] for s in range(n_chunks) for h in range(halves)]
                        pieces.append(jnp.zeros((LANES - cols, n_dap2 * LANES), jnp.bfloat16))
                    return jnp.concatenate(pieces, axis=0)

                def dot(a, b):
                    return lax.dot_general(a, b, (((1,), (1,)), ((), ())), preferred_element_type=jnp.float32)

                b_tiles = [b_rows(t) for t in range(TILES)]
                blocks = [dot(low[t], b_tiles[t]) for t in range(TILES)]
                blocks.append(dot(high[0], b_tiles[0]) + dot(high[1], b_tiles[1]) + dot(high[2], b_tiles[2]))
                contract_chunk(r, pair, blocks)

            send_x(r)

        for part in range(n_chunks + 1):
            wait_received(parity, part)
        pl.loop(0, n_chunks)(chunk)

    def contract_incoming(parity):
        def chunk(r):
            @pl.when(r == 1)
            def _():
                wait_received(parity, n_chunks + 1)

            part = LANES - cols
            turned = [recv[parity, TILES + r, :, q * LANES:(q + 1) * LANES].T for q in range(n_dap2)]
            a_all = [jnp.concatenate([a[g * part:(g + 1) * part] for a in turned], axis=0) for g in range(GROUPS)]

            @pl.loop(0, n_dap2 // 2)
            def _(pair):
                lanes = pl.ds(pl.multiple_of(pair * 2 * LANES, LANES), 2 * LANES)
                b_all = [*[recv[parity, t, :, lanes] for t in range(TILES)], bl[:, lanes]]
                contract_chunk(r, pair, [jnp.dot(a, b, preferred_element_type=jnp.float32) for a, b in zip(a_all, b_all)])

            send_x(r)

        @pl.loop(0, n_chunks)
        def _(r):
            wait_bytes(recv.at[parity, pl.ds(0, first_tiles(parity)), pl.ds(0, n_dap * CHUNK), :], recv_sem.at[parity, r])

            @pl.loop(0, n_dap // 2)
            def _(k):
                for here, q in [(chunk_rows(2 * k + h, r), q) for h in range(2) for q in range(n_dap2)]:
                    lanes = slice(q * LANES, (q + 1) * LANES)
                    tiles = [recv[parity, t, here, lanes].astype(jnp.float32) for t in range(TILES)]
                    bl[here, lanes] = last_group(tiles, cols).astype(jnp.bfloat16)

        pl.loop(0, n_chunks)(chunk)

    def exchange(update, parity, contract, more):
        contract(parity)
        for part in parts_of(parity):
            wait_sent(parity, part)
        load_finish(update)

        def arrived(r):
            wait_bytes(xs.at[:, :, pl.ds(0, n_dap * CHUNK), :], xrecv_sem.at[r])

        def go_on():
            load_projection(update + 1)

            def body(indices, local):
                states = finish_rows(indices)
                for i, state in zip(indices, states):
                    zt[i] = state
                project_rows(indices, local, states, incoming=parity == 0)

            @pl.loop(0, n_chunks)
            def _(r):
                arrived(r)
                for_rows(r, body)
                send_chunk(r, 1 - parity)

        def end():
            @pl.loop(0, n_chunks)
            def _(r):
                arrived(r)

                def body(indices, local):
                    for i, state in zip(indices, finish_rows(indices)):
                        turned = state.T
                        for s in range(n_chunks):
                            for h in range(halves):
                                lane = (s * halves + h) * CHUNK
                                out_ref[i, h * rows + s * CHUNK:h * rows + (s + 1) * CHUNK, :] = turned[lane:lane + CHUNK]

                for_rows(r, body)

        if more is None:
            go_on()
        else:
            pl.when(more)(go_on)
            pl.when(jnp.logical_not(more))(end)
        for r in range(n_chunks):
            wait_bytes(xr.at[:, pl.ds(0, (n_all - 1) * CHUNK), :], xsend_sem.at[r])

    load_projection(0)
    m_ref[...] = jnp.zeros((rows, LANES), jnp.float32)
    m_ref[:, :cols] = turn_columns(mask_ref[...].astype(jnp.float32).T).T

    @pl.loop(0, rows // UNROLL)
    def _(k):
        for s in range(UNROLL):
            i = k * UNROLL + s
            zt[i] = jnp.concatenate([turn_columns(z_ref[i]).T, jnp.zeros((width, LANES - cols), jnp.float32)], axis=1)

    pl.semaphore_wait(barrier, n_all - 1)

    def first(indices, local):
        project_rows(indices, local, [zt[i] for i in indices], incoming=False)

    @pl.loop(0, n_chunks)
    def _(r):
        for_rows(r, first)
        send_chunk(r, 0)

    @pl.loop(0, n_updates // 2)
    def _(layer):
        exchange(2 * layer, 0, contract_outgoing, None)
        exchange(2 * layer + 1, 1, contract_incoming, layer < n_updates // 2 - 1)


def solution(mesh):
    n_dap, n_dap2 = mesh.shape["dap"], mesh.shape["dap2"]
    n_all = n_dap * n_dap2
    pair_spec = P(("data", "dap"), "dap2", None)
    mask_spec = P(("data", "dap"), "dap2")

    def local_stack(pair_act, pair_mask, ln_z, w_ab, w_g, ln_x, w_o):
        rows, cols, width = pair_act.shape
        n_updates = w_o.shape[0] * w_o.shape[1]
        full = rows * n_dap
        pitch, stage_pitch = rows + 8, CHUNK + 8
        n_chunks = rows // CHUNK
        flat = [array.reshape(n_updates, *array.shape[2:]) for array in (ln_z, w_ab, w_g, ln_x, w_o)]
        vmem = pl.BlockSpec(memory_space=pltpu.VMEM)
        return pl.pallas_call(
            functools.partial(kernel, n_dap, n_dap2, n_updates),
            out_shape=jax.ShapeDtypeStruct((rows, cols, width), jnp.float32),
            in_specs=[vmem] * 7,
            out_specs=vmem,
            scratch_shapes=[
                pltpu.VMEM((rows, LANES), jnp.float32),
                pltpu.VMEM((6 * width, width), jnp.bfloat16),
                pltpu.VMEM((rows, width, LANES), jnp.float32),
                pltpu.VMEM((rows, width, LANES), jnp.bfloat16),
                pltpu.VMEM((2 * TILES, n_all * stage_pitch, LANES), jnp.float32),
                pltpu.VMEM((n_all, 2 * TILES, rows, LANES), jnp.bfloat16),
                pltpu.VMEM((2, 2 * TILES, full, n_dap2 * LANES), jnp.bfloat16),
                pltpu.VMEM((full, n_dap2 * LANES), jnp.bfloat16),
                pltpu.VMEM((n_dap2, TILES, full, LANES), jnp.float32),
                pltpu.VMEM((TILES, n_all * pitch, LANES), jnp.float32),
                pltpu.VMEM((4, width, LANES), jnp.float32),
                pltpu.SemaphoreType.DMA((n_chunks + 2,)),
                pltpu.SemaphoreType.DMA((2, n_chunks + 2)),
                pltpu.SemaphoreType.DMA((n_chunks,)),
                pltpu.SemaphoreType.DMA((n_chunks,)),
            ],
            compiler_params=pltpu.CompilerParams(collective_id=0, has_side_effects=True, vmem_limit_bytes=60 * 1024 * 1024),
            name="triangle_stack",
        )(pair_act, pair_mask, *flat)

    return jax.shard_map(local_stack, mesh=mesh, in_specs=(pair_spec, mask_spec, P(), P(), P(), P(), P()), out_specs=pair_spec, check_vma=False)
```
